32 devices in a mesh: tx: 4 (over x, core), ty: 4 (over z), src: 2 (over y).
Axes of the slice: x: 2, y: 2, z: 4, core: 2. Of those that a mesh axis runs over, the one named last changes fastest.
Arguments:
- spectrum: bfloat16 [2, 512, 512], P(None, ('tx', 'ty'), 'src'), may hold values from -0.0234375 to 0.0234375
- pupil_mask: int32 [256, 256], replicated, may hold values 0 or 1
- source_shifts: int32 [64, 2], P('src'), may hold values from 0 to 256
- source_weights: int32 [64], P('src'), may hold values from 0 to 8, as said below
Outputs:
- acid_level: float32 [2048, 1024], P(('tx', 'src'), 'ty')
The draws below stay inside these ranges and needn't reach their ends.
Inputs may be any that keep to these rules, and one draw needn't show every extreme that they name: `source_weights`: the 32 consecutive sources of each group (one index of src) hold at least 4 points with weight above 0; some group has all 32 points on.
All inputs are finite; a program needn't handle non-finite values.
Results may differ from the reference program's by a relative error of at most 0.0017.
Values may be sent and summed in bfloat16 or wider, within the bound.
A program may use at most 64 MiB of HBM per device.

```python
import jax
import jax.numpy as jnp
from jax import lax

K = 256
MW = 512
FRAME = 2048
SRC_DEV = 32
SOURCES = 64
NX = 2048
NY = 1024


def slot_order(subkey):
    return jax.random.permutation(subkey, SRC_DEV)


def draw_source_weights(key, part):
    group_count = SOURCES // SRC_DEV
    subkeys = jax.random.split(jax.random.fold_in(key, 11), 4)
    counts = jax.random.randint(subkeys[0], (group_count,), SRC_DEV // 8, SRC_DEV // 2 + 1)
    full_group = jax.random.randint(subkeys[1], (), 0, group_count)
    counts = jnp.where(jnp.arange(group_count) == full_group, SRC_DEV, counts)
    slot_rank = jax.vmap(slot_order)(jax.random.split(subkeys[2], group_count))
    levels = jax.random.randint(subkeys[3], (group_count, SRC_DEV), 1, 9)
    levels = levels.at[full_group, 0].set(8)
    chosen = jnp.where(slot_rank < counts[:, None], levels, 0)
    return chosen.reshape(SOURCES).astype(jnp.int32)


def touch_ends(values, key, low, top_value):
    longest = values.shape.index(max(values.shape))
    spots = []
    for shift in (0, 1):
        where = [jax.random.randint(jax.random.fold_in(key, axis), (), 0, length) for axis, length in enumerate(values.shape)]
        where[longest] = (where[longest] + shift) % values.shape[longest]
        spots.append(tuple(where))
    return values.at[spots[0]].set(low).at[spots[1]].set(top_value)


def block_scale(key, dims, shards, least, high):
    factor_of = 1.0
    for dim, parts in shards:
        steps = jax.random.uniform(jax.random.fold_in(jax.random.fold_in(key, 6), dim), (parts,), jnp.float32, least / len(shards), high / len(shards))
        factor_of = factor_of * jnp.repeat(jnp.exp(steps), dims[dim] // parts).reshape((-1,) + (1,) * (len(dims) - 1 - dim))
    return factor_of


def centred(stream_key, shape, spread, most, cuts=(), kind=jnp.bfloat16):
    level = block_scale(stream_key, shape, cuts, -0.22, 0.18) if cuts else 1.0
    entries = jax.random.normal(stream_key, shape, jnp.float32) * spread * level
    return jnp.minimum(jnp.maximum(entries, -most), most).astype(kind)


def setup_inputs(seed: int = 0) -> dict:
    splits = jax.random.split(jax.random.key(seed), 5)
    return {
        "spectrum": centred(splits[0], (2, MW, MW), (K * K) ** -0.5, 0.0234375, ((1, 16), (2, 2))),
        "pupil_mask": touch_ends((jax.random.randint(splits[1], (K, K), 0, 4) < 3).astype(jnp.int32), jax.random.fold_in(splits[1], 1), 0, 1),
        "source_shifts": touch_ends(jax.random.randint(splits[2], (SOURCES, 2), 0, MW - K + 1), jax.random.fold_in(splits[2], 1), 0, MW - K).astype(jnp.int32),
        "source_weights": draw_source_weights(jax.random.fold_in(splits[4], 71), 0),
    }


diffusion_rate = 0.2


def phase_table(positions, frequency_count, frame_points):
    frequency = jnp.arange(frequency_count, dtype=jnp.int32) - frequency_count // 2
    phase_turns = (positions[:, None] * frequency[None, :]) % frame_points
    phase_angle = phase_turns.astype(jnp.float32) * (2.0 * jnp.pi / frame_points)
    return jnp.cos(phase_angle), jnp.sin(phase_angle)


def rotation_table(cosine, sine):
    upper = jnp.concatenate([cosine, -sine], axis=1)
    lower = jnp.concatenate([sine, cosine], axis=1)
    return jnp.concatenate([upper, lower], axis=0).astype(jnp.bfloat16)


def diffuse(level, padded):
    beside = padded[2:, 1:-1] + padded[:-2, 1:-1] + padded[1:-1, 2:] + padded[1:-1, :-2]
    return level + diffusion_rate * (beside - 4.0 * level)


def reference(spectrum, pupil_mask, source_shifts, source_weights):
    passband = pupil_mask.shape[0]
    pupil_bf = pupil_mask.astype(jnp.bfloat16)
    row_cos, row_sin = phase_table(jnp.arange(NX, dtype=jnp.int32), passband, FRAME)
    row_table = rotation_table(row_cos, row_sin).astype(jnp.float32)
    col_cos, col_sin = phase_table(jnp.arange(NY, dtype=jnp.int32), passband, FRAME)
    col_table = jnp.concatenate([col_cos.T, col_sin.T], axis=1).astype(jnp.bfloat16).astype(jnp.float32)

    def one_source(running, item):
        shift_pair, weight_value = item
        window_cut = lax.dynamic_slice(spectrum, (jnp.int32(0), shift_pair[0].astype(jnp.int32), shift_pair[1].astype(jnp.int32)), (2, passband, passband)) * pupil_bf
        product = jnp.dot(window_cut.reshape(2 * passband, passband).astype(jnp.float32), col_table)
        real_part = product[:passband, :NY] - product[passband:, NY:]
        imag_part = product[:passband, NY:] + product[passband:, :NY]
        inner_block = jnp.concatenate([real_part, imag_part], axis=0).astype(jnp.bfloat16)
        field_pair = jnp.dot(row_table, inner_block.astype(jnp.float32))
        square = field_pair[:NX] ** 2 + field_pair[NX:] ** 2
        return running + weight_value.astype(jnp.float32) * square, None

    intensity_sum, _ = lax.scan(one_source, jnp.zeros((NX, NY), jnp.float32), (source_shifts, source_weights))
    intensity = intensity_sum / (2.0 * SOURCES)
    acid_level = 1.0 - jnp.exp(-intensity)
    for repeat in range(2):
        padded = jnp.pad(acid_level, 1)
        acid_level = diffuse(acid_level, padded)
    return acid_level
```

```python
import functools
import math

import jax
import jax.numpy as jnp
from jax import lax
from jax.experimental import pallas as pl
from jax.experimental.pallas import tpu as pltpu
from jax.sharding import PartitionSpec as P

FRAME = 2048
LANES = 128
COLS = 256
EDGE = 8
PACK = 16
GROUP = 2
MESH = pl.DeviceIdType.MESH

diffusion_rate = 0.2


def wave(turns, period):
    quarter = period // 4
    turn = (turns + quarter // 2) // quarter
    angle = (turns - turn * quarter).astype(jnp.float32) * (2 * math.pi / period)
    square = angle * angle
    sine = angle * (1 + square * (-1 / 6 + square * (1 / 120 + square * (-1 / 5040 + square / 362880))))
    cosine = 1 + square * (-1 / 2 + square * (1 / 24 + square * (-1 / 720 + square / 40320)))
    odd = (turn & 1) == 1
    first, second = jnp.where(odd, sine, cosine), jnp.where(odd, cosine, sine)
    return jnp.where(((turn + 1) & 2) == 2, -first, first), jnp.where((turn & 2) == 2, -second, second)


def iota(shape, dim):
    return lax.broadcasted_iota(jnp.int32, shape, dim)


def dot(a, b):
    return jnp.dot(a, b, preferred_element_type=jnp.float32)


def flip_bits(index, mask):
    bit = 1
    while bit <= mask:
        if mask & bit:
            index = index + bit * (1 - 2 * lax.rem(index // bit, 2))
        bit *= 2
    return index


def others(index, count):
    if count & (count - 1) == 0:
        return [flip_bits(index, d) for d in range(1, count)]
    return [lax.rem(index + d, count) for d in range(1, count)]


def row_table(row_ref, block, blocks):
    count, half = row_ref.shape[0] // 2, row_ref.shape[1] // 2
    step = FRAME // (count * blocks)
    x = step * (blocks * iota((count, half), 0) + block)
    cosine, sine = wave((x * iota((count, half), 1)) & (FRAME - 1), FRAME)
    row_ref[:count, :half] = cosine.astype(jnp.bfloat16)
    row_ref[:count, half:] = (-sine).astype(jnp.bfloat16)
    row_ref[count:, :half] = sine.astype(jnp.bfloat16)
    row_ref[count:, half:] = cosine.astype(jnp.bfloat16)


def col_table(col_ref, t):
    length, cols = col_ref.shape[0], col_ref.shape[1] // 2
    y = t * cols + iota((length, cols), 1)
    cosine, sine = wave((y * iota((length, cols), 0)) & (FRAME - 1), FRAME)
    col_ref[:, :cols] = cosine.astype(jnp.bfloat16)
    col_ref[:, cols:] = sine.astype(jnp.bfloat16)


def masks(mask_ref, pupil_ref, block):
    half = pupil_ref.shape[0] // 2
    power = lax.rem(block, 4)
    real = (1 - 2 * lax.rem((power + 1) // 2, 2)).astype(jnp.float32)
    imag = (1 - 2 * (power // 2)).astype(jnp.float32)
    pupil = pupil_ref[...].astype(jnp.float32)
    mask_ref[0] = pupil[:half].astype(jnp.bfloat16)
    mask_ref[1] = (pupil[half:] * real).astype(jnp.bfloat16)
    mask_ref[2] = (pupil[half:] * imag).astype(jnp.bfloat16)


def blend_table(blend_ref, block, blocks):
    _, tall, samples = blend_ref.shape
    rows = tall - 2 * EDGE
    step = FRAME // samples
    count = samples // blocks
    x = block * rows - EDGE + iota((tall, samples), 0)
    column = iota((tall, samples), 1)
    owner = column // count
    gap = x - step * (blocks * (column - owner * count) + owner)
    gap = ((gap + FRAME // 2) & (FRAME - 1)) - FRAME // 2
    cosine, sine = wave(gap, 2 * FRAME)
    place = x & (2 * step - 1)
    scale = jnp.zeros_like(cosine)
    for n in range(2 * step):
        if n % step:
            scale = jnp.where(place == n, math.sin(math.pi * n / step) / samples, scale)
    scale = jnp.where((owner & 1) == 1, -scale, scale)
    here = gap == 0
    table = jnp.where(here, 1.0, scale * cosine / jnp.where(here, 1.0, sine))
    high = table.astype(jnp.bfloat16)
    blend_ref[0] = high
    blend_ref[1] = (table - high.astype(jnp.float32)).astype(jnp.bfloat16)


def gather_kernel(
    sizes, spec_hbm, shift_ref, weight_ref, pupil_hbm, all_ref, shifts_ref, weights_ref, row_ref, col_ref, mask_ref,
    blend_ref, spec_ref, pupil_ref, local_sem, send_sem, recv_sem, side_send, side_recv,
):
    tx_count, ty_count, src_count = sizes
    pair_count = tx_count // 2
    tx, t, s = lax.axis_index("tx"), lax.axis_index("ty"), lax.axis_index("src")
    pair, core = tx // 2, lax.rem(tx, 2)
    other_core = 1 - core
    far_t = others(t, ty_count)
    far_s = others(s, src_count)
    far_pair = others(pair, pair_count)

    def along_ty(i):
        return {"tx": tx, "ty": i, "src": s}

    def along_src(i):
        return {"tx": tx, "ty": t, "src": i}

    def along_pair(i):
        return {"tx": 2 * i + core, "ty": t, "src": s}

    loads = [
        pltpu.make_async_copy(src, dst, local_sem.at[n])
        for n, (src, dst) in enumerate(
            (
                (spec_hbm, spec_ref),
                (pupil_hbm, pupil_ref),
                (shift_ref, shifts_ref.at[s]),
                (weight_ref, weights_ref.at[s]),
            )
        )
    ]
    for load in loads:
        load.start()

    across = {"tx": 2 * pair + other_core, "ty": t, "src": s}
    partners = [along_ty(i) for i in far_t] + [along_src(i) for i in far_s]
    partners += [along_pair(i) for i in far_pair] + [across]
    barrier = pltpu.get_barrier_semaphore()
    for partner in partners:
        pl.semaphore_signal(barrier, inc=1, device_id=partner, device_id_type=MESH)
    pl.semaphore_wait(barrier, len(partners))
    loads[0].wait()

    started = []
    own = (tx, t, s)

    both = slice(None)

    def part(plane, piece):
        i, j, k = piece
        return all_ref.at[k, plane, i, j], recv_sem.at[0 if plane is both else plane, k, i, j]

    def send(plane, piece, device):
        slot, arrived = part(plane, piece)
        copy = pltpu.make_async_remote_copy(
            src_ref=spec_ref if piece is own else slot,
            dst_ref=slot,
            send_sem=send_sem.at[len(started)],
            recv_sem=arrived,
            device_id=device,
            device_id_type=MESH,
        )
        copy.start()
        started.append(copy)

    def arrive(plane, piece):
        slot, arrived = part(plane, piece)
        pltpu.make_async_remote_copy(
            src_ref=slot,
            dst_ref=slot,
            send_sem=send_sem.at[0],
            recv_sem=arrived,
            device_id=across,
            device_id_type=MESH,
        ).wait_recv()

    def spread(piece):
        for i in far_s:
            send(both, piece, along_src(i))
        for i in far_pair:
            send(both, piece, along_pair(i))

    for i in far_t:
        send(both, own, along_ty(i))
    spread(own)
    send(both, own, across)

    side = []
    for n, i in enumerate(far_s):
        for m, (src, dst) in enumerate(((shift_ref, shifts_ref), (weight_ref, weights_ref))):
            copy = pltpu.make_async_remote_copy(
                src_ref=src,
                dst_ref=dst.at[s],
                send_sem=side_send.at[m, n],
                recv_sem=side_recv.at[m, s],
                device_id=along_src(i),
                device_id_type=MESH,
            )
            copy.start()
            side.append(copy)

    for load in loads[1:]:
        load.wait()
    for plane in range(2):
        all_ref[s, plane, tx, t] = spec_ref[plane]
    block = tx * src_count + s
    row_table(row_ref, block, tx_count * src_count)
    col_table(col_ref, t)
    masks(mask_ref, pupil_ref, block)
    blend_table(blend_ref, block, tx_count * src_count)

    near_first = [t] + far_t
    for j in far_t:
        arrive(both, (tx, j, s))
        spread((tx, j, s))
    for j in near_first:
        for k in far_s:
            arrive(both, (tx, j, k))
            for i in far_pair:
                send(0, (tx, j, k), along_pair(i))
        for i in far_pair:
            there = 2 * i + core
            arrive(both, (there, j, s))
            for k in far_s:
                send(1, (there, j, s), along_src(k))
        if j is not t:
            send(both, (tx, j, s), across)
        for k in far_s:
            send(both, (tx, j, k), across)
        for i in far_pair:
            send(both, (2 * i + core, j, s), across)
    for j in near_first:
        for i in far_pair:
            for k in far_s:
                for plane in range(2):
                    arrive(plane, (2 * i + core, j, k))
                send(both, (2 * i + core, j, k), across)
    for j in near_first:
        for i in [pair] + far_pair:
            for k in [s] + far_s:
                arrive(both, (2 * i + other_core, j, k))
    for n, i in enumerate(far_s):
        for m, (src, dst) in enumerate(((shift_ref, shifts_ref), (weight_ref, weights_ref))):
            pltpu.make_async_remote_copy(
                src_ref=src,
                dst_ref=dst.at[i],
                send_sem=side_send.at[m, n],
                recv_sem=side_recv.at[m, i],
                device_id=across,
                device_id_type=MESH,
            ).wait_recv()
    for copy in started + side:
        copy.wait_send()


def gather(spectrum, source_shifts, source_weights, pupil_mask, sizes, cols):
    tx_count, ty_count, src_count = sizes
    pair_count = tx_count // 2
    _, block_rows, block_cols = spectrum.shape
    slots = source_weights.shape[0]
    length = pupil_mask.shape[0]
    blocks = tx_count * src_count
    samples = 2 * length
    vmem = pl.BlockSpec(memory_space=pltpu.VMEM)
    lines = pair_count * src_count * ty_count
    sends = ty_count - 1 + lines + ty_count * (src_count - 1 + pair_count - 1)
    sends += 2 * ty_count * (src_count - 1) * (pair_count - 1)
    return pl.pallas_call(
        functools.partial(gather_kernel, sizes),
        out_shape=(
            jax.ShapeDtypeStruct((src_count, 2, tx_count, ty_count, block_rows, block_cols), jnp.bfloat16),
            jax.ShapeDtypeStruct((src_count, 2, slots), jnp.int32),
            jax.ShapeDtypeStruct((src_count, 1, slots), jnp.int32),
            jax.ShapeDtypeStruct((2 * samples // blocks, length), jnp.bfloat16),
            jax.ShapeDtypeStruct((length, 2 * cols), jnp.bfloat16),
            jax.ShapeDtypeStruct((3, length // 2, length), jnp.bfloat16),
            jax.ShapeDtypeStruct((2, FRAME // blocks + 2 * EDGE, samples), jnp.bfloat16),
        ),
        in_specs=[pl.BlockSpec(memory_space=pltpu.HBM)] * 4,
        out_specs=(vmem,) * 7,
        scratch_shapes=[
            pltpu.VMEM(spectrum.shape, jnp.bfloat16),
            pltpu.VMEM(pupil_mask.shape, jnp.int32),
            pltpu.SemaphoreType.DMA((4,)),
            pltpu.SemaphoreType.DMA((sends,)),
            pltpu.SemaphoreType.DMA((2, src_count, tx_count, ty_count)),
            pltpu.SemaphoreType.DMA((2, src_count)),
            pltpu.SemaphoreType.DMA((2, src_count)),
        ],
        compiler_params=pltpu.CompilerParams(collective_id=0, has_side_effects=True, vmem_limit_bytes=12 << 20),
        name="gather",
    )(*(pltpu.with_memory_space_constraint(a, pltpu.HBM) for a in (spectrum, source_shifts.T, source_weights[None], pupil_mask)))


def image_kernel(
    sizes, shifts, weights, spec_ref, masks, row_ref, col_ref, out_ref, strip_ref,
    spec, acc, folded, inner, live_row, live_col, live_weight,
):
    _, _, part_count = sizes
    src_count, _, slots = weights.shape
    source_count = src_count * slots
    length = col_ref.shape[0]
    half = length // 2
    count_x = out_ref.shape[0]
    cols = out_ref.shape[1]
    height, part = spec_ref.shape[2:]
    tiles = src_count * part // LANES
    block = lax.axis_index("tx") * src_count + lax.axis_index("src")
    swap = lax.rem(block, 2)

    for plane in range(2):
        for tile in range(tiles):
            if part >= LANES:
                at = tile * LANES % part
                cell = spec_ref[tile * LANES // part, plane, :, at : at + LANES]
            else:
                first = tile * LANES // part
                cell = jnp.concatenate([spec_ref[k, plane] for k in range(first, first + LANES // part)], axis=1)
            spec[plane * tiles + tile] = cell.astype(jnp.float32)

    unroll = 8

    def pick(turn, count):
        for n in range(unroll):
            i = turn * unroll + n
            group, slot = i // slots, lax.rem(i, slots)
            weight = weights[group, 0, slot]
            live_row[count] = shifts[group, 0, slot]
            live_col[count] = shifts[group, 1, slot]
            live_weight[count + GROUP] = weight
            count = count + (weight > 0).astype(jnp.int32)
        return count

    for g in range(GROUP):
        live_weight[g] = 0
    count = lax.fori_loop(0, source_count // unroll, pick, jnp.int32(0))
    for g in range(4 * GROUP):
        live_row[count + g] = 0
        live_col[count + g] = 0
        live_weight[count + GROUP + g] = 0

    acc[...] = jnp.zeros_like(acc)
    lane = lax.broadcasted_iota(jnp.int32, (half, LANES), 1)

    def fold(a, b, slot):
        tile, rest = b // LANES, lax.rem(b, LANES)
        back = lax.rem(LANES - rest, LANES)
        keep = lane >= rest

        def window(plane, part):
            rows = pl.ds(a + part * half, half)
            base = plane * tiles
            found = [spec[base + jnp.minimum(tile + n, tiles - 1), rows, :] for n in range(length // LANES + 1)]
            return [
                pltpu.roll(jnp.where(keep, found[n], found[n + 1]), back, 1) for n in range(length // LANES)
            ]

        for plane in range(2):
            upper = window(plane, 0)
            lower = window(jnp.where(swap == 1, 1 - plane, plane), 1)
            for n in range(length // LANES):
                at = slice(n * LANES, (n + 1) * LANES)
                first = upper[n] * masks[0, :, at].astype(jnp.float32)
                second = lower[n] * masks[1 + plane, :, at].astype(jnp.float32)
                slot[half * plane : half * (plane + 1), at] = (first + second).astype(jnp.bfloat16)

    def step(n, parity):
        for g in range(GROUP):
            fold(live_row[(n + 1) * GROUP + g], live_col[(n + 1) * GROUP + g], folded[1 - parity].at[g])
        for g in range(GROUP):
            inner[parity][2 * count_x * g : 2 * count_x * (g + 1)] = dot(row_ref[...], folded[parity][g]).astype(jnp.bfloat16)
        wide = dot(inner[1 - parity][...], col_ref[...])
        total = acc[...]
        for g in range(GROUP):
            top = wide[2 * count_x * g : 2 * count_x * g + count_x]
            low = wide[2 * count_x * g + count_x : 2 * count_x * (g + 1)]
            real = top[:, :cols] - low[:, cols:]
            imag = top[:, cols:] + low[:, :cols]
            total += live_weight[n * GROUP + g].astype(jnp.float32) * (real * real + imag * imag)
        acc[...] = total

    inner[1][...] = jnp.zeros_like(inner[1])
    for g in range(GROUP):
        fold(live_row[g], live_col[g], folded[0].at[g])

    def turn_body(turn_index, carry):
        for g in range(2):
            step(turn_index * 2 + g, g)
        return carry

    steps = (count + GROUP - 1) // GROUP + 1
    lax.fori_loop(0, (steps + 1) // 2, turn_body, 0)
    level = acc[...] / (2.0 * source_count)
    out_ref[...] = level.astype(jnp.bfloat16)
    strip_ref[0] = level[:, :LANES].T[:PACK].astype(jnp.bfloat16)
    strip_ref[1] = level[:, cols - LANES :].T[LANES - PACK :].astype(jnp.bfloat16)


def image(spectrum, shifts, weights, row_table, col_table, masks, sizes):
    source_count = weights.shape[0] * weights.shape[2]
    src_count, _, height, part = spectrum.shape
    count_x, cols = row_table.shape[0] // 2, col_table.shape[1] // 2
    length = col_table.shape[0]
    smem = pl.BlockSpec(memory_space=pltpu.SMEM)
    vmem = pl.BlockSpec(memory_space=pltpu.VMEM)
    return pl.pallas_call(
        functools.partial(image_kernel, sizes),
        out_shape=(
            jax.ShapeDtypeStruct((count_x, cols), jnp.bfloat16),
            jax.ShapeDtypeStruct((2, PACK, count_x), jnp.bfloat16),
        ),
        in_specs=[smem, smem, vmem, vmem, vmem, vmem],
        out_specs=(vmem, vmem),
        scratch_shapes=[
            pltpu.VMEM((2 * src_count * part // LANES, height, LANES), jnp.float32),
            pltpu.VMEM((count_x, cols), jnp.float32),
            [pltpu.VMEM((GROUP, length, length), jnp.bfloat16)] * 2,
            [pltpu.VMEM((GROUP * 2 * count_x, length), jnp.bfloat16)] * 2,
        ]
        + [pltpu.SMEM((source_count + 6 * GROUP,), jnp.int32)] * 3,
        compiler_params=pltpu.CompilerParams(vmem_limit_bytes=16 << 20),
        name="image",
    )(shifts, weights, spectrum, masks, row_table, col_table)


def exchange_kernel(sizes, own_ref, strip_ref, all_ref, beside, send_sem, recv_sem, side_send, side_recv):
    tx_count, ty_count, src_count = sizes
    pair_count = tx_count // 2
    tx, t, s = lax.axis_index("tx"), lax.axis_index("ty"), lax.axis_index("src")
    pair, core = tx // 2, lax.rem(tx, 2)
    far_s = [s] + others(s, src_count)
    far_pair = [pair] + others(pair, pair_count)
    chips = [(i, k) for k in far_s for i in far_pair]

    def device(chip, other, z):
        return {"tx": 2 * chip[0] + (1 - core if other else core), "ty": z, "src": chip[1]}

    def block(chip, other):
        return (2 * chip[0] + (1 - core if other else core)) * src_count + chip[1]

    across = device(chips[0], True, t)
    barrier = pltpu.get_barrier_semaphore()

    def greet(chip, z):
        pl.semaphore_signal(barrier, inc=1, device_id=device(chip, False, z), device_id_type=MESH)

    has = (t > 0, t < ty_count - 1)
    beside[...] = jnp.zeros_like(beside)
    pl.semaphore_signal(barrier, inc=1, device_id=across, device_id_type=MESH)
    for chip in chips[1:]:
        greet(chip, t)
    for side in range(2):

        @pl.when(has[side])
        def _():
            for chip in chips:
                greet(chip, t + 2 * side - 1)

    all_ref[block(chips[0], False)] = own_ref[...]
    sides = jnp.minimum(t, 1) + jnp.minimum(ty_count - 1 - t, 1)
    pl.semaphore_wait(barrier, len(chips) * (1 + sides))

    def copy(src, dst, send, recv, target):
        return pltpu.make_async_remote_copy(
            src_ref=src, dst_ref=dst, send_sem=send, recv_sem=recv, device_id=target, device_id_type=MESH
        )

    def level_copy(n, chip, other, target, own=False):
        at = block(chip, other)
        return copy(own_ref if own else all_ref.at[at], all_ref.at[at], send_sem.at[n], recv_sem.at[at], target)

    def side_copy(n, side, chip, other, target, own=False):
        at = block(chip, other)
        slot = beside.at[side, at]
        return copy(strip_ref.at[1 - side] if own else slot, slot, side_send.at[side, n], side_recv.at[side, at], target)

    started = []
    for n, chip in enumerate(chips[1:]):
        started.append(level_copy(n, chips[0], False, device(chip, False, t), True))
        started[-1].start()
    for side in range(2):

        @pl.when(has[1 - side])
        def _():
            for n, chip in enumerate(chips):
                side_copy(n, side, chips[0], False, device(chip, False, t + 1 - 2 * side), True).start()

    n = len(chips) - 1
    started.append(level_copy(n, chips[0], False, across, True))
    started[-1].start()
    for chip in chips[1:]:
        n += 1
        level_copy(0, chip, False, across).wait_recv()
        started.append(level_copy(n, chip, False, across))
        started[-1].start()
    for side in range(2):

        @pl.when(has[side])
        def _():
            for n, chip in enumerate(chips):
                side_copy(0, side, chip, False, across).wait_recv()
                side_copy(len(chips) + n, side, chip, False, across).start()

    for chip in chips:
        level_copy(0, chip, True, across).wait_recv()
    for side in range(2):

        @pl.when(has[side])
        def _():
            for n, chip in enumerate(chips):
                side_copy(0, side, chip, True, across).wait_recv()
                side_copy(len(chips) + n, side, chip, False, across).wait_send()

        @pl.when(has[1 - side])
        def _():
            for n, chip in enumerate(chips):
                side_copy(n, side, chips[0], False, device(chip, False, t + 1 - 2 * side), True).wait_send()

    for one in started:
        one.wait_send()


def exchange(level, strips, sizes):
    tx_count, ty_count, src_count = sizes
    blocks = tx_count * src_count
    vmem = pl.BlockSpec(memory_space=pltpu.VMEM)
    return pl.pallas_call(
        functools.partial(exchange_kernel, sizes),
        out_shape=(
            jax.ShapeDtypeStruct((blocks,) + level.shape, level.dtype),
            jax.ShapeDtypeStruct((2, blocks) + strips.shape[1:], strips.dtype),
        ),
        in_specs=[vmem] * 2,
        out_specs=(vmem,) * 2,
        scratch_shapes=[
            pltpu.SemaphoreType.DMA((blocks,)),
            pltpu.SemaphoreType.DMA((blocks,)),
            pltpu.SemaphoreType.DMA((2, blocks)),
            pltpu.SemaphoreType.DMA((2, blocks)),
        ],
        compiler_params=pltpu.CompilerParams(collective_id=1, has_side_effects=True, vmem_limit_bytes=4 << 20),
        name="exchange",
    )(level, strips)


def diffuse_kernel(sizes, all_ref, beside, blend_ref, out_ref):
    tx_count, ty_count, src_count = sizes
    rows, cols = out_ref.shape
    blocks, count, _ = all_ref.shape
    samples = blocks * count
    tall = rows + 2 * EDGE
    level = all_ref[...].reshape(samples, cols)
    sides = [jnp.concatenate([beside[side, n] for n in range(blocks)], axis=1) for side in range(2)]
    strip = jnp.concatenate([sides[1], jnp.zeros((LANES - 2 * PACK, samples), jnp.bfloat16), sides[0]], axis=0)
    turned = (((1,), (1,)), ((), ()))
    middle = dot(blend_ref[0], level) + dot(blend_ref[1], level)
    edge = lax.dot_general(blend_ref[0], strip, turned, preferred_element_type=jnp.float32)
    edge += lax.dot_general(blend_ref[1], strip, turned, preferred_element_type=jnp.float32)
    acid = 1.0 - jnp.exp(-jnp.concatenate([middle, edge], axis=1))
    wide = cols + LANES
    row_block = lax.axis_index("tx") * src_count + lax.axis_index("src")
    col_block = lax.axis_index("ty")
    x = row_block * rows - EDGE + iota(acid.shape, 0)
    column = iota(acid.shape, 1)
    y = col_block * cols + jnp.where(column >= cols + LANES // 2, column - wide, column)
    inside = (x >= 0) & (x < blocks * rows) & (y >= 0) & (y < ty_count * cols)
    for repeat in range(2):
        acid = jnp.where(inside, acid, 0.0)
        near = (
            pltpu.roll(acid, 1, 0)
            + pltpu.roll(acid, tall - 1, 0)
            + pltpu.roll(acid, 1, 1)
            + pltpu.roll(acid, wide - 1, 1)
        )
        acid = acid + diffusion_rate * (near - 4.0 * acid)
    out_ref[...] = acid[EDGE : EDGE + rows, :cols]


def diffuse(levels, beside, blend, sizes):
    rows = blend.shape[1] - 2 * EDGE
    vmem = pl.BlockSpec(memory_space=pltpu.VMEM)
    return pl.pallas_call(
        functools.partial(diffuse_kernel, sizes),
        out_shape=jax.ShapeDtypeStruct((rows, levels.shape[2]), jnp.float32),
        in_specs=[vmem] * 3,
        out_specs=vmem,
        compiler_params=pltpu.CompilerParams(vmem_limit_bytes=12 << 20),
        name="diffuse",
    )(levels, beside, blend)


def body(sizes, cols, spectrum, pupil_mask, source_shifts, source_weights):
    pieces, shifts, weights, row_table, col_table, masks, blend = gather(
        spectrum, source_shifts, source_weights, pupil_mask, sizes, cols
    )
    src_count, _, tx_count, ty_count, block_rows, block_cols = pieces.shape
    columns = pieces.reshape(src_count, 2, tx_count * ty_count * block_rows, block_cols)
    level, strips = image(columns, shifts, weights, row_table, col_table, masks, sizes)
    levels, beside = exchange(level, strips, sizes)
    return diffuse(levels, beside, blend, sizes)


def solution(mesh):
    sizes = (mesh.shape["tx"], mesh.shape["ty"], mesh.shape["src"])
    placed = (P(None, ("tx", "ty"), "src"), P(), P("src", None), P("src"))
    return jax.shard_map(
        functools.partial(body, sizes, COLS),
        mesh=mesh,
        in_specs=placed,
        out_specs=P(("tx", "src"), "ty"),
        check_vma=False,
    )
```

```python
import functools
import math

import jax
import jax.numpy as jnp
from jax import lax
from jax.experimental import pallas as pl
from jax.experimental.pallas import tpu as pltpu
from jax.sharding import PartitionSpec as P

FRAME = 2048
LANES = 128
COLS = 256
EDGE = 8
PACK = 16
GROUP = 2
UNROLL = 4
MESH = pl.DeviceIdType.MESH

diffusion_rate = 0.2


def wave(turns, period):
    quarter = period // 4
    turn = (turns + quarter // 2) // quarter
    angle = (turns - turn * quarter).astype(jnp.float32) * (2 * math.pi / period)
    square = angle * angle
    sine = angle * (1 + square * (-1 / 6 + square * (1 / 120 + square * (-1 / 5040 + square / 362880))))
    cosine = 1 + square * (-1 / 2 + square * (1 / 24 + square * (-1 / 720 + square / 40320)))
    odd = (turn & 1) == 1
    first, second = jnp.where(odd, sine, cosine), jnp.where(odd, cosine, sine)
    return jnp.where(((turn + 1) & 2) == 2, -first, first), jnp.where((turn & 2) == 2, -second, second)


def iota(shape, dim):
    return lax.broadcasted_iota(jnp.int32, shape, dim)


def dot(a, b):
    return jnp.dot(a, b, preferred_element_type=jnp.float32)


def flip_bits(index, mask):
    bit = 1
    while bit <= mask:
        if mask & bit:
            index = index + bit * (1 - 2 * lax.rem(index // bit, 2))
        bit *= 2
    return index


def others(index, count):
    if count & (count - 1) == 0:
        return [flip_bits(index, d) for d in range(1, count)]
    return [lax.rem(index + d, count) for d in range(1, count)]


def nearest(index, count):
    orders = [sorted((i for i in range(count) if i != at), key=lambda i: (abs(i - at), i)) for at in range(count)]
    return [sum(jnp.where(index == at, orders[at][n], 0) for at in range(count)) for n in range(count - 1)]


def row_table(row_ref, count, block, blocks):
    half = row_ref.shape[0] // (2 * GROUP)
    each = LANES // GROUP
    step = FRAME // (count * blocks)
    sample = iota((half, each), 1)
    x = step * (blocks * sample + block)
    cosine, sine = wave((x * iota((half, each), 0)) & (FRAME - 1), FRAME)
    cosine = jnp.where(sample < count, cosine, 0.0)
    sine = jnp.where(sample < count, sine, 0.0)
    none = jnp.zeros((half, each), jnp.float32)
    for g in range(GROUP):
        for part, (real, imag) in enumerate(((cosine, sine), (-sine, cosine))):
            row = [real if n == g else none for n in range(GROUP)] + [imag if n == g else none for n in range(GROUP)]
            at = (2 * g + part) * half
            row_ref[at : at + half] = jnp.concatenate(row, axis=1).astype(jnp.bfloat16)


def col_table(col_ref, t):
    cols, length = col_ref.shape[0] // 2, col_ref.shape[1]
    chunk = 32

    def fill(n, carry):
        start = pl.multiple_of(n * chunk, chunk)
        y = t * cols + start + iota((chunk, length), 0)
        cosine, sine = wave((y * iota((chunk, length), 1)) & (FRAME - 1), FRAME)
        col_ref[pl.ds(start, chunk)] = cosine.astype(jnp.bfloat16)
        col_ref[pl.ds(cols + start, chunk)] = sine.astype(jnp.bfloat16)
        return carry

    lax.fori_loop(0, cols // chunk, fill, 0)


def blend_table(blend_ref, block, blocks):
    _, tall, samples = blend_ref.shape
    rows = tall - 2 * EDGE
    step = FRAME // samples
    count = samples // blocks
    chunk = PACK

    def fill(n, carry):
        start = pl.multiple_of(n * chunk, chunk)
        x = block * rows - EDGE + start + iota((chunk, samples), 0)
        column = iota((chunk, samples), 1)
        owner = column // count
        gap = x - step * (blocks * (column - owner * count) + owner)
        gap = ((gap + FRAME // 2) & (FRAME - 1)) - FRAME // 2
        cosine, sine = wave(gap, 2 * FRAME)
        place = block * rows - EDGE + start + iota((chunk, 1), 0)
        place = place & (2 * step - 1)
        scale = jnp.zeros((chunk, 1), jnp.float32)
        for n in range(2 * step):
            if n % step:
                scale = jnp.where(place == n, math.sin(math.pi * n / step) / samples, scale)
        scale = jnp.where((owner & 1) == 1, -scale, scale)
        here = gap == 0
        table = jnp.where(here, 1.0, scale * cosine / jnp.where(here, 1.0, sine))
        high = table.astype(jnp.bfloat16)
        blend_ref[0, pl.ds(start, chunk)] = high
        blend_ref[1, pl.ds(start, chunk)] = (table - high.astype(jnp.float32)).astype(jnp.bfloat16)
        return carry

    lax.fori_loop(0, tall // chunk, fill, 0)


def gather_kernel(
    sizes, spec_hbm, shift_ref, weight_ref, pupil_hbm, all_ref, shifts_ref, weights_ref, row_ref, col_ref, mask_ref,
    blend_ref, spec_ref, pupil_ref, local_sem, send_sem, recv_sem, side_send, side_recv,
):
    tx_count, ty_count, src_count = sizes
    pair_count = tx_count // 2
    tx, t, s = lax.axis_index("tx"), lax.axis_index("ty"), lax.axis_index("src")
    pair, core = tx // 2, lax.rem(tx, 2)
    other_core = 1 - core
    far_t = nearest(t, ty_count)
    far_s = others(s, src_count)
    far_pair = others(pair, pair_count)

    def along_ty(i):
        return {"tx": tx, "ty": i, "src": s}

    def along_src(i):
        return {"tx": tx, "ty": t, "src": i}

    def along_pair(i):
        return {"tx": 2 * i + core, "ty": t, "src": s}

    loads = [
        pltpu.make_async_copy(src, dst, local_sem.at[n])
        for n, (src, dst) in enumerate(
            (
                (spec_hbm, spec_ref),
                (pupil_hbm, pupil_ref),
                (shift_ref, shifts_ref.at[s]),
                (weight_ref, weights_ref.at[s]),
            )
        )
    ]
    for load in loads:
        load.start()

    across = {"tx": 2 * pair + other_core, "ty": t, "src": s}
    partners = [along_ty(i) for i in far_t] + [along_src(i) for i in far_s]
    partners += [along_pair(i) for i in far_pair] + [across]
    barrier = pltpu.get_barrier_semaphore()
    for partner in partners:
        pl.semaphore_signal(barrier, inc=1, device_id=partner, device_id_type=MESH)
    pl.semaphore_wait(barrier, len(partners))
    loads[0].wait()

    started = []
    own = (tx, t, s)

    both = slice(None)

    def part(plane, piece):
        i, j, k = piece
        return all_ref.at[k, plane, i, j], recv_sem.at[0 if plane is both else plane, k, i, j]

    def send(plane, piece, device):
        slot, arrived = part(plane, piece)
        copy = pltpu.make_async_remote_copy(
            src_ref=spec_ref if piece is own else slot,
            dst_ref=slot,
            send_sem=send_sem.at[len(started)],
            recv_sem=arrived,
            device_id=device,
            device_id_type=MESH,
        )
        copy.start()
        started.append(copy)

    def arrive(plane, piece):
        slot, arrived = part(plane, piece)
        pltpu.make_async_remote_copy(
            src_ref=slot,
            dst_ref=slot,
            send_sem=send_sem.at[0],
            recv_sem=arrived,
            device_id=across,
            device_id_type=MESH,
        ).wait_recv()

    def spread(piece):
        for i in far_s:
            send(both, piece, along_src(i))
        for i in far_pair:
            send(both, piece, along_pair(i))

    for i in far_t:
        send(both, own, along_ty(i))
    spread(own)
    send(both, own, across)

    side = []
    for n, i in enumerate(far_s):
        for m, (src, dst) in enumerate(((shift_ref, shifts_ref), (weight_ref, weights_ref))):
            copy = pltpu.make_async_remote_copy(
                src_ref=src,
                dst_ref=dst.at[s],
                send_sem=side_send.at[m, n],
                recv_sem=side_recv.at[m, s],
                device_id=along_src(i),
                device_id_type=MESH,
            )
            copy.start()
            side.append(copy)

    for load in loads[1:]:
        load.wait()
    for plane in range(2):
        all_ref[s, plane, tx, t] = spec_ref[plane]
    block = tx * src_count + s
    blocks = tx_count * src_count
    row_table(row_ref, blend_ref.shape[2] // blocks, block, blocks)
    col_table(col_ref, t)
    mask_ref[...] = pupil_ref[...].astype(jnp.float32).T.astype(jnp.bfloat16)

    def second(j):
        for k in far_s:
            arrive(both, (tx, j, k))
            for i in far_pair:
                send(0, (tx, j, k), along_pair(i))
        for i in far_pair:
            there = 2 * i + core
            arrive(both, (there, j, s))
            for k in far_s:
                send(1, (there, j, s), along_src(k))
        if j is not t:
            send(both, (tx, j, s), across)
        for k in far_s:
            send(both, (tx, j, k), across)
        for i in far_pair:
            send(both, (2 * i + core, j, s), across)

    near_first = [t] + far_t
    for n, j in enumerate(far_t):
        arrive(both, (tx, j, s))
        spread((tx, j, s))
        if n == 0:
            second(t)
    blend_table(blend_ref, block, blocks)
    for j in far_t:
        second(j)
    for j in near_first:
        for i in far_pair:
            for k in far_s:
                for plane in range(2):
                    arrive(plane, (2 * i + core, j, k))
                send(both, (2 * i + core, j, k), across)
    for j in near_first:
        for i in [pair] + far_pair:
            for k in [s] + far_s:
                arrive(both, (2 * i + other_core, j, k))
    for n, i in enumerate(far_s):
        for m, (src, dst) in enumerate(((shift_ref, shifts_ref), (weight_ref, weights_ref))):
            pltpu.make_async_remote_copy(
                src_ref=src,
                dst_ref=dst.at[i],
                send_sem=side_send.at[m, n],
                recv_sem=side_recv.at[m, i],
                device_id=across,
                device_id_type=MESH,
            ).wait_recv()
    for copy in started + side:
        copy.wait_send()


def gather(spectrum, source_shifts, source_weights, pupil_mask, sizes, cols):
    tx_count, ty_count, src_count = sizes
    pair_count = tx_count // 2
    _, block_rows, block_cols = spectrum.shape
    slots = source_weights.shape[0]
    length = pupil_mask.shape[0]
    blocks = tx_count * src_count
    samples = 2 * length
    vmem = pl.BlockSpec(memory_space=pltpu.VMEM)
    lines = pair_count * src_count * ty_count
    sends = ty_count - 1 + lines + ty_count * (src_count - 1 + pair_count - 1)
    sends += 2 * ty_count * (src_count - 1) * (pair_count - 1)
    return pl.pallas_call(
        functools.partial(gather_kernel, sizes),
        out_shape=(
            jax.ShapeDtypeStruct((src_count, 2, tx_count, ty_count, block_rows, block_cols), jnp.bfloat16),
            jax.ShapeDtypeStruct((src_count, 2, slots), jnp.int32),
            jax.ShapeDtypeStruct((src_count, 1, slots), jnp.int32),
            jax.ShapeDtypeStruct((GROUP * length, 2 * LANES), jnp.bfloat16),
            jax.ShapeDtypeStruct((2 * cols, length), jnp.bfloat16),
            jax.ShapeDtypeStruct((length, length), jnp.bfloat16),
            jax.ShapeDtypeStruct((2, FRAME // blocks + 2 * EDGE, samples), jnp.bfloat16),
        ),
        in_specs=[pl.BlockSpec(memory_space=pltpu.HBM)] * 4,
        out_specs=(vmem,) * 7,
        scratch_shapes=[
            pltpu.VMEM(spectrum.shape, jnp.bfloat16),
            pltpu.VMEM(pupil_mask.shape, jnp.int32),
            pltpu.SemaphoreType.DMA((4,)),
            pltpu.SemaphoreType.DMA((sends,)),
            pltpu.SemaphoreType.DMA((2, src_count, tx_count, ty_count)),
            pltpu.SemaphoreType.DMA((2, src_count)),
            pltpu.SemaphoreType.DMA((2, src_count)),
        ],
        compiler_params=pltpu.CompilerParams(collective_id=0, has_side_effects=True, vmem_limit_bytes=12 << 20),
        name="gather",
    )(*(pltpu.with_memory_space_constraint(a, pltpu.HBM) for a in (spectrum, source_shifts.T, source_weights[None], pupil_mask)))


def image_kernel(
    sizes, shifts, weights, spec_ref, mask_ref, row_ref, col_ref, out_ref, strip_ref, spec, acc, folded, inner, live
):
    src_count, _, slots = weights.shape
    source_count = src_count * slots
    length = col_ref.shape[1]
    cols = col_ref.shape[0] // 2
    count_x = out_ref.shape[0]
    height, part = spec_ref.shape[2:]
    tiles = height // LANES
    side = 2 * LANES
    block = lax.axis_index("tx") * src_count + lax.axis_index("src")
    power = lax.rem(block, 4)
    flip = 2 * lax.rem(power, 2)
    middle = (lax.rem(4 - power, 4), power + 1 - 2 * lax.rem(power, 2))

    def pick(turn, count):
        for n in range(unroll):
            i = turn * unroll + n
            group, slot = (n // slots, n % slots) if unroll == source_count else (i // slots, lax.rem(i, slots))
            weight = weights[group, 0, slot]
            live[count + GROUP] = shifts[group, 0, slot] + (shifts[group, 1, slot] << 10) + (weight << 20)
            count = count + jnp.minimum(weight, 1)
        return count

    for g in range(GROUP):
        live[g] = 0
    unroll = min(source_count, 64)
    count = jnp.int32(0)
    if unroll == source_count:
        count = pick(0, count)
    else:
        count = lax.fori_loop(0, source_count // unroll, pick, count)
    for g in range((UNROLL + 1) * GROUP):
        live[count + GROUP + g] = 0

    same = jnp.where(iota((side, side), 0) == iota((side, side), 1), 1.0, 0.0).astype(jnp.bfloat16)
    turned = (((1,), (1,)), ((), ()))
    for plane in range(2):
        for i in range(height // side):
            rows = slice(side * i, side * (i + 1))
            for j in range(src_count * part // side):
                cells = [spec_ref[k, plane, rows] for k in range(side * j // part, -(-side * (j + 1) // part))]
                cell = cells[0] if len(cells) == 1 else jnp.concatenate(cells, axis=1)
                value = lax.dot_general(same, cell, turned, preferred_element_type=jnp.float32)
                for n in range(side // LANES):
                    tile = value[:, n * LANES : (n + 1) * LANES]
                    at = side // LANES * i + n
                    spec[plane * tiles + at, side * j : side * (j + 1)] = tile
                    spec[(plane + 2) * tiles + at, side * j : side * (j + 1)] = -tile

    acc[...] = jnp.zeros_like(acc)
    lane = iota((length, LANES), 1)

    def fold(word, slot, at):
        a, b = word & 1023, (word >> 10) & 1023
        tile, rest = a // LANES, lax.rem(a, LANES)
        rows = pl.ds(b, length)
        keep = lane >= rest
        low = pltpu.roll(mask_ref[:, :LANES], rest, 1)
        high = pltpu.roll(mask_ref[:, LANES:], rest, 1)
        ends = jnp.where(keep, low, high)
        centre = jnp.where(keep, high, low)
        last = jnp.minimum(tile + 2, tiles - 1)
        for plane in range(2):
            outer = jnp.where(keep, spec[plane * tiles + tile, rows, :], spec[(plane + flip) * tiles + last, rows, :]).astype(jnp.bfloat16)
            between = spec[middle[plane] * tiles + tile + 1, rows, :].astype(jnp.bfloat16)
            slot[:, at + plane * LANES : at + (plane + 1) * LANES] = outer * ends + between * centre

    first_half = iota((1, LANES), 1) < LANES // 2

    def step(n, parity):
        for g in range(GROUP):
            fold(live[(n + 2) * GROUP + g], folded[1 - parity], 2 * g * LANES)
        inner[parity][...] = dot(folded[parity][...], row_ref[...]).astype(jnp.bfloat16)
        wide = dot(col_ref[...], inner[1 - parity][...])
        real = wide[:cols, :LANES] - wide[cols:, LANES:]
        imag = wide[:cols, LANES:] + wide[cols:, :LANES]
        pair = [(live[n * GROUP + g] >> 20).astype(jnp.float32) for g in range(GROUP)]
        acc[...] += jnp.where(first_half, pair[0], pair[1]) * (real * real + imag * imag)

    inner[1][...] = jnp.zeros_like(inner[1])
    for g in range(GROUP):
        fold(live[GROUP + g], folded[0], 2 * g * LANES)

    def turn_body(turn_index, carry):
        for g in range(UNROLL):
            step(turn_index * UNROLL + g, g % 2)
        return carry

    steps = (count + GROUP - 1) // GROUP + 1
    lax.fori_loop(0, (steps + UNROLL - 1) // UNROLL, turn_body, 0)
    level = acc[...]
    level = (level + pltpu.roll(level, LANES // 2, 1)) / (2.0 * source_count)
    out_ref[...] = level.T[:count_x].astype(jnp.bfloat16)
    strip_ref[0] = level[:PACK, :count_x].astype(jnp.bfloat16)
    strip_ref[1] = level[cols - PACK :, :count_x].astype(jnp.bfloat16)


def image(spectrum, shifts, weights, row_table, col_table, masks, count_x, sizes):
    source_count = weights.shape[0] * weights.shape[2]
    src_count, _, height, part = spectrum.shape
    cols, length = col_table.shape[0] // 2, col_table.shape[1]
    smem = pl.BlockSpec(memory_space=pltpu.SMEM)
    vmem = pl.BlockSpec(memory_space=pltpu.VMEM)
    return pl.pallas_call(
        functools.partial(image_kernel, sizes),
        out_shape=(
            jax.ShapeDtypeStruct((count_x, cols), jnp.bfloat16),
            jax.ShapeDtypeStruct((2, PACK, count_x), jnp.bfloat16),
        ),
        in_specs=[smem, smem, vmem, vmem, vmem, vmem],
        out_specs=(vmem, vmem),
        scratch_shapes=[
            pltpu.VMEM((4 * height // LANES, src_count * part, LANES), jnp.float32),
            pltpu.VMEM((cols, LANES), jnp.float32),
            [pltpu.VMEM((length, GROUP * 2 * LANES), jnp.bfloat16)] * 2,
            [pltpu.VMEM((length, 2 * LANES), jnp.bfloat16)] * 2,
            pltpu.SMEM((source_count + (UNROLL + 3) * GROUP,), jnp.int32),
        ],
        compiler_params=pltpu.CompilerParams(vmem_limit_bytes=16 << 20),
        name="image",
    )(shifts, weights, spectrum, masks, row_table, col_table)


def exchange_kernel(sizes, own_ref, strip_ref, all_ref, beside, send_sem, recv_sem, side_send, side_recv):
    tx_count, ty_count, src_count = sizes
    pair_count = tx_count // 2
    tx, t, s = lax.axis_index("tx"), lax.axis_index("ty"), lax.axis_index("src")
    pair, core = tx // 2, lax.rem(tx, 2)
    far_s = [s] + others(s, src_count)
    far_pair = [pair] + others(pair, pair_count)
    chips = [(i, k) for k in far_s for i in far_pair]

    def device(chip, other, z):
        return {"tx": 2 * chip[0] + (1 - core if other else core), "ty": z, "src": chip[1]}

    def block(chip, other):
        return (2 * chip[0] + (1 - core if other else core)) * src_count + chip[1]

    across = device(chips[0], True, t)
    barrier = pltpu.get_barrier_semaphore()

    def greet(chip, z):
        pl.semaphore_signal(barrier, inc=1, device_id=device(chip, False, z), device_id_type=MESH)

    has = (t > 0, t < ty_count - 1)
    beside[...] = jnp.zeros_like(beside)
    pl.semaphore_signal(barrier, inc=1, device_id=across, device_id_type=MESH)
    for chip in chips[1:]:
        greet(chip, t)
    for side in range(2):

        @pl.when(has[side])
        def _():
            for chip in chips:
                greet(chip, t + 2 * side - 1)

    all_ref[block(chips[0], False)] = own_ref[...]
    sides = jnp.minimum(t, 1) + jnp.minimum(ty_count - 1 - t, 1)
    pl.semaphore_wait(barrier, len(chips) * (1 + sides))

    def copy(src, dst, send, recv, target):
        return pltpu.make_async_remote_copy(
            src_ref=src, dst_ref=dst, send_sem=send, recv_sem=recv, device_id=target, device_id_type=MESH
        )

    def level_copy(n, chip, other, target, own=False):
        at = block(chip, other)
        return copy(own_ref if own else all_ref.at[at], all_ref.at[at], send_sem.at[n], recv_sem.at[at], target)

    def side_copy(n, side, chip, other, target, own=False):
        at = block(chip, other)
        slot = beside.at[side, at]
        return copy(strip_ref.at[1 - side] if own else slot, slot, side_send.at[side, n], side_recv.at[side, at], target)

    started = []
    for n, chip in enumerate(chips[1:]):
        started.append(level_copy(n, chips[0], False, device(chip, False, t), True))
        started[-1].start()
    for side in range(2):

        @pl.when(has[1 - side])
        def _():
            for n, chip in enumerate(chips):
                side_copy(n, side, chips[0], False, device(chip, False, t + 1 - 2 * side), True).start()

    n = len(chips) - 1
    started.append(level_copy(n, chips[0], False, across, True))
    started[-1].start()
    for chip in chips[1:]:
        n += 1
        level_copy(0, chip, False, across).wait_recv()
        started.append(level_copy(n, chip, False, across))
        started[-1].start()
    for side in range(2):

        @pl.when(has[side])
        def _():
            for n, chip in enumerate(chips):
                side_copy(0, side, chip, False, across).wait_recv()
                side_copy(len(chips) + n, side, chip, False, across).start()

    for chip in chips:
        level_copy(0, chip, True, across).wait_recv()
    for side in range(2):

        @pl.when(has[side])
        def _():
            for n, chip in enumerate(chips):
                side_copy(0, side, chip, True, across).wait_recv()
                side_copy(len(chips) + n, side, chip, False, across).wait_send()

        @pl.when(has[1 - side])
        def _():
            for n, chip in enumerate(chips):
                side_copy(n, side, chips[0], False, device(chip, False, t + 1 - 2 * side), True).wait_send()

    for one in started:
        one.wait_send()


def exchange(level, strips, sizes):
    tx_count, ty_count, src_count = sizes
    blocks = tx_count * src_count
    vmem = pl.BlockSpec(memory_space=pltpu.VMEM)
    return pl.pallas_call(
        functools.partial(exchange_kernel, sizes),
        out_shape=(
            jax.ShapeDtypeStruct((blocks,) + level.shape, level.dtype),
            jax.ShapeDtypeStruct((2, blocks) + strips.shape[1:], strips.dtype),
        ),
        in_specs=[vmem] * 2,
        out_specs=(vmem,) * 2,
        scratch_shapes=[
            pltpu.SemaphoreType.DMA((blocks,)),
            pltpu.SemaphoreType.DMA((blocks,)),
            pltpu.SemaphoreType.DMA((2, blocks)),
            pltpu.SemaphoreType.DMA((2, blocks)),
        ],
        compiler_params=pltpu.CompilerParams(collective_id=1, has_side_effects=True, vmem_limit_bytes=4 << 20),
        name="exchange",
    )(level, strips)


def diffuse_kernel(sizes, all_ref, beside, blend_ref, out_ref):
    tx_count, ty_count, src_count = sizes
    rows, cols = out_ref.shape
    blocks, count, _ = all_ref.shape
    samples = blocks * count
    tall = rows + 2 * EDGE
    level = all_ref[...].reshape(samples, cols)
    sides = [jnp.concatenate([beside[side, n] for n in range(blocks)], axis=1) for side in range(2)]
    strip = jnp.concatenate([sides[1], jnp.zeros((LANES - 2 * PACK, samples), jnp.bfloat16), sides[0]], axis=0)
    turned = (((1,), (1,)), ((), ()))
    middle = dot(blend_ref[0], level) + dot(blend_ref[1], level)
    edge = lax.dot_general(blend_ref[0], strip, turned, preferred_element_type=jnp.float32)
    edge += lax.dot_general(blend_ref[1], strip, turned, preferred_element_type=jnp.float32)
    acid = 1.0 - jnp.exp(-jnp.concatenate([middle, edge], axis=1))
    wide = cols + LANES
    row_block = lax.axis_index("tx") * src_count + lax.axis_index("src")
    col_block = lax.axis_index("ty")
    x = row_block * rows - EDGE + iota(acid.shape, 0)
    column = iota(acid.shape, 1)
    y = col_block * cols + jnp.where(column >= cols + LANES // 2, column - wide, column)
    inside = (x >= 0) & (x < blocks * rows) & (y >= 0) & (y < ty_count * cols)
    for repeat in range(2):
        acid = jnp.where(inside, acid, 0.0)
        near = (
            pltpu.roll(acid, 1, 0)
            + pltpu.roll(acid, tall - 1, 0)
            + pltpu.roll(acid, 1, 1)
            + pltpu.roll(acid, wide - 1, 1)
        )
        acid = acid + diffusion_rate * (near - 4.0 * acid)
    out_ref[...] = acid[EDGE : EDGE + rows, :cols]


def diffuse(levels, beside, blend, sizes):
    rows = blend.shape[1] - 2 * EDGE
    vmem = pl.BlockSpec(memory_space=pltpu.VMEM)
    return pl.pallas_call(
        functools.partial(diffuse_kernel, sizes),
        out_shape=jax.ShapeDtypeStruct((rows, levels.shape[2]), jnp.float32),
        in_specs=[vmem] * 3,
        out_specs=vmem,
        compiler_params=pltpu.CompilerParams(vmem_limit_bytes=12 << 20),
        name="diffuse",
    )(levels, beside, blend)


def body(sizes, cols, spectrum, pupil_mask, source_shifts, source_weights):
    pieces, shifts, weights, row_table, col_table, masks, blend = gather(
        spectrum, source_shifts, source_weights, pupil_mask, sizes, cols
    )
    src_count, _, tx_count, ty_count, block_rows, block_cols = pieces.shape
    columns = pieces.reshape(src_count, 2, tx_count * ty_count * block_rows, block_cols)
    count_x = blend.shape[2] // (tx_count * src_count)
    level, strips = image(columns, shifts, weights, row_table, col_table, masks, count_x, sizes)
    levels, beside = exchange(level, strips, sizes)
    return diffuse(levels, beside, blend, sizes)


def solution(mesh):
    sizes = (mesh.shape["tx"], mesh.shape["ty"], mesh.shape["src"])
    placed = (P(None, ("tx", "ty"), "src"), P(), P("src", None), P("src"))
    return jax.shard_map(
        functools.partial(body, sizes, COLS),
        mesh=mesh,
        in_specs=placed,
        out_specs=P(("tx", "src"), "ty"),
        check_vma=False,
    )
```

```python
import functools
import math

import jax
import jax.numpy as jnp
from jax import lax
from jax.experimental import pallas as pl
from jax.experimental.pallas import tpu as pltpu
from jax.sharding import PartitionSpec as P

FRAME = 2048
LANES = 128
COLS = 256
EDGE = 8
PACK = 16
GROUP = 2
UNROLL = 4
TAIL = 4
MESH = pl.DeviceIdType.MESH

diffusion_rate = 0.2


def wave(turns, period):
    quarter = period // 4
    turn = (turns + quarter // 2) // quarter
    angle = (turns - turn * quarter).astype(jnp.float32) * (2 * math.pi / period)
    square = angle * angle
    sine = angle * (1 + square * (-1 / 6 + square * (1 / 120 + square * (-1 / 5040 + square / 362880))))
    cosine = 1 + square * (-1 / 2 + square * (1 / 24 + square * (-1 / 720 + square / 40320)))
    odd = (turn & 1) == 1
    first, second = jnp.where(odd, sine, cosine), jnp.where(odd, cosine, sine)
    return jnp.where(((turn + 1) & 2) == 2, -first, first), jnp.where((turn & 2) == 2, -second, second)


def iota(shape, dim):
    return lax.broadcasted_iota(jnp.int32, shape, dim)


def dot(a, b):
    return jnp.dot(a, b, preferred_element_type=jnp.float32)


def flip_bits(index, mask):
    bit = 1
    while bit <= mask:
        if mask & bit:
            index = index + bit * (1 - 2 * lax.rem(index // bit, 2))
        bit *= 2
    return index


def others(index, count):
    if count & (count - 1) == 0:
        return [flip_bits(index, d) for d in range(1, count)]
    return [lax.rem(index + d, count) for d in range(1, count)]


def nearest(index, count):
    orders = [sorted((i for i in range(count) if i != at), key=lambda i: (abs(i - at), i)) for at in range(count)]
    return [sum(jnp.where(index == at, orders[at][n], 0) for at in range(count)) for n in range(count - 1)]


def row_table(row_ref, count, block, blocks):
    half = row_ref.shape[0] // (2 * GROUP)
    each = LANES // GROUP
    step = FRAME // (count * blocks)
    sample = iota((half, each), 1)
    x = step * (blocks * sample + block)
    cosine, sine = wave((x * iota((half, each), 0)) & (FRAME - 1), FRAME)
    cosine = jnp.where(sample < count, cosine, 0.0)
    sine = jnp.where(sample < count, sine, 0.0)
    none = jnp.zeros((half, each), jnp.float32)
    for g in range(GROUP):
        for part, (real, imag) in enumerate(((cosine, sine), (-sine, cosine))):
            row = [real if n == g else none for n in range(GROUP)] + [imag if n == g else none for n in range(GROUP)]
            at = (2 * g + part) * half
            row_ref[at : at + half] = jnp.concatenate(row, axis=1).astype(jnp.bfloat16)


def col_table(col_ref, t):
    cols, length = col_ref.shape[0] // 2, col_ref.shape[1]
    chunk = 32

    def fill(n, carry):
        start = pl.multiple_of(n * chunk, chunk)
        y = t * cols + start + iota((chunk, length), 0)
        cosine, sine = wave((y * iota((chunk, length), 1)) & (FRAME - 1), FRAME)
        col_ref[pl.ds(start, chunk)] = cosine.astype(jnp.bfloat16)
        col_ref[pl.ds(cols + start, chunk)] = sine.astype(jnp.bfloat16)
        return carry

    lax.fori_loop(0, cols // chunk, fill, 0)


def blend_table(blend_ref, block, blocks):
    _, tall, samples = blend_ref.shape
    rows = tall - 2 * EDGE
    step = FRAME // samples
    count = samples // blocks
    chunk = PACK

    def fill(n, carry):
        start = pl.multiple_of(n * chunk, chunk)
        x = block * rows - EDGE + start + iota((chunk, samples), 0)
        column = iota((chunk, samples), 1)
        owner = column // count
        gap = x - step * (blocks * (column - owner * count) + owner)
        gap = ((gap + FRAME // 2) & (FRAME - 1)) - FRAME // 2
        cosine, sine = wave(gap, 2 * FRAME)
        place = block * rows - EDGE + start + iota((chunk, 1), 0)
        place = place & (2 * step - 1)
        scale = jnp.zeros((chunk, 1), jnp.float32)
        for n in range(2 * step):
            if n % step:
                scale = jnp.where(place == n, math.sin(math.pi * n / step) / samples, scale)
        scale = jnp.where((owner & 1) == 1, -scale, scale)
        here = gap == 0
        table = jnp.where(here, 1.0, scale * cosine / jnp.where(here, 1.0, sine))
        high = table.astype(jnp.bfloat16)
        blend_ref[0, pl.ds(start, chunk)] = high
        blend_ref[1, pl.ds(start, chunk)] = (table - high.astype(jnp.float32)).astype(jnp.bfloat16)
        return carry

    lax.fori_loop(0, tall // chunk, fill, 0)


def gather_kernel(
    sizes, spec_hbm, shift_ref, weight_ref, pupil_hbm, turned_ref, word_ref, row_ref, col_ref, mask_ref, blend_ref,
    shifts_ref, weights_ref, all_ref, spec_ref, pupil_ref, local_sem, send_sem, recv_sem, side_send, side_recv,
):
    tx_count, ty_count, src_count = sizes
    pair_count = tx_count // 2
    tx, t, s = lax.axis_index("tx"), lax.axis_index("ty"), lax.axis_index("src")
    pair, core = tx // 2, lax.rem(tx, 2)
    other_core = 1 - core
    far_t = nearest(t, ty_count)
    far_s = others(s, src_count)
    far_pair = others(pair, pair_count)

    def along_ty(i):
        return {"tx": tx, "ty": i, "src": s}

    def along_src(i):
        return {"tx": tx, "ty": t, "src": i}

    def along_pair(i):
        return {"tx": 2 * i + core, "ty": t, "src": s}

    loads = [
        pltpu.make_async_copy(src, dst, local_sem.at[n])
        for n, (src, dst) in enumerate(
            (
                (spec_hbm, spec_ref),
                (pupil_hbm, pupil_ref),
                (shift_ref, shifts_ref.at[s]),
                (weight_ref, weights_ref.at[s]),
            )
        )
    ]
    for load in loads:
        load.start()

    across = {"tx": 2 * pair + other_core, "ty": t, "src": s}
    partners = [along_ty(i) for i in far_t] + [along_src(i) for i in far_s]
    partners += [along_pair(i) for i in far_pair] + [across]
    barrier = pltpu.get_barrier_semaphore()
    for partner in partners:
        pl.semaphore_signal(barrier, inc=1, device_id=partner, device_id_type=MESH)
    pl.semaphore_wait(barrier, len(partners))
    loads[0].wait()

    started = []
    own = (tx, t, s)

    both = slice(None)

    def part(plane, piece):
        i, j, k = piece
        return all_ref.at[k, plane, i, j], recv_sem.at[0 if plane is both else plane, k, i, j]

    def send(plane, piece, device):
        slot, arrived = part(plane, piece)
        copy = pltpu.make_async_remote_copy(
            src_ref=spec_ref if piece is own else slot,
            dst_ref=slot,
            send_sem=send_sem.at[len(started)],
            recv_sem=arrived,
            device_id=device,
            device_id_type=MESH,
        )
        copy.start()
        started.append(copy)

    def arrive(plane, piece):
        slot, arrived = part(plane, piece)
        pltpu.make_async_remote_copy(
            src_ref=slot,
            dst_ref=slot,
            send_sem=send_sem.at[0],
            recv_sem=arrived,
            device_id=across,
            device_id_type=MESH,
        ).wait_recv()

    def spread(piece):
        for i in far_s:
            send(both, piece, along_src(i))
        for i in far_pair:
            send(both, piece, along_pair(i))

    for i in far_t:
        send(both, own, along_ty(i))
    spread(own)
    send(both, own, across)

    side = []
    for n, i in enumerate(far_s):
        for m, (src, dst) in enumerate(((shift_ref, shifts_ref), (weight_ref, weights_ref))):
            copy = pltpu.make_async_remote_copy(
                src_ref=src,
                dst_ref=dst.at[s],
                send_sem=side_send.at[m, n],
                recv_sem=side_recv.at[m, s],
                device_id=along_src(i),
                device_id_type=MESH,
            )
            copy.start()
            side.append(copy)

    for load in loads[1:]:
        load.wait()
    for plane in range(2):
        all_ref[s, plane, tx, t] = spec_ref[plane]
    block = tx * src_count + s
    blocks = tx_count * src_count
    row_table(row_ref, blend_ref.shape[2] // blocks, block, blocks)
    col_table(col_ref, t)
    mask_ref[...] = pupil_ref[...].astype(jnp.float32).T.astype(jnp.bfloat16)

    part_rows, part_cols = ty_count * spec_ref.shape[1], spec_ref.shape[2]
    same = jnp.where(iota((part_cols,) * 2, 0) == iota((part_cols,) * 2, 1), 1.0, 0.0).astype(jnp.bfloat16)

    def turn(i, k):
        rows = pl.ds(pl.multiple_of(k * part_cols, part_cols), part_cols)
        for plane in range(2):
            cell = all_ref[k, plane, i].reshape(part_rows, part_cols)
            value = lax.dot_general(same, cell, (((1,), (1,)), ((), ())), preferred_element_type=jnp.float32)
            turned_ref[plane * tx_count + i, rows] = value
            turned_ref[(plane + 2) * tx_count + i, rows] = -value

    def second(j):
        for k in far_s:
            arrive(both, (tx, j, k))
            for i in far_pair:
                send(0, (tx, j, k), along_pair(i))
        for i in far_pair:
            there = 2 * i + core
            arrive(both, (there, j, s))
            for k in far_s:
                send(1, (there, j, s), along_src(k))
        if j is not t:
            send(both, (tx, j, s), across)
        for k in far_s:
            send(both, (tx, j, k), across)
        for i in far_pair:
            send(both, (2 * i + core, j, s), across)

    near_first = [t] + far_t
    for n, j in enumerate(far_t):
        arrive(both, (tx, j, s))
        spread((tx, j, s))
        if n == 0:
            second(t)
    turn(tx, s)
    blend_table(blend_ref, block, blocks)
    for j in far_t:
        second(j)
    for k in far_s:
        turn(tx, k)
    for i in far_pair:
        turn(2 * i + core, s)
    for j in near_first:
        for i in far_pair:
            for k in far_s:
                for plane in range(2):
                    arrive(plane, (2 * i + core, j, k))
                send(both, (2 * i + core, j, k), across)
    for i in far_pair:
        for k in far_s:
            turn(2 * i + core, k)
    for n, i in enumerate(far_s):
        for m, (src, dst) in enumerate(((shift_ref, shifts_ref), (weight_ref, weights_ref))):
            pltpu.make_async_remote_copy(
                src_ref=src,
                dst_ref=dst.at[i],
                send_sem=side_send.at[m, n],
                recv_sem=side_recv.at[m, i],
                device_id=across,
                device_id_type=MESH,
            ).wait_recv()
    word_ref[...] = shifts_ref[:, 0:1] + shifts_ref[:, 1:2] * 1024 + weights_ref[...] * (1 << 20)
    for i in [pair] + far_pair:
        for k in [s] + far_s:
            for j in near_first:
                arrive(both, (2 * i + other_core, j, k))
            turn(2 * i + other_core, k)
    for copy in started + side:
        copy.wait_send()


def gather(spectrum, source_shifts, source_weights, pupil_mask, sizes, cols):
    tx_count, ty_count, src_count = sizes
    pair_count = tx_count // 2
    _, block_rows, block_cols = spectrum.shape
    slots = source_weights.shape[0]
    length = pupil_mask.shape[0]
    blocks = tx_count * src_count
    samples = 2 * length
    vmem = pl.BlockSpec(memory_space=pltpu.VMEM)
    lines = pair_count * src_count * ty_count
    sends = ty_count - 1 + lines + ty_count * (src_count - 1 + pair_count - 1)
    sends += 2 * ty_count * (src_count - 1) * (pair_count - 1)
    return pl.pallas_call(
        functools.partial(gather_kernel, sizes),
        out_shape=(
            jax.ShapeDtypeStruct((4 * tx_count, src_count * block_cols, ty_count * block_rows), jnp.float32),
            jax.ShapeDtypeStruct((src_count, 1, slots), jnp.int32),
            jax.ShapeDtypeStruct((GROUP * length, 2 * LANES), jnp.bfloat16),
            jax.ShapeDtypeStruct((2 * cols, length), jnp.bfloat16),
            jax.ShapeDtypeStruct((length, length), jnp.bfloat16),
            jax.ShapeDtypeStruct((2, FRAME // blocks + 2 * EDGE, samples), jnp.bfloat16),
        ),
        in_specs=[pl.BlockSpec(memory_space=pltpu.HBM)] * 4,
        out_specs=(vmem,) * 6,
        scratch_shapes=[
            pltpu.VMEM((src_count, 2, slots), jnp.int32),
            pltpu.VMEM((src_count, 1, slots), jnp.int32),
            pltpu.VMEM((src_count, 2, tx_count, ty_count, block_rows, block_cols), jnp.bfloat16),
            pltpu.VMEM(spectrum.shape, jnp.bfloat16),
            pltpu.VMEM(pupil_mask.shape, jnp.int32),
            pltpu.SemaphoreType.DMA((4,)),
            pltpu.SemaphoreType.DMA((sends,)),
            pltpu.SemaphoreType.DMA((2, src_count, tx_count, ty_count)),
            pltpu.SemaphoreType.DMA((2, src_count)),
            pltpu.SemaphoreType.DMA((2, src_count)),
        ],
        compiler_params=pltpu.CompilerParams(collective_id=0, has_side_effects=True, vmem_limit_bytes=16 << 20),
        name="gather",
    )(*(pltpu.with_memory_space_constraint(a, pltpu.HBM) for a in (spectrum, source_shifts.T, source_weights[None], pupil_mask)))


def stages(sizes, spec, mask_ref, row_ref, col_ref, live):
    length = col_ref.shape[1]
    cols = col_ref.shape[0] // 2
    tiles = spec.shape[0] // 4
    block = lax.axis_index("tx") * sizes[2] + lax.axis_index("src")
    power = lax.rem(block, 4)
    flip = 2 * lax.rem(power, 2)
    middle = (lax.rem(4 - power, 4), power + 1 - 2 * lax.rem(power, 2))
    lane = iota((length, LANES), 1)
    first_half = iota((1, LANES), 1) < LANES // 2

    def fold(n, slot):
        for g in range(GROUP):
            word = live[(n + 1) * GROUP + g]
            a, b = word & 1023, (word >> 10) & 1023
            tile, rest = a // LANES, lax.rem(a, LANES)
            rows = pl.ds(b, length)
            keep = lane >= rest
            low = pltpu.roll(mask_ref[:, :LANES], rest, 1)
            high = pltpu.roll(mask_ref[:, LANES:], rest, 1)
            ends = jnp.where(keep, low, high)
            centre = jnp.where(keep, high, low)
            last = jnp.minimum(tile + 2, tiles - 1)
            for plane in range(2):
                outer = jnp.where(keep, spec[plane * tiles + tile, rows, :], spec[(plane + flip) * tiles + last, rows, :])
                between = spec[middle[plane] * tiles + tile + 1, rows, :]
                at = (2 * g + plane) * LANES
                slot[:, at : at + LANES] = outer.astype(jnp.bfloat16) * ends + between.astype(jnp.bfloat16) * centre

    def cross(source, slot):
        slot[...] = dot(source[...], row_ref[...]).astype(jnp.bfloat16)

    def square(n, source):
        wide = dot(col_ref[...], source[...])
        real = wide[:cols, :LANES] - wide[cols:, LANES:]
        imag = wide[:cols, LANES:] + wide[cols:, :LANES]
        pair = [(live[(n + 1) * GROUP + g] >> 20).astype(jnp.float32) for g in range(GROUP)]
        return jnp.where(first_half, pair[0], pair[1]) * (real * real + imag * imag)

    return fold, cross, square


def image_kernel(
    sizes, words, spec, mask_ref, row_ref, col_ref, live, acc, next_folded, next_inner, other_folded, other_inner
):
    src_count, _, slots = words.shape
    source_count = src_count * slots

    def pick(turn, count):
        for n in range(unroll):
            i = turn * unroll + n
            group, slot = (n // slots, n % slots) if unroll == source_count else (i // slots, lax.rem(i, slots))
            word = words[group, 0, slot]
            live[count + GROUP] = word
            count = count + jnp.minimum(word >> 20, 1)
        return count

    for g in range(GROUP):
        live[g] = 0
    unroll = min(source_count, 64)
    count = jnp.int32(0)
    if unroll == source_count:
        count = pick(0, count)
    else:
        count = lax.fori_loop(0, source_count // unroll, pick, count)
    for g in range((UNROLL + TAIL) * GROUP):
        live[count + GROUP + g] = 0

    fold, cross, square = stages(sizes, spec, mask_ref, row_ref, col_ref, live)
    folded = (next_folded, other_folded)
    inner = (other_inner, next_inner)
    acc[...] = jnp.zeros_like(acc)
    next_inner[...] = jnp.zeros_like(next_inner)
    fold(0, folded[0])

    def turn_body(turn_index, carry):
        for g in range(UNROLL):
            n = turn_index * UNROLL + g
            fold(n + 1, folded[1 - g % 2])
            cross(folded[g % 2], inner[g % 2])
            acc[...] += square(n - 1, inner[1 - g % 2])
        return carry

    steps = (count + GROUP - 1) // GROUP + 1 - TAIL
    turns = jnp.maximum(steps + UNROLL - 1, 0) // UNROLL
    live[live.shape[0] - 1] = turns * UNROLL
    lax.fori_loop(0, turns, turn_body, 0)


def image(spectrum, words, row_table, col_table, masks, sizes):
    source_count = words.shape[0] * words.shape[2]
    cols, length = col_table.shape[0] // 2, col_table.shape[1]
    smem = pl.BlockSpec(memory_space=pltpu.SMEM)
    vmem = pl.BlockSpec(memory_space=pltpu.VMEM)
    return pl.pallas_call(
        functools.partial(image_kernel, sizes),
        out_shape=(
            jax.ShapeDtypeStruct((source_count + (UNROLL + TAIL + 2) * GROUP,), jnp.int32),
            jax.ShapeDtypeStruct((cols, LANES), jnp.float32),
            jax.ShapeDtypeStruct((length, GROUP * 2 * LANES), jnp.bfloat16),
            jax.ShapeDtypeStruct((length, 2 * LANES), jnp.bfloat16),
        ),
        in_specs=[smem, vmem, vmem, vmem, vmem],
        out_specs=(smem, vmem, vmem, vmem),
        scratch_shapes=[
            pltpu.VMEM((length, GROUP * 2 * LANES), jnp.bfloat16),
            pltpu.VMEM((length, 2 * LANES), jnp.bfloat16),
        ],
        compiler_params=pltpu.CompilerParams(vmem_limit_bytes=12 << 20),
        name="image",
    )(words, spectrum, masks, row_table, col_table)


def exchange_kernel(
    sizes, live_ref, acc, first_folded, first_inner, spec, mask_ref, row_ref, col_ref, all_ref, beside,
    live, own_ref, strip_ref, folded, inner, live_sem, send_sem, recv_sem, side_send, side_recv,
):
    tx_count, ty_count, src_count = sizes
    pair_count = tx_count // 2
    tx, t, s = lax.axis_index("tx"), lax.axis_index("ty"), lax.axis_index("src")
    pair, core = tx // 2, lax.rem(tx, 2)
    far_s = [s] + others(s, src_count)
    far_pair = [pair] + others(pair, pair_count)
    chips = [(i, k) for k in far_s for i in far_pair]

    def device(chip, other, z):
        return {"tx": 2 * chip[0] + (1 - core if other else core), "ty": z, "src": chip[1]}

    def block(chip, other):
        return (2 * chip[0] + (1 - core if other else core)) * src_count + chip[1]

    across = device(chips[0], True, t)
    barrier = pltpu.get_barrier_semaphore()

    def greet(chip, z):
        pl.semaphore_signal(barrier, inc=1, device_id=device(chip, False, z), device_id_type=MESH)

    load = pltpu.make_async_copy(live_ref, live, live_sem)
    load.start()
    has = (t > 0, t < ty_count - 1)
    beside[...] = jnp.zeros_like(beside)
    pl.semaphore_signal(barrier, inc=1, device_id=across, device_id_type=MESH)
    for chip in chips[1:]:
        greet(chip, t)
    for side in range(2):

        @pl.when(has[side])
        def _():
            for chip in chips:
                greet(chip, t + 2 * side - 1)

    fold, cross, square = stages(sizes, spec, mask_ref, row_ref, col_ref, live)
    load.wait()
    n = live[live.shape[0] - 1]
    level = acc[...]
    source_folded, source_inner = first_folded, first_inner
    for g in range(TAIL):
        if g < TAIL - 2:
            fold(n + g + 1, folded[g % 2])
        if g < TAIL - 1:
            cross(source_folded, inner[g % 2])
        level += square(n + g - 1, source_inner)
        source_folded, source_inner = folded[g % 2], inner[g % 2]

    cols = level.shape[0]
    count_x = own_ref.shape[0]
    level = (level + pltpu.roll(level, LANES // 2, 1)) / (2.0 * (live.shape[0] - (UNROLL + TAIL + 2) * GROUP))
    own = level.T[:count_x].astype(jnp.bfloat16)
    own_ref[...] = own
    strip_ref[0] = level[:PACK, :count_x].astype(jnp.bfloat16)
    strip_ref[1] = level[cols - PACK :, :count_x].astype(jnp.bfloat16)
    all_ref[block(chips[0], False)] = own
    sides = jnp.minimum(t, 1) + jnp.minimum(ty_count - 1 - t, 1)
    pl.semaphore_wait(barrier, len(chips) * (1 + sides))

    def copy(src, dst, send, recv, target):
        return pltpu.make_async_remote_copy(
            src_ref=src, dst_ref=dst, send_sem=send, recv_sem=recv, device_id=target, device_id_type=MESH
        )

    def level_copy(n, chip, other, target, own=False):
        at = block(chip, other)
        return copy(own_ref if own else all_ref.at[at], all_ref.at[at], send_sem.at[n], recv_sem.at[at], target)

    def side_copy(n, side, chip, other, target, own=False):
        at = block(chip, other)
        slot = beside.at[side, at]
        return copy(strip_ref.at[1 - side] if own else slot, slot, side_send.at[side, n], side_recv.at[side, at], target)

    started = []
    for n, chip in enumerate(chips[1:]):
        started.append(level_copy(n, chips[0], False, device(chip, False, t), True))
        started[-1].start()
    for side in range(2):

        @pl.when(has[1 - side])
        def _():
            for n, chip in enumerate(chips):
                side_copy(n, side, chips[0], False, device(chip, False, t + 1 - 2 * side), True).start()

    n = len(chips) - 1
    started.append(level_copy(n, chips[0], False, across, True))
    started[-1].start()
    for chip in chips[1:]:
        n += 1
        level_copy(0, chip, False, across).wait_recv()
        started.append(level_copy(n, chip, False, across))
        started[-1].start()
    for side in range(2):

        @pl.when(has[side])
        def _():
            for n, chip in enumerate(chips):
                side_copy(0, side, chip, False, across).wait_recv()
                side_copy(len(chips) + n, side, chip, False, across).start()

    for chip in chips:
        level_copy(0, chip, True, across).wait_recv()
    for side in range(2):

        @pl.when(has[side])
        def _():
            for n, chip in enumerate(chips):
                side_copy(0, side, chip, True, across).wait_recv()
                side_copy(len(chips) + n, side, chip, False, across).wait_send()

        @pl.when(has[1 - side])
        def _():
            for n, chip in enumerate(chips):
                side_copy(n, side, chips[0], False, device(chip, False, t + 1 - 2 * side), True).wait_send()

    for one in started:
        one.wait_send()


def exchange(live, acc, folded, inner, spectrum, masks, row_table, col_table, count_x, sizes):
    tx_count, ty_count, src_count = sizes
    blocks = tx_count * src_count
    vmem = pl.BlockSpec(memory_space=pltpu.VMEM)
    cols = acc.shape[0]
    return pl.pallas_call(
        functools.partial(exchange_kernel, sizes),
        out_shape=(
            jax.ShapeDtypeStruct((blocks, count_x, cols), jnp.bfloat16),
            jax.ShapeDtypeStruct((2, blocks, PACK, count_x), jnp.bfloat16),
        ),
        in_specs=[vmem] * 8,
        out_specs=(vmem,) * 2,
        scratch_shapes=[
            pltpu.SMEM(live.shape, jnp.int32),
            pltpu.VMEM((count_x, cols), jnp.bfloat16),
            pltpu.VMEM((2, PACK, count_x), jnp.bfloat16),
            [pltpu.VMEM(folded.shape, jnp.bfloat16)] * 2,
            [pltpu.VMEM(inner.shape, jnp.bfloat16)] * 2,
            pltpu.SemaphoreType.DMA(()),
            pltpu.SemaphoreType.DMA((blocks,)),
            pltpu.SemaphoreType.DMA((blocks,)),
            pltpu.SemaphoreType.DMA((2, blocks)),
            pltpu.SemaphoreType.DMA((2, blocks)),
        ],
        compiler_params=pltpu.CompilerParams(collective_id=1, has_side_effects=True, vmem_limit_bytes=12 << 20),
        name="exchange",
    )(live, acc, folded, inner, spectrum, masks, row_table, col_table)


def diffuse_kernel(sizes, all_ref, beside, blend_ref, out_ref):
    tx_count, ty_count, src_count = sizes
    rows, cols = out_ref.shape
    blocks, count, _ = all_ref.shape
    samples = blocks * count
    tall = rows + 2 * EDGE
    level = all_ref[...].reshape(samples, cols)
    sides = [jnp.concatenate([beside[side, n] for n in range(blocks)], axis=1) for side in range(2)]
    strip = jnp.concatenate([sides[1], jnp.zeros((LANES - 2 * PACK, samples), jnp.bfloat16), sides[0]], axis=0)
    turned = (((1,), (1,)), ((), ()))
    middle = dot(blend_ref[0], level) + dot(blend_ref[1], level)
    edge = lax.dot_general(blend_ref[0], strip, turned, preferred_element_type=jnp.float32)
    edge += lax.dot_general(blend_ref[1], strip, turned, preferred_element_type=jnp.float32)
    acid = 1.0 - jnp.exp(-jnp.concatenate([middle, edge], axis=1))
    wide = cols + LANES
    row_block = lax.axis_index("tx") * src_count + lax.axis_index("src")
    col_block = lax.axis_index("ty")
    x = row_block * rows - EDGE + iota(acid.shape, 0)
    column = iota(acid.shape, 1)
    y = col_block * cols + jnp.where(column >= cols + LANES // 2, column - wide, column)
    inside = (x >= 0) & (x < blocks * rows) & (y >= 0) & (y < ty_count * cols)
    for repeat in range(2):
        acid = jnp.where(inside, acid, 0.0)
        near = (
            pltpu.roll(acid, 1, 0)
            + pltpu.roll(acid, tall - 1, 0)
            + pltpu.roll(acid, 1, 1)
            + pltpu.roll(acid, wide - 1, 1)
        )
        acid = acid + diffusion_rate * (near - 4.0 * acid)
    out_ref[...] = acid[EDGE : EDGE + rows, :cols]


def diffuse(levels, beside, blend, sizes):
    rows = blend.shape[1] - 2 * EDGE
    vmem = pl.BlockSpec(memory_space=pltpu.VMEM)
    return pl.pallas_call(
        functools.partial(diffuse_kernel, sizes),
        out_shape=jax.ShapeDtypeStruct((rows, levels.shape[2]), jnp.float32),
        in_specs=[vmem] * 3,
        out_specs=vmem,
        compiler_params=pltpu.CompilerParams(vmem_limit_bytes=12 << 20),
        name="diffuse",
    )(levels, beside, blend)


def body(sizes, cols, spectrum, pupil_mask, source_shifts, source_weights):
    turned, words, row_table, col_table, masks, blend = gather(
        spectrum, source_shifts, source_weights, pupil_mask, sizes, cols
    )
    count_x = blend.shape[2] // (sizes[0] * sizes[2])
    live, acc, folded, inner = image(turned, words, row_table, col_table, masks, sizes)
    levels, beside = exchange(live, acc, folded, inner, turned, masks, row_table, col_table, count_x, sizes)
    return diffuse(levels, beside, blend, sizes)


def solution(mesh):
    sizes = (mesh.shape["tx"], mesh.shape["ty"], mesh.shape["src"])
    placed = (P(None, ("tx", "ty"), "src"), P(), P("src", None), P("src"))
    return jax.shard_map(
        functools.partial(body, sizes, COLS),
        mesh=mesh,
        in_specs=placed,
        out_specs=P(("tx", "src"), "ty"),
        check_vma=False,
    )
```

```python
import functools
import math

import jax
import jax.numpy as jnp
from jax import lax
from jax.experimental import pallas as pl
from jax.experimental.pallas import tpu as pltpu
from jax.sharding import PartitionSpec as P

FRAME = 2048
LANES = 128
COLS = 256
EDGE = 8
PACK = 16
GROUP = 2
UNROLL = 4
TAIL = 8
MESH = pl.DeviceIdType.MESH

diffusion_rate = 0.2


def wave(turns, period):
    quarter = period // 4
    turn = (turns + quarter // 2) // quarter
    angle = (turns - turn * quarter).astype(jnp.float32) * (2 * math.pi / period)
    square = angle * angle
    sine = angle * (1 + square * (-1 / 6 + square * (1 / 120 + square * (-1 / 5040 + square / 362880))))
    cosine = 1 + square * (-1 / 2 + square * (1 / 24 + square * (-1 / 720 + square / 40320)))
    odd = (turn & 1) == 1
    first, second = jnp.where(odd, sine, cosine), jnp.where(odd, cosine, sine)
    return jnp.where(((turn + 1) & 2) == 2, -first, first), jnp.where((turn & 2) == 2, -second, second)


def iota(shape, dim):
    return lax.broadcasted_iota(jnp.int32, shape, dim)


def dot(a, b):
    return jnp.dot(a, b, preferred_element_type=jnp.float32)


def flip_bits(index, mask):
    bit = 1
    while bit <= mask:
        if mask & bit:
            index = index + bit * (1 - 2 * lax.rem(index // bit, 2))
        bit *= 2
    return index


def others(index, count):
    if count & (count - 1) == 0:
        return [flip_bits(index, d) for d in range(1, count)]
    return [lax.rem(index + d, count) for d in range(1, count)]


def mates(index, count):
    orders = [
        sorted((i for i in range(count) if i != at), key=lambda i: (i != at ^ 1, abs(i - at), i)) for at in range(count)
    ]
    return [sum(jnp.where(index == at, orders[at][n], 0) for at in range(count)) for n in range(count - 1)]


def row_table(row_ref, count, block, blocks):
    half = row_ref.shape[0] // (2 * GROUP)
    each = LANES // GROUP
    step = FRAME // (count * blocks)
    sample = iota((half, each), 1)
    x = step * (blocks * sample + block)
    cosine, sine = wave((x * iota((half, each), 0)) & (FRAME - 1), FRAME)
    cosine = jnp.where(sample < count, cosine, 0.0)
    sine = jnp.where(sample < count, sine, 0.0)
    none = jnp.zeros((half, each), jnp.float32)
    for g in range(GROUP):
        for part, (real, imag) in enumerate(((cosine, sine), (-sine, cosine))):
            row = [real if n == g else none for n in range(GROUP)] + [imag if n == g else none for n in range(GROUP)]
            at = (2 * g + part) * half
            row_ref[at : at + half] = jnp.concatenate(row, axis=1).astype(jnp.bfloat16)


def col_table(col_ref, t):
    cols, length = col_ref.shape[0] // 2, col_ref.shape[1]
    chunk = 32

    def fill(n, carry):
        start = pl.multiple_of(n * chunk, chunk)
        y = t * cols + start + iota((chunk, length), 0)
        cosine, sine = wave((y * iota((chunk, length), 1)) & (FRAME - 1), FRAME)
        col_ref[pl.ds(start, chunk)] = cosine.astype(jnp.bfloat16)
        col_ref[pl.ds(cols + start, chunk)] = sine.astype(jnp.bfloat16)
        return carry

    lax.fori_loop(0, cols // chunk, fill, 0)


def blend_table(blend_ref, block, blocks):
    _, tall, samples = blend_ref.shape
    rows = tall - 2 * EDGE
    step = FRAME // samples
    count = samples // blocks
    chunk = PACK

    def fill(n, carry):
        start = pl.multiple_of(n * chunk, chunk)
        x = block * rows - EDGE + start + iota((chunk, samples), 0)
        column = iota((chunk, samples), 1)
        owner = column // count
        gap = x - step * (blocks * (column - owner * count) + owner)
        gap = ((gap + FRAME // 2) & (FRAME - 1)) - FRAME // 2
        cosine, sine = wave(gap, 2 * FRAME)
        place = block * rows - EDGE + start + iota((chunk, 1), 0)
        place = place & (2 * step - 1)
        scale = jnp.zeros((chunk, 1), jnp.float32)
        for n in range(2 * step):
            if n % step:
                scale = jnp.where(place == n, math.sin(math.pi * n / step) / samples, scale)
        scale = jnp.where((owner & 1) == 1, -scale, scale)
        here = gap == 0
        table = jnp.where(here, 1.0, scale * cosine / jnp.where(here, 1.0, sine))
        high = table.astype(jnp.bfloat16)
        blend_ref[0, pl.ds(start, chunk)] = high
        blend_ref[1, pl.ds(start, chunk)] = (table - high.astype(jnp.float32)).astype(jnp.bfloat16)
        return carry

    lax.fori_loop(0, tall // chunk, fill, 0)


def gather_kernel(
    sizes, spec_hbm, shift_ref, weight_ref, pupil_hbm, turned_ref, word_ref, row_ref, col_ref, mask_ref, blend_ref,
    shifts_ref, weights_ref, all_ref, spec_ref, pupil_ref, local_sem, send_sem, recv_sem, side_send, side_recv,
):
    tx_count, ty_count, src_count = sizes
    pair_count = tx_count // 2
    tx, t, s = lax.axis_index("tx"), lax.axis_index("ty"), lax.axis_index("src")
    pair, core = tx // 2, lax.rem(tx, 2)
    other_core = 1 - core
    far_t = mates(t, ty_count)
    far_s = others(s, src_count)
    far_pair = others(pair, pair_count)

    def along_ty(i):
        return {"tx": tx, "ty": i, "src": s}

    def along_src(i):
        return {"tx": tx, "ty": t, "src": i}

    loads = [
        pltpu.make_async_copy(src, dst, local_sem.at[n])
        for n, (src, dst) in enumerate(
            (
                (spec_hbm, spec_ref),
                (pupil_hbm, pupil_ref),
                (shift_ref, shifts_ref.at[s]),
                (weight_ref, weights_ref.at[s]),
            )
        )
    ]
    for load in loads:
        load.start()

    across = {"tx": 2 * pair + other_core, "ty": t, "src": s}
    hood = [(i, k) for k in far_s + [s] for i in far_pair + [pair] if i is not pair or k is not s]
    partners = [along_ty(i) for i in far_t] + [{"tx": 2 * i + core, "ty": t, "src": k} for i, k in hood] + [across]
    barrier = pltpu.get_barrier_semaphore()
    for partner in partners:
        pl.semaphore_signal(barrier, inc=1, device_id=partner, device_id_type=MESH)
    pl.semaphore_wait(barrier, len(partners))
    loads[0].wait()

    started = []
    own = (tx, t, s)

    both = slice(None)

    def part(plane, piece):
        i, j, k = piece
        return all_ref.at[k, plane, i, j], recv_sem.at[0, k, i, j]

    def send(plane, piece, device):
        slot, arrived = part(plane, piece)
        copy = pltpu.make_async_remote_copy(
            src_ref=spec_ref if piece is own else slot,
            dst_ref=slot,
            send_sem=send_sem.at[len(started)],
            recv_sem=arrived,
            device_id=device,
            device_id_type=MESH,
        )
        copy.start()
        started.append(copy)

    def arrive(plane, piece):
        slot, arrived = part(plane, piece)
        pltpu.make_async_remote_copy(
            src_ref=slot,
            dst_ref=slot,
            send_sem=send_sem.at[0],
            recv_sem=arrived,
            device_id=across,
            device_id_type=MESH,
        ).wait_recv()

    def spread(piece):
        for i, k in hood:
            send(both, piece, {"tx": 2 * i + core, "ty": t, "src": k})

    for j in far_t:
        send(both, own, along_ty(j))
    spread(own)
    send(both, own, across)

    side = []
    for n, i in enumerate(far_s):
        for m, (src, dst) in enumerate(((shift_ref, shifts_ref), (weight_ref, weights_ref))):
            copy = pltpu.make_async_remote_copy(
                src_ref=src,
                dst_ref=dst.at[s],
                send_sem=side_send.at[m, n],
                recv_sem=side_recv.at[m, s],
                device_id=along_src(i),
                device_id_type=MESH,
            )
            copy.start()
            side.append(copy)

    for load in loads[1:]:
        load.wait()
    for plane in range(2):
        all_ref[s, plane, tx, t] = spec_ref[plane]
    block = tx * src_count + s
    blocks = tx_count * src_count
    row_table(row_ref, blend_ref.shape[2] // blocks, block, blocks)
    col_table(col_ref, t)
    mask_ref[...] = pupil_ref[...].astype(jnp.float32).T.astype(jnp.bfloat16)

    part_rows, part_cols = ty_count * spec_ref.shape[1], spec_ref.shape[2]
    same = jnp.where(iota((part_cols,) * 2, 0) == iota((part_cols,) * 2, 1), 1.0, 0.0).astype(jnp.bfloat16)

    def turn(i, k):
        rows = pl.ds(pl.multiple_of(k * part_cols, part_cols), part_cols)
        for plane in range(2):
            cell = all_ref[k, plane, i].reshape(part_rows, part_cols)
            value = lax.dot_general(same, cell, (((1,), (1,)), ((), ())), preferred_element_type=jnp.float32)
            turned_ref[plane * tx_count + i, rows] = value
            turned_ref[(plane + 2) * tx_count + i, rows] = -value

    def pass_on(i, j, k, also=None):
        piece = (2 * i + core, j, k)
        arrive(both, piece)
        if also is not None:
            send(both, piece, along_ty(also))
        send(both, piece, across)

    mate, far_t = far_t[0], far_t[1:]
    near, distant = hood[1:], hood[:1]
    for i, k in near:
        pass_on(i, t, k, mate)
    for n, j in enumerate(far_t):
        arrive(both, (tx, j, s))
        spread((tx, j, s))
        if n == 0:
            for i, k in distant:
                pass_on(i, t, k, mate)
    for j in [mate] + far_t:
        if j is mate:
            arrive(both, (tx, j, s))
        send(both, (tx, j, s), across)
    turn(tx, s)
    blend_table(blend_ref, block, blocks)
    for i, k in near + distant:
        pass_on(i, mate, k)
    for j in far_t:
        for i, k in near + distant:
            pass_on(i, j, k)
    for i, k in near + distant:
        turn(2 * i + core, k)
    near_first = [t, mate] + far_t
    for n, i in enumerate(far_s):
        for m, (src, dst) in enumerate(((shift_ref, shifts_ref), (weight_ref, weights_ref))):
            pltpu.make_async_remote_copy(
                src_ref=src,
                dst_ref=dst.at[i],
                send_sem=side_send.at[m, n],
                recv_sem=side_recv.at[m, i],
                device_id=across,
                device_id_type=MESH,
            ).wait_recv()
    word_ref[...] = shifts_ref[:, 0:1] + shifts_ref[:, 1:2] * 1024 + weights_ref[...] * (1 << 20)
    for i in [pair] + far_pair:
        for k in [s] + far_s:
            for j in near_first:
                arrive(both, (2 * i + other_core, j, k))
            turn(2 * i + other_core, k)
    for copy in started + side:
        copy.wait_send()


def gather(spectrum, source_shifts, source_weights, pupil_mask, sizes, cols):
    tx_count, ty_count, src_count = sizes
    pair_count = tx_count // 2
    _, block_rows, block_cols = spectrum.shape
    slots = source_weights.shape[0]
    length = pupil_mask.shape[0]
    blocks = tx_count * src_count
    samples = 2 * length
    vmem = pl.BlockSpec(memory_space=pltpu.VMEM)
    lines = pair_count * src_count * ty_count
    sends = ty_count - 1 + lines + ty_count * (src_count - 1 + pair_count - 1)
    sends += 3 * ty_count * (src_count - 1) * (pair_count - 1)
    return pl.pallas_call(
        functools.partial(gather_kernel, sizes),
        out_shape=(
            jax.ShapeDtypeStruct((4 * tx_count, src_count * block_cols, ty_count * block_rows), jnp.float32),
            jax.ShapeDtypeStruct((src_count, 1, slots), jnp.int32),
            jax.ShapeDtypeStruct((GROUP * length, 2 * LANES), jnp.bfloat16),
            jax.ShapeDtypeStruct((2 * cols, length), jnp.bfloat16),
            jax.ShapeDtypeStruct((length, length), jnp.bfloat16),
            jax.ShapeDtypeStruct((2, FRAME // blocks + 2 * EDGE, samples), jnp.bfloat16),
        ),
        in_specs=[pl.BlockSpec(memory_space=pltpu.HBM)] * 4,
        out_specs=(vmem,) * 6,
        scratch_shapes=[
            pltpu.VMEM((src_count, 2, slots), jnp.int32),
            pltpu.VMEM((src_count, 1, slots), jnp.int32),
            pltpu.VMEM((src_count, 2, tx_count, ty_count, block_rows, block_cols), jnp.bfloat16),
            pltpu.VMEM(spectrum.shape, jnp.bfloat16),
            pltpu.VMEM(pupil_mask.shape, jnp.int32),
            pltpu.SemaphoreType.DMA((4,)),
            pltpu.SemaphoreType.DMA((sends,)),
            pltpu.SemaphoreType.DMA((2, src_count, tx_count, ty_count)),
            pltpu.SemaphoreType.DMA((2, src_count)),
            pltpu.SemaphoreType.DMA((2, src_count)),
        ],
        compiler_params=pltpu.CompilerParams(collective_id=0, has_side_effects=True, vmem_limit_bytes=16 << 20),
        name="gather",
    )(*(pltpu.with_memory_space_constraint(a, pltpu.HBM) for a in (spectrum, source_shifts.T, source_weights[None], pupil_mask)))


def stages(sizes, spec, mask_ref, row_ref, col_ref, live):
    length = col_ref.shape[1]
    cols = col_ref.shape[0] // 2
    tiles = spec.shape[0] // 4
    block = lax.axis_index("tx") * sizes[2] + lax.axis_index("src")
    power = lax.rem(block, 4)
    flip = 2 * lax.rem(power, 2)
    middle = (lax.rem(4 - power, 4), power + 1 - 2 * lax.rem(power, 2))
    lane = iota((length, LANES), 1)
    first_half = iota((1, LANES), 1) < LANES // 2

    def fold(n, slot):
        for g in range(GROUP):
            word = live[(n + 1) * GROUP + g]
            a, b = word & 1023, (word >> 10) & 1023
            tile, rest = a // LANES, lax.rem(a, LANES)
            rows = pl.ds(b, length)
            keep = lane >= rest
            low = pltpu.roll(mask_ref[:, :LANES], rest, 1)
            high = pltpu.roll(mask_ref[:, LANES:], rest, 1)
            ends = jnp.where(keep, low, high)
            centre = jnp.where(keep, high, low)
            last = jnp.minimum(tile + 2, tiles - 1)
            for plane in range(2):
                outer = jnp.where(keep, spec[plane * tiles + tile, rows, :], spec[(plane + flip) * tiles + last, rows, :])
                between = spec[middle[plane] * tiles + tile + 1, rows, :]
                at = (2 * g + plane) * LANES
                slot[:, at : at + LANES] = outer.astype(jnp.bfloat16) * ends + between.astype(jnp.bfloat16) * centre

    def cross(source, slot):
        slot[...] = dot(source[...], row_ref[...]).astype(jnp.bfloat16)

    def square(n, source):
        wide = dot(col_ref[...], source[...])
        real = wide[:cols, :LANES] - wide[cols:, LANES:]
        imag = wide[:cols, LANES:] + wide[cols:, :LANES]
        pair = [(live[(n + 1) * GROUP + g] >> 20).astype(jnp.float32) for g in range(GROUP)]
        return jnp.where(first_half, pair[0], pair[1]) * (real * real + imag * imag)

    return fold, cross, square


def image_kernel(
    sizes, words, spec, mask_ref, row_ref, col_ref, live, acc, next_folded, next_inner, other_folded, other_inner
):
    src_count, _, slots = words.shape
    source_count = src_count * slots

    def pick(turn, count):
        for n in range(unroll):
            i = turn * unroll + n
            group, slot = (n // slots, n % slots) if unroll == source_count else (i // slots, lax.rem(i, slots))
            word = words[group, 0, slot]
            live[count + GROUP] = word
            count = count + jnp.minimum(word >> 20, 1)
        return count

    for g in range(GROUP):
        live[g] = 0
    unroll = min(source_count, 64)
    count = jnp.int32(0)
    if unroll == source_count:
        count = pick(0, count)
    else:
        count = lax.fori_loop(0, source_count // unroll, pick, count)
    for g in range((UNROLL + TAIL) * GROUP):
        live[count + GROUP + g] = 0

    fold, cross, square = stages(sizes, spec, mask_ref, row_ref, col_ref, live)
    folded = (next_folded, other_folded)
    inner = (other_inner, next_inner)
    acc[...] = jnp.zeros_like(acc)
    next_inner[...] = jnp.zeros_like(next_inner)
    fold(0, folded[0])

    def turn_body(turn_index, carry):
        for g in range(UNROLL):
            n = turn_index * UNROLL + g
            fold(n + 1, folded[1 - g % 2])
            cross(folded[g % 2], inner[g % 2])
            acc[...] += square(n - 1, inner[1 - g % 2])
        return carry

    steps = (count + GROUP - 1) // GROUP + 1 - TAIL
    turns = jnp.maximum(steps + UNROLL - 1, 0) // UNROLL
    live[live.shape[0] - 1] = turns * UNROLL
    lax.fori_loop(0, turns, turn_body, 0)


def image(spectrum, words, row_table, col_table, masks, sizes):
    source_count = words.shape[0] * words.shape[2]
    cols, length = col_table.shape[0] // 2, col_table.shape[1]
    smem = pl.BlockSpec(memory_space=pltpu.SMEM)
    vmem = pl.BlockSpec(memory_space=pltpu.VMEM)
    return pl.pallas_call(
        functools.partial(image_kernel, sizes),
        out_shape=(
            jax.ShapeDtypeStruct((source_count + (UNROLL + TAIL + 2) * GROUP,), jnp.int32),
            jax.ShapeDtypeStruct((cols, LANES), jnp.float32),
            jax.ShapeDtypeStruct((length, GROUP * 2 * LANES), jnp.bfloat16),
            jax.ShapeDtypeStruct((length, 2 * LANES), jnp.bfloat16),
        ),
        in_specs=[smem, vmem, vmem, vmem, vmem],
        out_specs=(smem, vmem, vmem, vmem),
        scratch_shapes=[
            pltpu.VMEM((length, GROUP * 2 * LANES), jnp.bfloat16),
            pltpu.VMEM((length, 2 * LANES), jnp.bfloat16),
        ],
        compiler_params=pltpu.CompilerParams(vmem_limit_bytes=12 << 20),
        name="image",
    )(words, spectrum, masks, row_table, col_table)


def exchange_kernel(
    sizes, live_ref, acc, first_folded, first_inner, spec, mask_ref, row_ref, col_ref, all_ref, beside,
    live, own_ref, strip_ref, folded, inner, live_sem, send_sem, recv_sem, side_send, side_recv,
):
    tx_count, ty_count, src_count = sizes
    pair_count = tx_count // 2
    tx, t, s = lax.axis_index("tx"), lax.axis_index("ty"), lax.axis_index("src")
    pair, core = tx // 2, lax.rem(tx, 2)
    far_s = [s] + others(s, src_count)
    far_pair = [pair] + others(pair, pair_count)
    chips = [(i, k) for k in far_s for i in far_pair]

    def device(chip, other, z):
        return {"tx": 2 * chip[0] + (1 - core if other else core), "ty": z, "src": chip[1]}

    def block(chip, other):
        return (2 * chip[0] + (1 - core if other else core)) * src_count + chip[1]

    across = device(chips[0], True, t)
    barrier = pltpu.get_barrier_semaphore()

    def greet(chip, z):
        pl.semaphore_signal(barrier, inc=1, device_id=device(chip, False, z), device_id_type=MESH)

    load = pltpu.make_async_copy(live_ref, live, live_sem)
    load.start()
    has = (t > 0, t < ty_count - 1)
    beside[...] = jnp.zeros_like(beside)
    pl.semaphore_signal(barrier, inc=1, device_id=across, device_id_type=MESH)
    for chip in chips[1:]:
        greet(chip, t)
    for side in range(2):

        @pl.when(has[side])
        def _():
            for chip in chips:
                greet(chip, t + 2 * side - 1)

    fold, cross, square = stages(sizes, spec, mask_ref, row_ref, col_ref, live)
    load.wait()
    n = live[live.shape[0] - 1]
    level = acc[...]
    source_folded, source_inner = first_folded, first_inner
    for g in range(TAIL):
        if g < TAIL - 2:
            fold(n + g + 1, folded[g % 2])
        if g < TAIL - 1:
            cross(source_folded, inner[g % 2])
        level += square(n + g - 1, source_inner)
        source_folded, source_inner = folded[g % 2], inner[g % 2]

    cols = level.shape[0]
    count_x = own_ref.shape[0]
    level = (level + pltpu.roll(level, LANES // 2, 1)) / (2.0 * (live.shape[0] - (UNROLL + TAIL + 2) * GROUP))
    own = level.T[:count_x].astype(jnp.bfloat16)
    own_ref[...] = own
    strip_ref[0] = level[:PACK, :count_x].astype(jnp.bfloat16)
    strip_ref[1] = level[cols - PACK :, :count_x].astype(jnp.bfloat16)
    all_ref[block(chips[0], False)] = own
    sides = jnp.minimum(t, 1) + jnp.minimum(ty_count - 1 - t, 1)
    pl.semaphore_wait(barrier, len(chips) * (1 + sides))

    def copy(src, dst, send, recv, target):
        return pltpu.make_async_remote_copy(
            src_ref=src, dst_ref=dst, send_sem=send, recv_sem=recv, device_id=target, device_id_type=MESH
        )

    def level_copy(n, chip, other, target, own=False):
        at = block(chip, other)
        return copy(own_ref if own else all_ref.at[at], all_ref.at[at], send_sem.at[n], recv_sem.at[at], target)

    def side_copy(n, side, chip, other, target, own=False):
        at = block(chip, other)
        slot = beside.at[side, at]
        return copy(strip_ref.at[1 - side] if own else slot, slot, side_send.at[side, n], side_recv.at[side, at], target)

    started = []
    for side in range(2):

        @pl.when(has[1 - side])
        def _():
            for n, chip in enumerate(chips):
                side_copy(n, side, chips[0], False, device(chip, False, t + 1 - 2 * side), True).start()

    for n, chip in enumerate(chips[:0:-1]):
        started.append(level_copy(n, chips[0], False, device(chip, False, t), True))
        started[-1].start()
    n = len(chips) - 1
    started.append(level_copy(n, chips[0], False, across, True))
    started[-1].start()
    for chip in chips[1:]:
        n += 1
        level_copy(0, chip, False, across).wait_recv()
        started.append(level_copy(n, chip, False, across))
        started[-1].start()
    for side in range(2):

        @pl.when(has[side])
        def _():
            for n, chip in enumerate(chips):
                side_copy(0, side, chip, False, across).wait_recv()
                side_copy(len(chips) + n, side, chip, False, across).start()

    for chip in chips:
        level_copy(0, chip, True, across).wait_recv()
    for side in range(2):

        @pl.when(has[side])
        def _():
            for n, chip in enumerate(chips):
                side_copy(0, side, chip, True, across).wait_recv()
                side_copy(len(chips) + n, side, chip, False, across).wait_send()

        @pl.when(has[1 - side])
        def _():
            for n, chip in enumerate(chips):
                side_copy(n, side, chips[0], False, device(chip, False, t + 1 - 2 * side), True).wait_send()

    for one in started:
        one.wait_send()


def exchange(live, acc, folded, inner, spectrum, masks, row_table, col_table, count_x, sizes):
    tx_count, ty_count, src_count = sizes
    blocks = tx_count * src_count
    vmem = pl.BlockSpec(memory_space=pltpu.VMEM)
    cols = acc.shape[0]
    return pl.pallas_call(
        functools.partial(exchange_kernel, sizes),
        out_shape=(
            jax.ShapeDtypeStruct((blocks, count_x, cols), jnp.bfloat16),
            jax.ShapeDtypeStruct((2, blocks, PACK, count_x), jnp.bfloat16),
        ),
        in_specs=[vmem] * 8,
        out_specs=(vmem,) * 2,
        scratch_shapes=[
            pltpu.SMEM(live.shape, jnp.int32),
            pltpu.VMEM((count_x, cols), jnp.bfloat16),
            pltpu.VMEM((2, PACK, count_x), jnp.bfloat16),
            [pltpu.VMEM(folded.shape, jnp.bfloat16)] * 2,
            [pltpu.VMEM(inner.shape, jnp.bfloat16)] * 2,
            pltpu.SemaphoreType.DMA(()),
            pltpu.SemaphoreType.DMA((blocks,)),
            pltpu.SemaphoreType.DMA((blocks,)),
            pltpu.SemaphoreType.DMA((2, blocks)),
            pltpu.SemaphoreType.DMA((2, blocks)),
        ],
        compiler_params=pltpu.CompilerParams(collective_id=1, has_side_effects=True, vmem_limit_bytes=12 << 20),
        name="exchange",
    )(live, acc, folded, inner, spectrum, masks, row_table, col_table)


def diffuse_kernel(sizes, all_ref, beside, blend_ref, out_ref):
    tx_count, ty_count, src_count = sizes
    rows, cols = out_ref.shape
    blocks, count, _ = all_ref.shape
    samples = blocks * count
    tall = rows + 2 * EDGE
    level = all_ref[...].reshape(samples, cols)
    sides = [jnp.concatenate([beside[side, n] for n in range(blocks)], axis=1) for side in range(2)]
    strip = jnp.concatenate([sides[1], jnp.zeros((LANES - 2 * PACK, samples), jnp.bfloat16), sides[0]], axis=0)
    turned = (((1,), (1,)), ((), ()))
    middle = dot(blend_ref[0], level) + dot(blend_ref[1], level)
    edge = lax.dot_general(blend_ref[0], strip, turned, preferred_element_type=jnp.float32)
    edge += lax.dot_general(blend_ref[1], strip, turned, preferred_element_type=jnp.float32)
    acid = 1.0 - jnp.exp(-jnp.concatenate([middle, edge], axis=1))
    wide = cols + LANES
    row_block = lax.axis_index("tx") * src_count + lax.axis_index("src")
    col_block = lax.axis_index("ty")
    x = row_block * rows - EDGE + iota(acid.shape, 0)
    column = iota(acid.shape, 1)
    y = col_block * cols + jnp.where(column >= cols + LANES // 2, column - wide, column)
    inside = (x >= 0) & (x < blocks * rows) & (y >= 0) & (y < ty_count * cols)
    for repeat in range(2):
        acid = jnp.where(inside, acid, 0.0)
        near = (
            pltpu.roll(acid, 1, 0)
            + pltpu.roll(acid, tall - 1, 0)
            + pltpu.roll(acid, 1, 1)
            + pltpu.roll(acid, wide - 1, 1)
        )
        acid = acid + diffusion_rate * (near - 4.0 * acid)
    out_ref[...] = acid[EDGE : EDGE + rows, :cols]


def diffuse(levels, beside, blend, sizes):
    rows = blend.shape[1] - 2 * EDGE
    vmem = pl.BlockSpec(memory_space=pltpu.VMEM)
    return pl.pallas_call(
        functools.partial(diffuse_kernel, sizes),
        out_shape=jax.ShapeDtypeStruct((rows, levels.shape[2]), jnp.float32),
        in_specs=[vmem] * 3,
        out_specs=vmem,
        compiler_params=pltpu.CompilerParams(vmem_limit_bytes=12 << 20),
        name="diffuse",
    )(levels, beside, blend)


def body(sizes, cols, spectrum, pupil_mask, source_shifts, source_weights):
    turned, words, row_table, col_table, masks, blend = gather(
        spectrum, source_shifts, source_weights, pupil_mask, sizes, cols
    )
    count_x = blend.shape[2] // (sizes[0] * sizes[2])
    live, acc, folded, inner = image(turned, words, row_table, col_table, masks, sizes)
    levels, beside = exchange(live, acc, folded, inner, turned, masks, row_table, col_table, count_x, sizes)
    return diffuse(levels, beside, blend, sizes)


def solution(mesh):
    sizes = (mesh.shape["tx"], mesh.shape["ty"], mesh.shape["src"])
    placed = (P(None, ("tx", "ty"), "src"), P(), P("src", None), P("src"))
    return jax.shard_map(
        functools.partial(body, sizes, COLS),
        mesh=mesh,
        in_specs=placed,
        out_specs=P(("tx", "src"), "ty"),
        check_vma=False,
    )
```

```python
import functools
import math

import jax
import jax.numpy as jnp
from jax import lax
from jax.experimental import pallas as pl
from jax.experimental.pallas import tpu as pltpu
from jax.sharding import PartitionSpec as P

FRAME = 2048
LANES = 128
COLS = 256
EDGE = 8
PACK = 16
GROUP = 2
UNROLL = 4
TAIL = 8
MESH = pl.DeviceIdType.MESH

diffusion_rate = 0.2


def wave(turns, period):
    quarter = period // 4
    turn = (turns + quarter // 2) // quarter
    angle = (turns - turn * quarter).astype(jnp.float32) * (2 * math.pi / period)
    square = angle * angle
    sine = angle * (1 + square * (-1 / 6 + square * (1 / 120 + square * (-1 / 5040 + square / 362880))))
    cosine = 1 + square * (-1 / 2 + square * (1 / 24 + square * (-1 / 720 + square / 40320)))
    odd = (turn & 1) == 1
    first, second = jnp.where(odd, sine, cosine), jnp.where(odd, cosine, sine)
    return jnp.where(((turn + 1) & 2) == 2, -first, first), jnp.where((turn & 2) == 2, -second, second)


def iota(shape, dim):
    return lax.broadcasted_iota(jnp.int32, shape, dim)


def dot(a, b):
    return jnp.dot(a, b, preferred_element_type=jnp.float32)


def unit(size, back):
    rows, cols = iota((size, size), 0), iota((size, size), 1)
    return jnp.where(rows + cols == size - 1 if back else rows == cols, 1.0, 0.0).astype(jnp.bfloat16)


def flip_bits(index, mask):
    bit = 1
    while bit <= mask:
        if mask & bit:
            index = index + bit * (1 - 2 * lax.rem(index // bit, 2))
        bit *= 2
    return index


def others(index, count):
    if count & (count - 1) == 0:
        return [flip_bits(index, d) for d in range(1, count)]
    return [lax.rem(index + d, count) for d in range(1, count)]


def mates(index, count):
    orders = [
        sorted((i for i in range(count) if i != at), key=lambda i: (i != at ^ 1, abs(i - at), i)) for at in range(count)
    ]
    return [sum(jnp.where(index == at, orders[at][n], 0) for at in range(count)) for n in range(count - 1)]


def row_table(row_ref, count, block, blocks):
    half = row_ref.shape[0] // (2 * GROUP)
    each = LANES // GROUP
    step = FRAME // (count * blocks)
    sample = iota((half, each), 1)
    x = step * (blocks * sample + block)
    cosine, sine = wave((x * iota((half, each), 0)) & (FRAME - 1), FRAME)
    cosine = jnp.where(sample < count, cosine, 0.0)
    sine = jnp.where(sample < count, sine, 0.0)
    none = jnp.zeros((half, each), jnp.float32)
    for g in range(GROUP):
        for part, (real, imag) in enumerate(((cosine, sine), (-sine, cosine))):
            row = [real if n == g else none for n in range(GROUP)] + [imag if n == g else none for n in range(GROUP)]
            at = (2 * g + part) * half
            row_ref[at : at + half] = jnp.concatenate(row, axis=1).astype(jnp.bfloat16)


def col_table(col_ref, t):
    cols, half = col_ref.shape[0], col_ref.shape[1] // 2
    chunk = 64

    def fill(n, carry):
        start = pl.multiple_of(n * chunk, chunk)
        y = t * cols + start + iota((chunk, half), 0)
        cosine, sine = wave((y * (2 * iota((chunk, half), 1) + 1)) & (2 * FRAME - 1), 2 * FRAME)
        col_ref[pl.ds(start, chunk), :half] = cosine.astype(jnp.bfloat16)
        col_ref[pl.ds(start, chunk), half:] = sine.astype(jnp.bfloat16)
        return carry

    lax.fori_loop(0, cols // chunk, fill, 0)


def list_live(live_ref, shifts_ref, weights_ref):
    src_count, _, slots = shifts_ref.shape
    width = live_ref.shape[1]
    weights = weights_ref[:, 0, :].astype(jnp.float32)
    words = shifts_ref[:, 0, :].astype(jnp.float32) + shifts_ref[:, 1, :].astype(jnp.float32) * 1024.0 + weights * 1048576.0
    on = jnp.where(weights > 0, 1.0, 0.0)
    ahead = jnp.where(iota((slots, slots), 0) < iota((slots, slots), 1), 1.0, 0.0)
    rank = dot(on.astype(jnp.bfloat16), ahead.astype(jnp.bfloat16))
    before = jnp.zeros((1, 1), jnp.float32)
    ranks = []
    for k in range(src_count):
        ranks.append(rank[k : k + 1] + before)
        before = before + jnp.sum(on[k : k + 1], axis=1, keepdims=True)
    rank = jnp.where(on > 0, jnp.concatenate(ranks, axis=0), -1.0).T
    words = words.T
    place = (iota((slots, width), 1) - GROUP).astype(jnp.float32)
    total = jnp.zeros((slots, width), jnp.float32)
    for k in range(src_count):
        total += jnp.where(rank[:, k : k + 1] == place, words[:, k : k + 1], 0.0)
    found = jnp.sum(total, axis=0, keepdims=True)
    live_ref[...] = jnp.where(iota((1, width), 1) == width - 1, before, found).astype(jnp.int32)


def turns_before_tail(live):
    steps = (live[0, live.shape[1] - 1] + GROUP - 1) // GROUP + 1 - TAIL
    return jnp.maximum(steps + UNROLL - 1, 0) // UNROLL


def blend_table(blend_ref, block, blocks):
    _, tall, samples = blend_ref.shape
    rows = tall - 2 * EDGE
    step = FRAME // samples
    count = samples // blocks
    chunk = PACK

    def fill(n, carry):
        start = pl.multiple_of(n * chunk, chunk)
        x = block * rows - EDGE + start + iota((chunk, samples), 0)
        column = iota((chunk, samples), 1)
        owner = column // count
        gap = x - step * (blocks * (column - owner * count) + owner)
        gap = ((gap + FRAME // 2) & (FRAME - 1)) - FRAME // 2
        cosine, sine = wave(gap, 2 * FRAME)
        place = block * rows - EDGE + start + iota((chunk, 1), 0)
        place = place & (2 * step - 1)
        scale = jnp.zeros((chunk, 1), jnp.float32)
        for n in range(2 * step):
            if n % step:
                scale = jnp.where(place == n, math.sin(math.pi * n / step) / samples, scale)
        scale = jnp.where((owner & 1) == 1, -scale, scale)
        here = gap == 0
        table = jnp.where(here, 1.0, scale * cosine / jnp.where(here, 1.0, sine))
        high = table.astype(jnp.bfloat16)
        blend_ref[0, pl.ds(start, chunk)] = high
        blend_ref[1, pl.ds(start, chunk)] = (table - high.astype(jnp.float32)).astype(jnp.bfloat16)
        return carry

    lax.fori_loop(0, tall // chunk, fill, 0)


def gather_kernel(
    sizes, spec_hbm, shift_ref, weight_ref, pupil_hbm, turned_ref, mirror_ref, live_ref, row_ref, col_ref, mask_ref, blend_ref,
    shifts_ref, weights_ref, all_ref, spec_ref, pupil_ref, local_sem, send_sem, recv_sem, side_send, side_recv,
):
    tx_count, ty_count, src_count = sizes
    pair_count = tx_count // 2
    tx, t, s = lax.axis_index("tx"), lax.axis_index("ty"), lax.axis_index("src")
    pair, core = tx // 2, lax.rem(tx, 2)
    other_core = 1 - core
    far_t = mates(t, ty_count)
    far_s = others(s, src_count)
    far_pair = others(pair, pair_count)

    def along_ty(i):
        return {"tx": tx, "ty": i, "src": s}

    def along_src(i):
        return {"tx": tx, "ty": t, "src": i}

    loads = [
        pltpu.make_async_copy(src, dst, local_sem.at[n])
        for n, (src, dst) in enumerate(
            (
                (spec_hbm, spec_ref),
                (pupil_hbm, pupil_ref),
                (shift_ref, shifts_ref.at[s]),
                (weight_ref, weights_ref.at[s]),
            )
        )
    ]
    for load in loads:
        load.start()

    across = {"tx": 2 * pair + other_core, "ty": t, "src": s}
    hood = [(i, k) for k in far_s + [s] for i in far_pair + [pair] if i is not pair or k is not s]
    partners = [along_ty(i) for i in far_t] + [{"tx": 2 * i + core, "ty": t, "src": k} for i, k in hood] + [across]
    barrier = pltpu.get_barrier_semaphore()
    for partner in partners:
        pl.semaphore_signal(barrier, inc=1, device_id=partner, device_id_type=MESH)
    pl.semaphore_wait(barrier, len(partners))
    loads[0].wait()

    started = []
    own = (tx, t, s)

    both = slice(None)

    def part(plane, piece):
        i, j, k = piece
        return all_ref.at[k, plane, i, j], recv_sem.at[0, k, i, j]

    def send(plane, piece, device):
        slot, arrived = part(plane, piece)
        copy = pltpu.make_async_remote_copy(
            src_ref=spec_ref if piece is own else slot,
            dst_ref=slot,
            send_sem=send_sem.at[len(started)],
            recv_sem=arrived,
            device_id=device,
            device_id_type=MESH,
        )
        copy.start()
        started.append(copy)

    def arrive(plane, piece):
        slot, arrived = part(plane, piece)
        pltpu.make_async_remote_copy(
            src_ref=slot,
            dst_ref=slot,
            send_sem=send_sem.at[0],
            recv_sem=arrived,
            device_id=across,
            device_id_type=MESH,
        ).wait_recv()

    def spread(piece):
        for i, k in hood:
            send(both, piece, {"tx": 2 * i + core, "ty": t, "src": k})

    for j in far_t:
        send(both, own, along_ty(j))
    spread(own)
    send(both, own, across)

    side = []
    for n, i in enumerate(far_s):
        for m, (src, dst) in enumerate(((shift_ref, shifts_ref), (weight_ref, weights_ref))):
            copy = pltpu.make_async_remote_copy(
                src_ref=src,
                dst_ref=dst.at[s],
                send_sem=side_send.at[m, n],
                recv_sem=side_recv.at[m, s],
                device_id=along_src(i),
                device_id_type=MESH,
            )
            copy.start()
            side.append(copy)

    for load in loads[1:]:
        load.wait()
    for plane in range(2):
        all_ref[s, plane, tx, t] = spec_ref[plane]
    block = tx * src_count + s
    blocks = tx_count * src_count
    row_table(row_ref, blend_ref.shape[2] // blocks, block, blocks)
    col_table(col_ref, t)
    half = pupil_ref.shape[0] // 2
    pupil = pupil_ref[...].astype(jnp.float32).astype(jnp.bfloat16)
    turned = (((1,), (1,)), ((), ()))
    mask_ref[:half] = lax.dot_general(unit(half, False), pupil[:, half:], turned, preferred_element_type=jnp.float32).astype(jnp.bfloat16)
    mask_ref[half:] = lax.dot_general(unit(half, True), pupil[:, :half], turned, preferred_element_type=jnp.float32).astype(jnp.bfloat16)

    part_rows, part_cols = ty_count * spec_ref.shape[1], spec_ref.shape[2]

    def turn(i, k):
        cell = jnp.concatenate([all_ref[k, plane, i].reshape(part_rows, part_cols) for plane in range(2)], axis=0)
        for back, target in enumerate((turned_ref, mirror_ref)):
            start = (src_count - 1 - k if back else k) * part_cols
            rows = pl.ds(pl.multiple_of(start, part_cols), part_cols)
            value = lax.dot_general(unit(part_cols, back), cell, turned, preferred_element_type=jnp.float32)
            for plane in range(2):
                tile = value[:, plane * part_rows : (plane + 1) * part_rows]
                target[plane * tx_count + i, rows] = tile
                target[(plane + 2) * tx_count + i, rows] = -tile

    def pass_on(i, j, k, also=None):
        piece = (2 * i + core, j, k)
        arrive(both, piece)
        if also is not None:
            send(both, piece, along_ty(also))
        send(both, piece, across)

    mate, far_t = far_t[0], far_t[1:]
    near, distant = hood[1:], hood[:1]
    for i, k in near:
        pass_on(i, t, k, mate)
    for n, j in enumerate(far_t):
        arrive(both, (tx, j, s))
        spread((tx, j, s))
        if n == 0:
            for i, k in distant:
                pass_on(i, t, k, mate)
    for j in [mate] + far_t:
        if j is mate:
            arrive(both, (tx, j, s))
        send(both, (tx, j, s), across)
    turn(tx, s)
    blend_table(blend_ref, block, blocks)
    for i, k in near + distant:
        pass_on(i, mate, k)
    for j in far_t:
        for i, k in near + distant:
            pass_on(i, j, k)
    for i, k in near + distant:
        turn(2 * i + core, k)
    near_first = [t, mate] + far_t
    for n, i in enumerate(far_s):
        for m, (src, dst) in enumerate(((shift_ref, shifts_ref), (weight_ref, weights_ref))):
            pltpu.make_async_remote_copy(
                src_ref=src,
                dst_ref=dst.at[i],
                send_sem=side_send.at[m, n],
                recv_sem=side_recv.at[m, i],
                device_id=across,
                device_id_type=MESH,
            ).wait_recv()
    list_live(live_ref, shifts_ref, weights_ref)
    for i in [pair] + far_pair:
        for k in [s] + far_s:
            for j in near_first:
                arrive(both, (2 * i + other_core, j, k))
            turn(2 * i + other_core, k)
    for copy in started + side:
        copy.wait_send()


def gather(spectrum, source_shifts, source_weights, pupil_mask, sizes, cols):
    tx_count, ty_count, src_count = sizes
    pair_count = tx_count // 2
    _, block_rows, block_cols = spectrum.shape
    slots = source_weights.shape[0]
    length = pupil_mask.shape[0]
    blocks = tx_count * src_count
    samples = 2 * length
    width = pl.cdiv(src_count * slots + (UNROLL + TAIL + 2) * GROUP + 1, LANES) * LANES
    vmem = pl.BlockSpec(memory_space=pltpu.VMEM)
    lines = pair_count * src_count * ty_count
    sends = ty_count - 1 + lines + ty_count * (src_count - 1 + pair_count - 1)
    sends += 3 * ty_count * (src_count - 1) * (pair_count - 1)
    return pl.pallas_call(
        functools.partial(gather_kernel, sizes),
        out_shape=(
            jax.ShapeDtypeStruct((4 * tx_count, src_count * block_cols, ty_count * block_rows), jnp.float32),
            jax.ShapeDtypeStruct((4 * tx_count, src_count * block_cols, ty_count * block_rows), jnp.float32),
            jax.ShapeDtypeStruct((1, width), jnp.int32),
            jax.ShapeDtypeStruct((GROUP * length, 2 * LANES), jnp.bfloat16),
            jax.ShapeDtypeStruct((cols, length), jnp.bfloat16),
            jax.ShapeDtypeStruct((length, length), jnp.bfloat16),
            jax.ShapeDtypeStruct((2, FRAME // blocks + 2 * EDGE, samples), jnp.bfloat16),
        ),
        in_specs=[pl.BlockSpec(memory_space=pltpu.HBM)] * 4,
        out_specs=(vmem,) * 7,
        scratch_shapes=[
            pltpu.VMEM((src_count, 2, slots), jnp.int32),
            pltpu.VMEM((src_count, 1, slots), jnp.int32),
            pltpu.VMEM((src_count, 2, tx_count, ty_count, block_rows, block_cols), jnp.bfloat16),
            pltpu.VMEM(spectrum.shape, jnp.bfloat16),
            pltpu.VMEM(pupil_mask.shape, jnp.int32),
            pltpu.SemaphoreType.DMA((4,)),
            pltpu.SemaphoreType.DMA((sends,)),
            pltpu.SemaphoreType.DMA((2, src_count, tx_count, ty_count)),
            pltpu.SemaphoreType.DMA((2, src_count)),
            pltpu.SemaphoreType.DMA((2, src_count)),
        ],
        compiler_params=pltpu.CompilerParams(collective_id=0, has_side_effects=True, vmem_limit_bytes=24 << 20),
        name="gather",
    )(*(pltpu.with_memory_space_constraint(a, pltpu.HBM) for a in (spectrum, source_shifts.T, source_weights[None], pupil_mask)))


def stages(sizes, spec, mirror, mask_ref, row_ref, col_ref, live):
    half = col_ref.shape[1] // 2
    height = spec.shape[1]
    tiles = spec.shape[0] // 4
    block = lax.axis_index("tx") * sizes[2] + lax.axis_index("src")
    power = lax.rem(block, 4)
    flip = 2 * lax.rem(power, 2)
    middle = (lax.rem(4 - power, 4), power + 1 - 2 * lax.rem(power, 2))
    lane = iota((2 * half, LANES), 1)
    first_half = iota((1, LANES), 1) < LANES // 2

    def fold(n, slot):
        for g in range(GROUP):
            word = live[0, (n + 1) * GROUP + g]
            a, b = word & 1023, (word >> 10) & 1023
            tile, rest = a // LANES, lax.rem(a, LANES)
            keep = lane >= rest
            low = pltpu.roll(mask_ref[:, :LANES], rest, 1)
            high = pltpu.roll(mask_ref[:, LANES:], rest, 1)
            ends = jnp.where(keep, low, high)
            centre = jnp.where(keep, high, low)
            keep = keep[:half]
            last = jnp.minimum(tile + 2, tiles - 1)

            def window(source, start, plane, part):
                rows = pl.ds(start, half)
                at = slice(part * half, (part + 1) * half)
                outer = jnp.where(keep, source[plane * tiles + tile, rows, :], source[(plane + flip) * tiles + last, rows, :])
                between = source[middle[plane] * tiles + tile + 1, rows, :]
                return outer.astype(jnp.bfloat16) * ends[at] + between.astype(jnp.bfloat16) * centre[at]

            upper = [window(spec, b + half, plane, 0) for plane in range(2)]
            lower = [window(mirror, height - half - b, plane, 1) for plane in range(2)]
            at = 2 * g * LANES
            slot[:half, at : at + LANES] = upper[0] + lower[0]
            slot[:half, at + LANES : at + 2 * LANES] = upper[1] + lower[1]
            slot[half:, at : at + LANES] = lower[1] - upper[1]
            slot[half:, at + LANES : at + 2 * LANES] = upper[0] - lower[0]

    def cross(source, slot):
        slot[...] = dot(source[...], row_ref[...]).astype(jnp.bfloat16)

    def square(n, source):
        wide = dot(col_ref[...], source[...])
        real, imag = wide[:, :LANES], wide[:, LANES:]
        pair = [(live[0, (n + 1) * GROUP + g] >> 20).astype(jnp.float32) for g in range(GROUP)]
        return jnp.where(first_half, pair[0], pair[1]) * (real * real + imag * imag)

    return fold, cross, square


def image_kernel(
    sizes, live_ref, spec, mirror, mask_ref, row_ref, col_ref, acc, next_folded, next_inner,
    live, other_folded, other_inner, live_sem,
):
    load = pltpu.make_async_copy(live_ref, live, live_sem)
    load.start()
    fold, cross, square = stages(sizes, spec, mirror, mask_ref, row_ref, col_ref, live)
    folded = (next_folded, other_folded)
    inner = (other_inner, next_inner)
    acc[...] = jnp.zeros_like(acc)
    next_inner[...] = jnp.zeros_like(next_inner)
    load.wait()
    fold(0, folded[0])

    def turn_body(turn_index, carry):
        for g in range(UNROLL):
            n = turn_index * UNROLL + g
            fold(n + 1, folded[1 - g % 2])
            cross(folded[g % 2], inner[g % 2])
            acc[...] += square(n - 1, inner[1 - g % 2])
        return carry

    lax.fori_loop(0, turns_before_tail(live), turn_body, 0)


def image(live, spectrum, mirror, row_table, col_table, masks, sizes):
    cols, length = col_table.shape
    vmem = pl.BlockSpec(memory_space=pltpu.VMEM)
    return pl.pallas_call(
        functools.partial(image_kernel, sizes),
        out_shape=(
            jax.ShapeDtypeStruct((cols, LANES), jnp.float32),
            jax.ShapeDtypeStruct((length, GROUP * 2 * LANES), jnp.bfloat16),
            jax.ShapeDtypeStruct((length, 2 * LANES), jnp.bfloat16),
        ),
        in_specs=[vmem] * 6,
        out_specs=(vmem,) * 3,
        scratch_shapes=[
            pltpu.SMEM(live.shape, jnp.int32),
            pltpu.VMEM((length, GROUP * 2 * LANES), jnp.bfloat16),
            pltpu.VMEM((length, 2 * LANES), jnp.bfloat16),
            pltpu.SemaphoreType.DMA(()),
        ],
        compiler_params=pltpu.CompilerParams(vmem_limit_bytes=12 << 20),
        name="image",
    )(live, spectrum, mirror, masks, row_table, col_table)


def exchange_kernel(
    sizes, sources, live_ref, acc, first_folded, first_inner, spec, mirror, mask_ref, row_ref, col_ref, all_ref, beside,
    live, own_ref, strip_ref, folded, inner, live_sem, send_sem, recv_sem, side_send, side_recv,
):
    tx_count, ty_count, src_count = sizes
    pair_count = tx_count // 2
    tx, t, s = lax.axis_index("tx"), lax.axis_index("ty"), lax.axis_index("src")
    pair, core = tx // 2, lax.rem(tx, 2)
    far_s = [s] + others(s, src_count)
    far_pair = [pair] + others(pair, pair_count)
    chips = [(i, k) for k in far_s for i in far_pair]

    def device(chip, other, z):
        return {"tx": 2 * chip[0] + (1 - core if other else core), "ty": z, "src": chip[1]}

    def block(chip, other):
        return (2 * chip[0] + (1 - core if other else core)) * src_count + chip[1]

    across = device(chips[0], True, t)
    barrier = pltpu.get_barrier_semaphore()

    def greet(chip, z):
        pl.semaphore_signal(barrier, inc=1, device_id=device(chip, False, z), device_id_type=MESH)

    load = pltpu.make_async_copy(live_ref, live, live_sem)
    load.start()
    has = (t > 0, t < ty_count - 1)
    beside[...] = jnp.zeros_like(beside)
    pl.semaphore_signal(barrier, inc=1, device_id=across, device_id_type=MESH)
    for chip in chips[1:]:
        greet(chip, t)
    for side in range(2):

        @pl.when(has[side])
        def _():
            for chip in chips:
                greet(chip, t + 2 * side - 1)

    fold, cross, square = stages(sizes, spec, mirror, mask_ref, row_ref, col_ref, live)
    load.wait()
    n = turns_before_tail(live) * UNROLL
    level = acc[...]
    source_folded, source_inner = first_folded, first_inner
    for g in range(TAIL):
        if g < TAIL - 2:
            fold(n + g + 1, folded[g % 2])
        if g < TAIL - 1:
            cross(source_folded, inner[g % 2])
        level += square(n + g - 1, source_inner)
        source_folded, source_inner = folded[g % 2], inner[g % 2]

    cols = level.shape[0]
    count_x = own_ref.shape[0]
    level = (level + pltpu.roll(level, LANES // 2, 1)) / (2.0 * sources)
    own = level.T[:count_x].astype(jnp.bfloat16)
    own_ref[...] = own
    strip_ref[0] = level[:PACK, :count_x].astype(jnp.bfloat16)
    strip_ref[1] = level[cols - PACK :, :count_x].astype(jnp.bfloat16)
    all_ref[block(chips[0], False)] = own
    sides = jnp.minimum(t, 1) + jnp.minimum(ty_count - 1 - t, 1)
    pl.semaphore_wait(barrier, len(chips) * (1 + sides))

    def copy(src, dst, send, recv, target):
        return pltpu.make_async_remote_copy(
            src_ref=src, dst_ref=dst, send_sem=send, recv_sem=recv, device_id=target, device_id_type=MESH
        )

    def level_copy(n, chip, other, target, own=False):
        at = block(chip, other)
        return copy(own_ref if own else all_ref.at[at], all_ref.at[at], send_sem.at[n], recv_sem.at[at], target)

    def side_copy(n, side, chip, other, target, own=False):
        at = block(chip, other)
        slot = beside.at[side, at]
        return copy(strip_ref.at[1 - side] if own else slot, slot, side_send.at[side, n], side_recv.at[side, at], target)

    started = []
    for side in range(2):

        @pl.when(has[1 - side])
        def _():
            for n, chip in enumerate(chips):
                side_copy(n, side, chips[0], False, device(chip, False, t + 1 - 2 * side), True).start()

    for n, chip in enumerate(chips[:0:-1]):
        started.append(level_copy(n, chips[0], False, device(chip, False, t), True))
        started[-1].start()
    n = len(chips) - 1
    started.append(level_copy(n, chips[0], False, across, True))
    started[-1].start()
    for chip in chips[1:]:
        n += 1
        level_copy(0, chip, False, across).wait_recv()
        started.append(level_copy(n, chip, False, across))
        started[-1].start()
    for side in range(2):

        @pl.when(has[side])
        def _():
            for n, chip in enumerate(chips):
                side_copy(0, side, chip, False, across).wait_recv()
                side_copy(len(chips) + n, side, chip, False, across).start()

    for chip in chips:
        level_copy(0, chip, True, across).wait_recv()
    for side in range(2):

        @pl.when(has[side])
        def _():
            for n, chip in enumerate(chips):
                side_copy(0, side, chip, True, across).wait_recv()
                side_copy(len(chips) + n, side, chip, False, across).wait_send()

        @pl.when(has[1 - side])
        def _():
            for n, chip in enumerate(chips):
                side_copy(n, side, chips[0], False, device(chip, False, t + 1 - 2 * side), True).wait_send()

    for one in started:
        one.wait_send()


def exchange(sources, live, acc, folded, inner, spectrum, mirror, masks, row_table, col_table, count_x, sizes):
    tx_count, ty_count, src_count = sizes
    blocks = tx_count * src_count
    vmem = pl.BlockSpec(memory_space=pltpu.VMEM)
    cols = acc.shape[0]
    return pl.pallas_call(
        functools.partial(exchange_kernel, sizes, sources),
        out_shape=(
            jax.ShapeDtypeStruct((blocks, count_x, cols), jnp.bfloat16),
            jax.ShapeDtypeStruct((2, blocks, PACK, count_x), jnp.bfloat16),
        ),
        in_specs=[vmem] * 9,
        out_specs=(vmem,) * 2,
        scratch_shapes=[
            pltpu.SMEM(live.shape, jnp.int32),
            pltpu.VMEM((count_x, cols), jnp.bfloat16),
            pltpu.VMEM((2, PACK, count_x), jnp.bfloat16),
            [pltpu.VMEM(folded.shape, jnp.bfloat16)] * 2,
            [pltpu.VMEM(inner.shape, jnp.bfloat16)] * 2,
            pltpu.SemaphoreType.DMA(()),
            pltpu.SemaphoreType.DMA((blocks,)),
            pltpu.SemaphoreType.DMA((blocks,)),
            pltpu.SemaphoreType.DMA((2, blocks)),
            pltpu.SemaphoreType.DMA((2, blocks)),
        ],
        compiler_params=pltpu.CompilerParams(collective_id=1, has_side_effects=True, vmem_limit_bytes=12 << 20),
        name="exchange",
    )(live, acc, folded, inner, spectrum, mirror, masks, row_table, col_table)


def diffuse_kernel(sizes, all_ref, beside, blend_ref, out_ref):
    tx_count, ty_count, src_count = sizes
    rows, cols = out_ref.shape
    blocks, count, _ = all_ref.shape
    samples = blocks * count
    tall = rows + 2 * EDGE
    level = all_ref[...].reshape(samples, cols)
    sides = [jnp.concatenate([beside[side, n] for n in range(blocks)], axis=1) for side in range(2)]
    strip = jnp.concatenate([sides[1], jnp.zeros((LANES - 2 * PACK, samples), jnp.bfloat16), sides[0]], axis=0)
    turned = (((1,), (1,)), ((), ()))
    middle = dot(blend_ref[0], level) + dot(blend_ref[1], level)
    edge = lax.dot_general(blend_ref[0], strip, turned, preferred_element_type=jnp.float32)
    edge += lax.dot_general(blend_ref[1], strip, turned, preferred_element_type=jnp.float32)
    acid = 1.0 - jnp.exp(-jnp.concatenate([middle, edge], axis=1))
    wide = cols + LANES
    row_block = lax.axis_index("tx") * src_count + lax.axis_index("src")
    col_block = lax.axis_index("ty")
    x = row_block * rows - EDGE + iota(acid.shape, 0)
    column = iota(acid.shape, 1)
    y = col_block * cols + jnp.where(column >= cols + LANES // 2, column - wide, column)
    inside = (x >= 0) & (x < blocks * rows) & (y >= 0) & (y < ty_count * cols)
    for repeat in range(2):
        acid = jnp.where(inside, acid, 0.0)
        near = (
            pltpu.roll(acid, 1, 0)
            + pltpu.roll(acid, tall - 1, 0)
            + pltpu.roll(acid, 1, 1)
            + pltpu.roll(acid, wide - 1, 1)
        )
        acid = acid + diffusion_rate * (near - 4.0 * acid)
    out_ref[...] = acid[EDGE : EDGE + rows, :cols]


def diffuse(levels, beside, blend, sizes):
    rows = blend.shape[1] - 2 * EDGE
    vmem = pl.BlockSpec(memory_space=pltpu.VMEM)
    return pl.pallas_call(
        functools.partial(diffuse_kernel, sizes),
        out_shape=jax.ShapeDtypeStruct((rows, levels.shape[2]), jnp.float32),
        in_specs=[vmem] * 3,
        out_specs=vmem,
        compiler_params=pltpu.CompilerParams(vmem_limit_bytes=12 << 20),
        name="diffuse",
    )(levels, beside, blend)


def body(sizes, cols, spectrum, pupil_mask, source_shifts, source_weights):
    turned, mirror, live, row_table, col_table, masks, blend = gather(
        spectrum, source_shifts, source_weights, pupil_mask, sizes, cols
    )
    sources = source_weights.shape[0] * sizes[2]
    count_x = blend.shape[2] // (sizes[0] * sizes[2])
    acc, folded, inner = image(live, turned, mirror, row_table, col_table, masks, sizes)
    levels, beside = exchange(
        sources, live, acc, folded, inner, turned, mirror, masks, row_table, col_table, count_x, sizes
    )
    return diffuse(levels, beside, blend, sizes)


def solution(mesh):
    sizes = (mesh.shape["tx"], mesh.shape["ty"], mesh.shape["src"])
    placed = (P(None, ("tx", "ty"), "src"), P(), P("src", None), P("src"))
    return jax.shard_map(
        functools.partial(body, sizes, COLS),
        mesh=mesh,
        in_specs=placed,
        out_specs=P(("tx", "src"), "ty"),
        check_vma=False,
    )
```

```python
import functools
import math

import jax
import jax.numpy as jnp
from jax import lax
from jax.experimental import pallas as pl
from jax.experimental.pallas import tpu as pltpu
from jax.sharding import PartitionSpec as P

FRAME = 2048
LANES = 128
COLS = 256
EDGE = 8
PACK = 16
GROUP = 2
UNROLL = 4
TAIL = 8
MESH = pl.DeviceIdType.MESH

diffusion_rate = 0.2


def wave(turns, period):
    quarter = period // 4
    turn = (turns + quarter // 2) // quarter
    angle = (turns - turn * quarter).astype(jnp.float32) * (2 * math.pi / period)
    square = angle * angle
    sine = angle * (1 + square * (-1 / 6 + square * (1 / 120 + square * (-1 / 5040 + square / 362880))))
    cosine = 1 + square * (-1 / 2 + square * (1 / 24 + square * (-1 / 720 + square / 40320)))
    odd = (turn & 1) == 1
    first, second = jnp.where(odd, sine, cosine), jnp.where(odd, cosine, sine)
    return jnp.where(((turn + 1) & 2) == 2, -first, first), jnp.where((turn & 2) == 2, -second, second)


def iota(shape, dim):
    return lax.broadcasted_iota(jnp.int32, shape, dim)


def dot(a, b):
    return jnp.dot(a, b, preferred_element_type=jnp.float32)


def unit(size, back):
    rows, cols = iota((size, size), 0), iota((size, size), 1)
    return jnp.where(rows + cols == size - 1 if back else rows == cols, 1.0, 0.0).astype(jnp.bfloat16)


def flip_bits(index, mask):
    bit = 1
    while bit <= mask:
        if mask & bit:
            index = index + bit * (1 - 2 * lax.rem(index // bit, 2))
        bit *= 2
    return index


def others(index, count):
    if count & (count - 1) == 0:
        return [flip_bits(index, d) for d in range(1, count)]
    return [lax.rem(index + d, count) for d in range(1, count)]


def mates(index, count):
    orders = [
        sorted((i for i in range(count) if i != at), key=lambda i: (i != at ^ 1, abs(i - at), i)) for at in range(count)
    ]
    return [sum(jnp.where(index == at, orders[at][n], 0) for at in range(count)) for n in range(count - 1)]


def row_table(row_ref, count, block, blocks):
    half = row_ref.shape[0] // (2 * GROUP)
    each = LANES // GROUP
    step = FRAME // (count * blocks)
    sample = iota((half, each), 1)
    x = step * (blocks * sample + block)
    cosine, sine = wave((x * iota((half, each), 0)) & (FRAME - 1), FRAME)
    cosine = jnp.where(sample < count, cosine, 0.0)
    sine = jnp.where(sample < count, sine, 0.0)
    none = jnp.zeros((half, each), jnp.float32)
    for g in range(GROUP):
        for part, (real, imag) in enumerate(((cosine, sine), (-sine, cosine))):
            row = [real if n == g else none for n in range(GROUP)] + [imag if n == g else none for n in range(GROUP)]
            at = (2 * g + part) * half
            row_ref[at : at + half] = jnp.concatenate(row, axis=1).astype(jnp.bfloat16)


def col_table(col_ref, t):
    cols, half = col_ref.shape[0], col_ref.shape[1] // 2
    chunk = 64

    def fill(n, carry):
        start = pl.multiple_of(n * chunk, chunk)
        y = t * cols + start + iota((chunk, half), 0)
        cosine, sine = wave((y * (2 * iota((chunk, half), 1) + 1)) & (2 * FRAME - 1), 2 * FRAME)
        col_ref[pl.ds(start, chunk), :half] = cosine.astype(jnp.bfloat16)
        col_ref[pl.ds(start, chunk), half:] = sine.astype(jnp.bfloat16)
        return carry

    lax.fori_loop(0, cols // chunk, fill, 0)


def list_live(live_ref, shifts_ref, weights_ref):
    src_count, _, slots = shifts_ref.shape
    width = live_ref.shape[1]
    weights = weights_ref[:, 0, :].astype(jnp.float32)
    words = shifts_ref[:, 0, :].astype(jnp.float32) + shifts_ref[:, 1, :].astype(jnp.float32) * 1024.0 + weights * 1048576.0
    on = jnp.where(weights > 0, 1.0, 0.0)
    ahead = jnp.where(iota((slots, slots), 0) < iota((slots, slots), 1), 1.0, 0.0)
    rank = dot(on.astype(jnp.bfloat16), ahead.astype(jnp.bfloat16))
    before = jnp.zeros((1, 1), jnp.float32)
    ranks = []
    for k in range(src_count):
        ranks.append(rank[k : k + 1] + before)
        before = before + jnp.sum(on[k : k + 1], axis=1, keepdims=True)
    rank = jnp.where(on > 0, jnp.concatenate(ranks, axis=0), -1.0).T
    words = words.T
    place = (iota((slots, width), 1) - GROUP).astype(jnp.float32)
    total = jnp.zeros((slots, width), jnp.float32)
    for k in range(src_count):
        total += jnp.where(rank[:, k : k + 1] == place, words[:, k : k + 1], 0.0)
    found = jnp.sum(total, axis=0, keepdims=True)
    live_ref[...] = jnp.where(iota((1, width), 1) == width - 1, before, found).astype(jnp.int32)


def turns_before_tail(live):
    steps = (live[0, live.shape[1] - 1] + GROUP - 1) // GROUP + 1 - TAIL
    return jnp.maximum(steps + UNROLL - 1, 0) // UNROLL


def blend_table(blend_ref, block, blocks):
    _, tall, samples = blend_ref.shape
    rows = tall - 2 * EDGE
    step = FRAME // samples
    count = samples // blocks
    chunk = PACK

    def fill(n, carry):
        start = pl.multiple_of(n * chunk, chunk)
        x = block * rows - EDGE + start + iota((chunk, samples), 0)
        column = iota((chunk, samples), 1)
        owner = column // count
        gap = x - step * (blocks * (column - owner * count) + owner)
        gap = ((gap + FRAME // 2) & (FRAME - 1)) - FRAME // 2
        cosine, sine = wave(gap, 2 * FRAME)
        place = block * rows - EDGE + start + iota((chunk, 1), 0)
        place = place & (2 * step - 1)
        scale = jnp.zeros((chunk, 1), jnp.float32)
        for n in range(2 * step):
            if n % step:
                scale = jnp.where(place == n, math.sin(math.pi * n / step) / samples, scale)
        scale = jnp.where((owner & 1) == 1, -scale, scale)
        here = gap == 0
        table = jnp.where(here, 1.0, scale * cosine / jnp.where(here, 1.0, sine))
        high = table.astype(jnp.bfloat16)
        blend_ref[0, pl.ds(start, chunk)] = high
        blend_ref[1, pl.ds(start, chunk)] = (table - high.astype(jnp.float32)).astype(jnp.bfloat16)
        return carry

    lax.fori_loop(0, tall // chunk, fill, 0)


def gather_kernel(
    sizes, spec_hbm, shift_ref, weight_ref, pupil_hbm, turned_ref, mirror_ref, live_ref, row_ref, col_ref, mask_ref, blend_ref,
    shifts_ref, weights_ref, all_ref, spec_ref, pupil_ref, local_sem, send_sem, recv_sem, side_send, side_recv,
):
    tx_count, ty_count, src_count = sizes
    pair_count = tx_count // 2
    tx, t, s = lax.axis_index("tx"), lax.axis_index("ty"), lax.axis_index("src")
    pair, core = tx // 2, lax.rem(tx, 2)
    other_core = 1 - core
    far_t = mates(t, ty_count)
    far_s = others(s, src_count)
    far_pair = others(pair, pair_count)

    def along_ty(i):
        return {"tx": tx, "ty": i, "src": s}

    def along_src(i):
        return {"tx": tx, "ty": t, "src": i}

    loads = [
        pltpu.make_async_copy(src, dst, local_sem.at[n])
        for n, (src, dst) in enumerate(
            (
                (spec_hbm, spec_ref),
                (pupil_hbm, pupil_ref),
                (shift_ref, shifts_ref.at[s]),
                (weight_ref, weights_ref.at[s]),
            )
        )
    ]
    for load in loads:
        load.start()

    across = {"tx": 2 * pair + other_core, "ty": t, "src": s}
    hood = [(i, k) for k in far_s + [s] for i in far_pair + [pair] if i is not pair or k is not s]
    partners = [along_ty(i) for i in far_t] + [{"tx": 2 * i + core, "ty": t, "src": k} for i, k in hood] + [across]
    barrier = pltpu.get_barrier_semaphore()
    for partner in partners:
        pl.semaphore_signal(barrier, inc=1, device_id=partner, device_id_type=MESH)
    pl.semaphore_wait(barrier, len(partners))
    loads[0].wait()

    started = []
    own = (tx, t, s)

    both = slice(None)

    def part(plane, piece):
        i, j, k = piece
        return all_ref.at[k, plane, i, j], recv_sem.at[0, k, i, j]

    def send(plane, piece, device):
        slot, arrived = part(plane, piece)
        copy = pltpu.make_async_remote_copy(
            src_ref=spec_ref if piece is own else slot,
            dst_ref=slot,
            send_sem=send_sem.at[len(started)],
            recv_sem=arrived,
            device_id=device,
            device_id_type=MESH,
        )
        copy.start()
        started.append(copy)

    def arrive(plane, piece):
        slot, arrived = part(plane, piece)
        pltpu.make_async_remote_copy(
            src_ref=slot,
            dst_ref=slot,
            send_sem=send_sem.at[0],
            recv_sem=arrived,
            device_id=across,
            device_id_type=MESH,
        ).wait_recv()

    def spread(piece):
        for i, k in hood:
            send(both, piece, {"tx": 2 * i + core, "ty": t, "src": k})

    for j in far_t:
        send(both, own, along_ty(j))
    spread(own)
    send(both, own, across)

    side = []
    for n, i in enumerate(far_s):
        for m, (src, dst) in enumerate(((shift_ref, shifts_ref), (weight_ref, weights_ref))):
            copy = pltpu.make_async_remote_copy(
                src_ref=src,
                dst_ref=dst.at[s],
                send_sem=side_send.at[m, n],
                recv_sem=side_recv.at[m, s],
                device_id=along_src(i),
                device_id_type=MESH,
            )
            copy.start()
            side.append(copy)

    for load in loads[1:]:
        load.wait()
    for plane in range(2):
        all_ref[s, plane, tx, t] = spec_ref[plane]
    block = tx * src_count + s
    blocks = tx_count * src_count
    row_table(row_ref, blend_ref.shape[2] // blocks, block, blocks)
    col_table(col_ref, t)
    half = pupil_ref.shape[0] // 2
    pupil = pupil_ref[...].astype(jnp.float32).astype(jnp.bfloat16)
    turned = (((1,), (1,)), ((), ()))
    mask_ref[:half] = lax.dot_general(unit(half, False), pupil[:, half:], turned, preferred_element_type=jnp.float32).astype(jnp.bfloat16)
    mask_ref[half:] = lax.dot_general(unit(half, True), pupil[:, :half], turned, preferred_element_type=jnp.float32).astype(jnp.bfloat16)

    part_rows, part_cols = ty_count * spec_ref.shape[1], spec_ref.shape[2]

    def turn(i, k):
        cell = jnp.concatenate([all_ref[k, plane, i].reshape(part_rows, part_cols) for plane in range(2)], axis=0)
        for back, target in enumerate((turned_ref, mirror_ref)):
            start = (src_count - 1 - k if back else k) * part_cols
            rows = pl.ds(pl.multiple_of(start, part_cols), part_cols)
            value = lax.dot_general(unit(part_cols, back), cell, turned, preferred_element_type=jnp.float32)
            for plane in range(2):
                tile = value[:, plane * part_rows : (plane + 1) * part_rows]
                target[plane * tx_count + i, rows] = tile
                target[(plane + 2) * tx_count + i, rows] = -tile

    def pass_on(i, j, k, also=None):
        piece = (2 * i + core, j, k)
        arrive(both, piece)
        if also is not None:
            send(both, piece, along_ty(also))
        send(both, piece, across)

    mate, far_t = far_t[0], far_t[1:]
    near, distant = hood[1:], hood[:1]
    for i, k in near:
        pass_on(i, t, k, mate)
    for n, j in enumerate(far_t):
        arrive(both, (tx, j, s))
        spread((tx, j, s))
        if n == 0:
            for i, k in distant:
                pass_on(i, t, k, mate)
    for j in [mate] + far_t:
        if j is mate:
            arrive(both, (tx, j, s))
        send(both, (tx, j, s), across)
    turn(tx, s)
    blend_table(blend_ref, block, blocks)
    for i, k in near + distant:
        pass_on(i, mate, k)
    for j in far_t:
        for i, k in near + distant:
            pass_on(i, j, k)
    for i, k in near + distant:
        turn(2 * i + core, k)
    near_first = [t, mate] + far_t
    for n, i in enumerate(far_s):
        for m, (src, dst) in enumerate(((shift_ref, shifts_ref), (weight_ref, weights_ref))):
            pltpu.make_async_remote_copy(
                src_ref=src,
                dst_ref=dst.at[i],
                send_sem=side_send.at[m, n],
                recv_sem=side_recv.at[m, i],
                device_id=across,
                device_id_type=MESH,
            ).wait_recv()
    list_live(live_ref, shifts_ref, weights_ref)
    for i in [pair] + far_pair:
        for k in [s] + far_s:
            for j in near_first:
                arrive(both, (2 * i + other_core, j, k))
            turn(2 * i + other_core, k)
    for copy in started + side:
        copy.wait_send()


def gather(spectrum, source_shifts, source_weights, pupil_mask, sizes, cols):
    tx_count, ty_count, src_count = sizes
    pair_count = tx_count // 2
    _, block_rows, block_cols = spectrum.shape
    slots = source_weights.shape[0]
    length = pupil_mask.shape[0]
    blocks = tx_count * src_count
    samples = 2 * length
    width = pl.cdiv(src_count * slots + (UNROLL + TAIL + 2) * GROUP + 1, LANES) * LANES
    vmem = pl.BlockSpec(memory_space=pltpu.VMEM)
    lines = pair_count * src_count * ty_count
    sends = ty_count - 1 + lines + ty_count * (src_count - 1 + pair_count - 1)
    sends += 3 * ty_count * (src_count - 1) * (pair_count - 1)
    return pl.pallas_call(
        functools.partial(gather_kernel, sizes),
        out_shape=(
            jax.ShapeDtypeStruct((4 * tx_count, src_count * block_cols, ty_count * block_rows), jnp.float32),
            jax.ShapeDtypeStruct((4 * tx_count, src_count * block_cols, ty_count * block_rows), jnp.float32),
            jax.ShapeDtypeStruct((1, width), jnp.int32),
            jax.ShapeDtypeStruct((GROUP * length, 2 * LANES), jnp.bfloat16),
            jax.ShapeDtypeStruct((cols, length), jnp.bfloat16),
            jax.ShapeDtypeStruct((length, length), jnp.bfloat16),
            jax.ShapeDtypeStruct((2, FRAME // blocks + 2 * EDGE, samples), jnp.bfloat16),
        ),
        in_specs=[pl.BlockSpec(memory_space=pltpu.HBM)] * 4,
        out_specs=(vmem,) * 7,
        scratch_shapes=[
            pltpu.VMEM((src_count, 2, slots), jnp.int32),
            pltpu.VMEM((src_count, 1, slots), jnp.int32),
            pltpu.VMEM((src_count, 2, tx_count, ty_count, block_rows, block_cols), jnp.bfloat16),
            pltpu.VMEM(spectrum.shape, jnp.bfloat16),
            pltpu.VMEM(pupil_mask.shape, jnp.int32),
            pltpu.SemaphoreType.DMA((4,)),
            pltpu.SemaphoreType.DMA((sends,)),
            pltpu.SemaphoreType.DMA((2, src_count, tx_count, ty_count)),
            pltpu.SemaphoreType.DMA((2, src_count)),
            pltpu.SemaphoreType.DMA((2, src_count)),
        ],
        compiler_params=pltpu.CompilerParams(collective_id=0, has_side_effects=True, vmem_limit_bytes=24 << 20),
        name="gather",
    )(*(pltpu.with_memory_space_constraint(a, pltpu.HBM) for a in (spectrum, source_shifts.T, source_weights[None], pupil_mask)))


def stages(sizes, spec, mirror, mask_ref, row_ref, col_ref, live):
    half = col_ref.shape[1] // 2
    height = spec.shape[1]
    tiles = spec.shape[0] // 4
    block = lax.axis_index("tx") * sizes[2] + lax.axis_index("src")
    power = lax.rem(block, 4)
    flip = 2 * lax.rem(power, 2)
    middle = (lax.rem(4 - power, 4), power + 1 - 2 * lax.rem(power, 2))
    lane = iota((half, LANES), 1)
    first_half = iota((1, LANES), 1) < LANES // 2

    def cross(n, slot):
        total = [[], []]
        for g in range(GROUP):
            word = live[0, (n + 1) * GROUP + g]
            a, b = word & 1023, (word >> 10) & 1023
            tile, rest = a // LANES, lax.rem(a, LANES)
            keep = lane >= rest
            last = jnp.minimum(tile + 2, tiles - 1)

            def window(source, start, part):
                rows = pl.ds(start, half)
                low = pltpu.roll(mask_ref[part * half : (part + 1) * half, :LANES], rest, 1)
                high = pltpu.roll(mask_ref[part * half : (part + 1) * half, LANES:], rest, 1)
                ends = jnp.where(keep, low, high)
                centre = jnp.where(keep, high, low)
                found = []
                for plane in range(2):
                    outer = jnp.where(keep, source[plane * tiles + tile, rows, :], source[(plane + flip) * tiles + last, rows, :])
                    between = source[middle[plane] * tiles + tile + 1, rows, :]
                    found.append(outer.astype(jnp.bfloat16) * ends + between.astype(jnp.bfloat16) * centre)
                return found

            upper = window(spec, b + half, 0)
            lower = window(mirror, height - half - b, 1)
            total[0].append(jnp.concatenate([upper[0] + lower[0], upper[1] + lower[1]], axis=1))
            total[1].append(jnp.concatenate([lower[1] - upper[1], upper[0] - lower[0]], axis=1))
        for n in range(2):
            slot[n * half : (n + 1) * half] = dot(jnp.concatenate(total[n], axis=1), row_ref[...]).astype(jnp.bfloat16)

    def square(n, source, acc):
        pair = [(live[0, (n + 1) * GROUP + g] >> 20).astype(jnp.float32) for g in range(GROUP)]
        scale = jnp.where(first_half, pair[0], pair[1])
        tall = col_ref.shape[0] // 2
        for part in range(2):
            rows = slice(part * tall, (part + 1) * tall)
            wide = dot(col_ref[rows], source[...])
            real, imag = wide[:, :LANES], wide[:, LANES:]
            acc[rows] += scale * (real * real + imag * imag)

    return cross, square


def image_kernel(
    sizes, live_ref, spec, mirror, mask_ref, row_ref, col_ref, acc, next_inner,
    live, other_inner, live_sem,
):
    load = pltpu.make_async_copy(live_ref, live, live_sem)
    load.start()
    cross, square = stages(sizes, spec, mirror, mask_ref, row_ref, col_ref, live)
    inner = (other_inner, next_inner)
    acc[...] = jnp.zeros_like(acc)
    next_inner[...] = jnp.zeros_like(next_inner)
    load.wait()

    def turn_body(turn_index, carry):
        for g in range(UNROLL):
            n = turn_index * UNROLL + g
            cross(n, inner[g % 2])
            square(n - 1, inner[1 - g % 2], acc)
        return carry

    lax.fori_loop(0, turns_before_tail(live), turn_body, 0)


def image(live, spectrum, mirror, row_table, col_table, masks, sizes):
    cols, length = col_table.shape
    vmem = pl.BlockSpec(memory_space=pltpu.VMEM)
    return pl.pallas_call(
        functools.partial(image_kernel, sizes),
        out_shape=(
            jax.ShapeDtypeStruct((cols, LANES), jnp.float32),
            jax.ShapeDtypeStruct((length, 2 * LANES), jnp.bfloat16),
        ),
        in_specs=[vmem] * 6,
        out_specs=(vmem,) * 2,
        scratch_shapes=[
            pltpu.SMEM(live.shape, jnp.int32),
            pltpu.VMEM((length, 2 * LANES), jnp.bfloat16),
            pltpu.SemaphoreType.DMA(()),
        ],
        compiler_params=pltpu.CompilerParams(vmem_limit_bytes=12 << 20),
        name="image",
    )(live, spectrum, mirror, masks, row_table, col_table)


def exchange_kernel(
    sizes, sources, live_ref, acc, first_inner, spec, mirror, mask_ref, row_ref, col_ref, all_ref, beside,
    live, total, own_ref, strip_ref, inner, live_sem, send_sem, recv_sem, side_send, side_recv,
):
    tx_count, ty_count, src_count = sizes
    pair_count = tx_count // 2
    tx, t, s = lax.axis_index("tx"), lax.axis_index("ty"), lax.axis_index("src")
    pair, core = tx // 2, lax.rem(tx, 2)
    far_s = [s] + others(s, src_count)
    far_pair = [pair] + others(pair, pair_count)
    chips = [(i, k) for k in far_s for i in far_pair]

    def device(chip, other, z):
        return {"tx": 2 * chip[0] + (1 - core if other else core), "ty": z, "src": chip[1]}

    def block(chip, other):
        return (2 * chip[0] + (1 - core if other else core)) * src_count + chip[1]

    across = device(chips[0], True, t)
    barrier = pltpu.get_barrier_semaphore()

    def greet(chip, z):
        pl.semaphore_signal(barrier, inc=1, device_id=device(chip, False, z), device_id_type=MESH)

    load = pltpu.make_async_copy(live_ref, live, live_sem)
    load.start()
    has = (t > 0, t < ty_count - 1)
    beside[...] = jnp.zeros_like(beside)
    pl.semaphore_signal(barrier, inc=1, device_id=across, device_id_type=MESH)
    for chip in chips[1:]:
        greet(chip, t)
    for side in range(2):

        @pl.when(has[side])
        def _():
            for chip in chips:
                greet(chip, t + 2 * side - 1)

    cross, square = stages(sizes, spec, mirror, mask_ref, row_ref, col_ref, live)
    load.wait()
    n = turns_before_tail(live) * UNROLL
    total[...] = acc[...]
    source_inner = first_inner
    for g in range(TAIL):
        if g < TAIL - 1:
            cross(n + g, inner[g % 2])
        square(n + g - 1, source_inner, total)
        source_inner = inner[g % 2]

    level = total[...]
    cols = level.shape[0]
    count_x = own_ref.shape[0]
    level = (level + pltpu.roll(level, LANES // 2, 1)) / (2.0 * sources)
    own = level.T[:count_x].astype(jnp.bfloat16)
    own_ref[...] = own
    strip_ref[0] = level[:PACK, :count_x].astype(jnp.bfloat16)
    strip_ref[1] = level[cols - PACK :, :count_x].astype(jnp.bfloat16)
    all_ref[block(chips[0], False)] = own
    sides = jnp.minimum(t, 1) + jnp.minimum(ty_count - 1 - t, 1)
    pl.semaphore_wait(barrier, len(chips) * (1 + sides))

    def copy(src, dst, send, recv, target):
        return pltpu.make_async_remote_copy(
            src_ref=src, dst_ref=dst, send_sem=send, recv_sem=recv, device_id=target, device_id_type=MESH
        )

    def level_copy(n, chip, other, target, own=False):
        at = block(chip, other)
        return copy(own_ref if own else all_ref.at[at], all_ref.at[at], send_sem.at[n], recv_sem.at[at], target)

    def side_copy(n, side, chip, other, target, own=False):
        at = block(chip, other)
        slot = beside.at[side, at]
        return copy(strip_ref.at[1 - side] if own else slot, slot, side_send.at[side, n], side_recv.at[side, at], target)

    started = []
    for side in range(2):

        @pl.when(has[1 - side])
        def _():
            for n, chip in enumerate(chips):
                side_copy(n, side, chips[0], False, device(chip, False, t + 1 - 2 * side), True).start()

    for n, chip in enumerate(chips[:0:-1]):
        started.append(level_copy(n, chips[0], False, device(chip, False, t), True))
        started[-1].start()
    n = len(chips) - 1
    started.append(level_copy(n, chips[0], False, across, True))
    started[-1].start()
    for chip in chips[1:]:
        n += 1
        level_copy(0, chip, False, across).wait_recv()
        started.append(level_copy(n, chip, False, across))
        started[-1].start()
    for side in range(2):

        @pl.when(has[side])
        def _():
            for n, chip in enumerate(chips):
                side_copy(0, side, chip, False, across).wait_recv()
                side_copy(len(chips) + n, side, chip, False, across).start()

    for chip in chips:
        level_copy(0, chip, True, across).wait_recv()
    for side in range(2):

        @pl.when(has[side])
        def _():
            for n, chip in enumerate(chips):
                side_copy(0, side, chip, True, across).wait_recv()
                side_copy(len(chips) + n, side, chip, False, across).wait_send()

        @pl.when(has[1 - side])
        def _():
            for n, chip in enumerate(chips):
                side_copy(n, side, chips[0], False, device(chip, False, t + 1 - 2 * side), True).wait_send()

    for one in started:
        one.wait_send()


def exchange(sources, live, acc, inner, spectrum, mirror, masks, row_table, col_table, count_x, sizes):
    tx_count, ty_count, src_count = sizes
    blocks = tx_count * src_count
    vmem = pl.BlockSpec(memory_space=pltpu.VMEM)
    cols = acc.shape[0]
    return pl.pallas_call(
        functools.partial(exchange_kernel, sizes, sources),
        out_shape=(
            jax.ShapeDtypeStruct((blocks, count_x, cols), jnp.bfloat16),
            jax.ShapeDtypeStruct((2, blocks, PACK, count_x), jnp.bfloat16),
        ),
        in_specs=[vmem] * 8,
        out_specs=(vmem,) * 2,
        scratch_shapes=[
            pltpu.SMEM(live.shape, jnp.int32),
            pltpu.VMEM(acc.shape, jnp.float32),
            pltpu.VMEM((count_x, cols), jnp.bfloat16),
            pltpu.VMEM((2, PACK, count_x), jnp.bfloat16),
            [pltpu.VMEM(inner.shape, jnp.bfloat16)] * 2,
            pltpu.SemaphoreType.DMA(()),
            pltpu.SemaphoreType.DMA((blocks,)),
            pltpu.SemaphoreType.DMA((blocks,)),
            pltpu.SemaphoreType.DMA((2, blocks)),
            pltpu.SemaphoreType.DMA((2, blocks)),
        ],
        compiler_params=pltpu.CompilerParams(collective_id=1, has_side_effects=True, vmem_limit_bytes=12 << 20),
        name="exchange",
    )(live, acc, inner, spectrum, mirror, masks, row_table, col_table)


def diffuse_kernel(sizes, all_ref, beside, blend_ref, out_ref):
    tx_count, ty_count, src_count = sizes
    rows, cols = out_ref.shape
    blocks, count, _ = all_ref.shape
    samples = blocks * count
    tall = rows + 2 * EDGE
    level = all_ref[...].reshape(samples, cols)
    sides = [jnp.concatenate([beside[side, n] for n in range(blocks)], axis=1) for side in range(2)]
    strip = jnp.concatenate([sides[1], jnp.zeros((LANES - 2 * PACK, samples), jnp.bfloat16), sides[0]], axis=0)
    turned = (((1,), (1,)), ((), ()))
    middle = dot(blend_ref[0], level) + dot(blend_ref[1], level)
    edge = lax.dot_general(blend_ref[0], strip, turned, preferred_element_type=jnp.float32)
    edge += lax.dot_general(blend_ref[1], strip, turned, preferred_element_type=jnp.float32)
    acid = 1.0 - jnp.exp(-jnp.concatenate([middle, edge], axis=1))
    wide = cols + LANES
    row_block = lax.axis_index("tx") * src_count + lax.axis_index("src")
    col_block = lax.axis_index("ty")
    x = row_block * rows - EDGE + iota(acid.shape, 0)
    column = iota(acid.shape, 1)
    y = col_block * cols + jnp.where(column >= cols + LANES // 2, column - wide, column)
    inside = (x >= 0) & (x < blocks * rows) & (y >= 0) & (y < ty_count * cols)
    for repeat in range(2):
        acid = jnp.where(inside, acid, 0.0)
        near = (
            pltpu.roll(acid, 1, 0)
            + pltpu.roll(acid, tall - 1, 0)
            + pltpu.roll(acid, 1, 1)
            + pltpu.roll(acid, wide - 1, 1)
        )
        acid = acid + diffusion_rate * (near - 4.0 * acid)
    out_ref[...] = acid[EDGE : EDGE + rows, :cols]


def diffuse(levels, beside, blend, sizes):
    rows = blend.shape[1] - 2 * EDGE
    vmem = pl.BlockSpec(memory_space=pltpu.VMEM)
    return pl.pallas_call(
        functools.partial(diffuse_kernel, sizes),
        out_shape=jax.ShapeDtypeStruct((rows, levels.shape[2]), jnp.float32),
        in_specs=[vmem] * 3,
        out_specs=vmem,
        compiler_params=pltpu.CompilerParams(vmem_limit_bytes=12 << 20),
        name="diffuse",
    )(levels, beside, blend)


def body(sizes, cols, spectrum, pupil_mask, source_shifts, source_weights):
    turned, mirror, live, row_table, col_table, masks, blend = gather(
        spectrum, source_shifts, source_weights, pupil_mask, sizes, cols
    )
    sources = source_weights.shape[0] * sizes[2]
    count_x = blend.shape[2] // (sizes[0] * sizes[2])
    acc, inner = image(live, turned, mirror, row_table, col_table, masks, sizes)
    levels, beside = exchange(
        sources, live, acc, inner, turned, mirror, masks, row_table, col_table, count_x, sizes
    )
    return diffuse(levels, beside, blend, sizes)


def solution(mesh):
    sizes = (mesh.shape["tx"], mesh.shape["ty"], mesh.shape["src"])
    placed = (P(None, ("tx", "ty"), "src"), P(), P("src", None), P("src"))
    return jax.shard_map(
        functools.partial(body, sizes, COLS),
        mesh=mesh,
        in_specs=placed,
        out_specs=P(("tx", "src"), "ty"),
        check_vma=False,
    )
```

```python
import functools
import math

import jax
import jax.numpy as jnp
from jax import lax
from jax.experimental import pallas as pl
from jax.experimental.pallas import tpu as pltpu
from jax.sharding import PartitionSpec as P

FRAME = 2048
LANES = 128
COLS = 256
EDGE = 8
PACK = 16
GROUP = 2
UNROLL = 4
TAIL = 12
MESH = pl.DeviceIdType.MESH

diffusion_rate = 0.2


def wave(turns, period):
    quarter = period // 4
    turn = (turns + quarter // 2) // quarter
    angle = (turns - turn * quarter).astype(jnp.float32) * (2 * math.pi / period)
    square = angle * angle
    sine = angle * (1 + square * (-1 / 6 + square * (1 / 120 + square * (-1 / 5040 + square / 362880))))
    cosine = 1 + square * (-1 / 2 + square * (1 / 24 + square * (-1 / 720 + square / 40320)))
    odd = (turn & 1) == 1
    first, second = jnp.where(odd, sine, cosine), jnp.where(odd, cosine, sine)
    return jnp.where(((turn + 1) & 2) == 2, -first, first), jnp.where((turn & 2) == 2, -second, second)


def iota(shape, dim):
    return lax.broadcasted_iota(jnp.int32, shape, dim)


def dot(a, b):
    return jnp.dot(a, b, preferred_element_type=jnp.float32)


def unit(size, back):
    rows, cols = iota((size, size), 0), iota((size, size), 1)
    return jnp.where(rows + cols == size - 1 if back else rows == cols, 1.0, 0.0).astype(jnp.bfloat16)


def flip_bits(index, mask):
    bit = 1
    while bit <= mask:
        if mask & bit:
            index = index + bit * (1 - 2 * lax.rem(index // bit, 2))
        bit *= 2
    return index


def others(index, count):
    if count & (count - 1) == 0:
        return [flip_bits(index, d) for d in range(1, count)]
    return [lax.rem(index + d, count) for d in range(1, count)]


def mates(index, count):
    orders = [
        sorted((i for i in range(count) if i != at), key=lambda i: (i != at ^ 1, abs(i - at), i)) for at in range(count)
    ]
    return [sum(jnp.where(index == at, orders[at][n], 0) for at in range(count)) for n in range(count - 1)]


def row_table(row_ref, count, block, blocks):
    half = row_ref.shape[0] // (2 * GROUP)
    each = LANES // GROUP
    step = FRAME // (count * blocks)
    sample = iota((half, each), 1)
    x = step * (blocks * sample + block)
    cosine, sine = wave((x * iota((half, each), 0)) & (FRAME - 1), FRAME)
    cosine = jnp.where(sample < count, cosine, 0.0)
    sine = jnp.where(sample < count, sine, 0.0)
    none = jnp.zeros((half, each), jnp.float32)
    for g in range(GROUP):
        for part, (real, imag) in enumerate(((cosine, sine), (-sine, cosine))):
            row = [real if n == g else none for n in range(GROUP)] + [imag if n == g else none for n in range(GROUP)]
            at = (2 * g + part) * half
            row_ref[at : at + half] = jnp.concatenate(row, axis=1).astype(jnp.bfloat16)


def col_table(col_ref, t):
    cols, half = col_ref.shape[0], col_ref.shape[1] // 2
    chunk = 64

    def fill(n, carry):
        start = pl.multiple_of(n * chunk, chunk)
        y = t * cols + start + iota((chunk, half), 0)
        cosine, sine = wave((y * (2 * iota((chunk, half), 1) + 1)) & (2 * FRAME - 1), 2 * FRAME)
        col_ref[pl.ds(start, chunk), :half] = cosine.astype(jnp.bfloat16)
        col_ref[pl.ds(start, chunk), half:] = sine.astype(jnp.bfloat16)
        return carry

    lax.fori_loop(0, cols // chunk, fill, 0)


def list_live(live_ref, shifts_ref, weights_ref):
    src_count, _, slots = shifts_ref.shape
    width = live_ref.shape[1]
    weights = weights_ref[:, 0, :].astype(jnp.float32)
    words = shifts_ref[:, 0, :].astype(jnp.float32) + shifts_ref[:, 1, :].astype(jnp.float32) * 1024.0 + weights * 1048576.0
    on = jnp.where(weights > 0, 1.0, 0.0)
    ahead = jnp.where(iota((slots, slots), 0) < iota((slots, slots), 1), 1.0, 0.0)
    rank = dot(on.astype(jnp.bfloat16), ahead.astype(jnp.bfloat16))
    before = jnp.zeros((1, 1), jnp.float32)
    ranks = []
    for k in range(src_count):
        ranks.append(rank[k : k + 1] + before)
        before = before + jnp.sum(on[k : k + 1], axis=1, keepdims=True)
    rank = jnp.where(on > 0, jnp.concatenate(ranks, axis=0), -1.0).T
    words = words.T
    place = (iota((slots, width), 1) - GROUP).astype(jnp.float32)
    total = jnp.zeros((slots, width), jnp.float32)
    for k in range(src_count):
        total += jnp.where(rank[:, k : k + 1] == place, words[:, k : k + 1], 0.0)
    found = jnp.sum(total, axis=0, keepdims=True)
    live_ref[...] = jnp.where(iota((1, width), 1) == width - 1, before, found).astype(jnp.int32)


def turns_before_tail(live):
    steps = (live[0, live.shape[1] - 1] + GROUP - 1) // GROUP + 1 - TAIL
    return jnp.maximum(steps + UNROLL - 1, 0) // UNROLL


def blend_table(blend_ref, block, blocks):
    tall, samples = blend_ref.shape
    rows = tall - 2 * EDGE
    step = FRAME // samples
    count = samples // blocks
    chunk = PACK

    def fill(n, carry):
        start = pl.multiple_of(n * chunk, chunk)
        x = block * rows - EDGE + start + iota((chunk, samples), 0)
        column = iota((chunk, samples), 1)
        owner = column // count
        gap = x - step * (blocks * (column - owner * count) + owner)
        gap = ((gap + FRAME // 2) & (FRAME - 1)) - FRAME // 2
        cosine, sine = wave(gap, 2 * FRAME)
        place = block * rows - EDGE + start + iota((chunk, 1), 0)
        place = place & (2 * step - 1)
        scale = jnp.zeros((chunk, 1), jnp.float32)
        for n in range(2 * step):
            if n % step:
                scale = jnp.where(place == n, math.sin(math.pi * n / step) / samples, scale)
        scale = jnp.where((owner & 1) == 1, -scale, scale)
        here = gap == 0
        table = jnp.where(here, 1.0, scale * cosine / jnp.where(here, 1.0, sine))
        blend_ref[pl.ds(start, chunk)] = table.astype(jnp.bfloat16)
        return carry

    lax.fori_loop(0, tall // chunk, fill, 0)


def gather_kernel(
    sizes, spec_hbm, shift_ref, weight_ref, pupil_hbm, turned_ref, mirror_ref, live_ref, row_ref, col_ref, mask_ref, blend_ref,
    shifts_ref, weights_ref, all_ref, spec_ref, pupil_ref, local_sem, send_sem, recv_sem, side_send, side_recv,
):
    tx_count, ty_count, src_count = sizes
    pair_count = tx_count // 2
    tx, t, s = lax.axis_index("tx"), lax.axis_index("ty"), lax.axis_index("src")
    pair, core = tx // 2, lax.rem(tx, 2)
    other_core = 1 - core
    far_t = mates(t, ty_count)
    far_s = others(s, src_count)
    far_pair = others(pair, pair_count)

    def along_ty(i):
        return {"tx": tx, "ty": i, "src": s}

    def along_src(i):
        return {"tx": tx, "ty": t, "src": i}

    loads = [
        pltpu.make_async_copy(src, dst, local_sem.at[n])
        for n, (src, dst) in enumerate(
            (
                (spec_hbm, spec_ref),
                (pupil_hbm, pupil_ref),
                (shift_ref, shifts_ref.at[s]),
                (weight_ref, weights_ref.at[s]),
            )
        )
    ]
    for load in loads:
        load.start()

    across = {"tx": 2 * pair + other_core, "ty": t, "src": s}
    hood = [(i, k) for k in far_s + [s] for i in far_pair + [pair] if i is not pair or k is not s]
    partners = [along_ty(i) for i in far_t] + [{"tx": 2 * i + core, "ty": t, "src": k} for i, k in hood] + [across]
    barrier = pltpu.get_barrier_semaphore()
    for partner in partners:
        pl.semaphore_signal(barrier, inc=1, device_id=partner, device_id_type=MESH)
    pl.semaphore_wait(barrier, len(partners))
    loads[0].wait()

    started = []
    own = (tx, t, s)

    both = slice(None)

    def part(plane, piece):
        i, j, k = piece
        return all_ref.at[k, plane, i, j], recv_sem.at[0, k, i, j]

    def send(plane, piece, device):
        slot, arrived = part(plane, piece)
        copy = pltpu.make_async_remote_copy(
            src_ref=spec_ref if piece is own else slot,
            dst_ref=slot,
            send_sem=send_sem.at[len(started)],
            recv_sem=arrived,
            device_id=device,
            device_id_type=MESH,
        )
        copy.start()
        started.append(copy)

    def arrive(plane, piece):
        slot, arrived = part(plane, piece)
        pltpu.make_async_remote_copy(
            src_ref=slot,
            dst_ref=slot,
            send_sem=send_sem.at[0],
            recv_sem=arrived,
            device_id=across,
            device_id_type=MESH,
        ).wait_recv()

    def spread(piece):
        for i, k in hood:
            send(both, piece, {"tx": 2 * i + core, "ty": t, "src": k})

    for j in far_t:
        send(both, own, along_ty(j))
    spread(own)
    send(both, own, across)

    side = []
    for n, i in enumerate(far_s):
        for m, (src, dst) in enumerate(((shift_ref, shifts_ref), (weight_ref, weights_ref))):
            copy = pltpu.make_async_remote_copy(
                src_ref=src,
                dst_ref=dst.at[s],
                send_sem=side_send.at[m, n],
                recv_sem=side_recv.at[m, s],
                device_id=along_src(i),
                device_id_type=MESH,
            )
            copy.start()
            side.append(copy)

    for load in loads[1:]:
        load.wait()
    for plane in range(2):
        all_ref[s, plane, tx, t] = spec_ref[plane]
    block = tx * src_count + s
    blocks = tx_count * src_count
    row_table(row_ref, blend_ref.shape[1] // blocks, block, blocks)
    col_table(col_ref, t)
    half = pupil_ref.shape[0] // 2
    pupil = pupil_ref[...].astype(jnp.float32).astype(jnp.bfloat16)
    turned = (((1,), (1,)), ((), ()))
    mask_ref[:half] = lax.dot_general(unit(half, False), pupil[:, half:], turned, preferred_element_type=jnp.float32).astype(jnp.bfloat16)
    mask_ref[half:] = lax.dot_general(unit(half, True), pupil[:, :half], turned, preferred_element_type=jnp.float32).astype(jnp.bfloat16)

    part_rows, part_cols = ty_count * spec_ref.shape[1], spec_ref.shape[2]

    def turn(i, k):
        cell = jnp.concatenate([all_ref[k, plane, i].reshape(part_rows, part_cols) for plane in range(2)], axis=0)
        for back, target in enumerate((turned_ref, mirror_ref)):
            start = (src_count - 1 - k if back else k) * part_cols
            rows = pl.ds(pl.multiple_of(start, part_cols), part_cols)
            value = lax.dot_general(unit(part_cols, back), cell, turned, preferred_element_type=jnp.float32)
            for plane in range(2):
                tile = value[:, plane * part_rows : (plane + 1) * part_rows]
                target[plane * tx_count + i, rows] = tile
                target[(plane + 2) * tx_count + i, rows] = -tile

    def pass_on(i, j, k, also=None):
        piece = (2 * i + core, j, k)
        arrive(both, piece)
        if also is not None:
            send(both, piece, along_ty(also))
        send(both, piece, across)

    mate, far_t = far_t[0], far_t[1:]
    near, distant = hood[1:], hood[:1]
    for i, k in near:
        pass_on(i, t, k, mate)
    for n, j in enumerate(far_t):
        arrive(both, (tx, j, s))
        spread((tx, j, s))
        if n == 0:
            for i, k in distant:
                pass_on(i, t, k, mate)
    for j in [mate] + far_t:
        if j is mate:
            arrive(both, (tx, j, s))
        send(both, (tx, j, s), across)
    turn(tx, s)
    blend_table(blend_ref, block, blocks)
    for i, k in near + distant:
        pass_on(i, mate, k)
    for j in far_t:
        for i, k in near + distant:
            pass_on(i, j, k)
    for i, k in near + distant:
        turn(2 * i + core, k)
    near_first = [t, mate] + far_t
    for n, i in enumerate(far_s):
        for m, (src, dst) in enumerate(((shift_ref, shifts_ref), (weight_ref, weights_ref))):
            pltpu.make_async_remote_copy(
                src_ref=src,
                dst_ref=dst.at[i],
                send_sem=side_send.at[m, n],
                recv_sem=side_recv.at[m, i],
                device_id=across,
                device_id_type=MESH,
            ).wait_recv()
    list_live(live_ref, shifts_ref, weights_ref)
    for i in [pair] + far_pair:
        for k in [s] + far_s:
            for j in near_first:
                arrive(both, (2 * i + other_core, j, k))
            turn(2 * i + other_core, k)
    for copy in started + side:
        copy.wait_send()


def gather(spectrum, source_shifts, source_weights, pupil_mask, sizes, cols):
    tx_count, ty_count, src_count = sizes
    pair_count = tx_count // 2
    _, block_rows, block_cols = spectrum.shape
    slots = source_weights.shape[0]
    length = pupil_mask.shape[0]
    blocks = tx_count * src_count
    samples = 2 * length
    width = pl.cdiv(src_count * slots + (UNROLL + TAIL + 2) * GROUP + 1, LANES) * LANES
    vmem = pl.BlockSpec(memory_space=pltpu.VMEM)
    lines = pair_count * src_count * ty_count
    sends = ty_count - 1 + lines + ty_count * (src_count - 1 + pair_count - 1)
    sends += 3 * ty_count * (src_count - 1) * (pair_count - 1)
    return pl.pallas_call(
        functools.partial(gather_kernel, sizes),
        out_shape=(
            jax.ShapeDtypeStruct((4 * tx_count, src_count * block_cols, ty_count * block_rows), jnp.float32),
            jax.ShapeDtypeStruct((4 * tx_count, src_count * block_cols, ty_count * block_rows), jnp.float32),
            jax.ShapeDtypeStruct((1, width), jnp.int32),
            jax.ShapeDtypeStruct((GROUP * length, 2 * LANES), jnp.bfloat16),
            jax.ShapeDtypeStruct((cols, length), jnp.bfloat16),
            jax.ShapeDtypeStruct((length, length), jnp.bfloat16),
            jax.ShapeDtypeStruct((FRAME // blocks + 2 * EDGE, samples), jnp.bfloat16),
        ),
        in_specs=[pl.BlockSpec(memory_space=pltpu.HBM)] * 4,
        out_specs=(vmem,) * 7,
        scratch_shapes=[
            pltpu.VMEM((src_count, 2, slots), jnp.int32),
            pltpu.VMEM((src_count, 1, slots), jnp.int32),
            pltpu.VMEM((src_count, 2, tx_count, ty_count, block_rows, block_cols), jnp.bfloat16),
            pltpu.VMEM(spectrum.shape, jnp.bfloat16),
            pltpu.VMEM(pupil_mask.shape, jnp.int32),
            pltpu.SemaphoreType.DMA((4,)),
            pltpu.SemaphoreType.DMA((sends,)),
            pltpu.SemaphoreType.DMA((2, src_count, tx_count, ty_count)),
            pltpu.SemaphoreType.DMA((2, src_count)),
            pltpu.SemaphoreType.DMA((2, src_count)),
        ],
        compiler_params=pltpu.CompilerParams(collective_id=0, has_side_effects=True, vmem_limit_bytes=24 << 20),
        name="gather",
    )(*(pltpu.with_memory_space_constraint(a, pltpu.HBM) for a in (spectrum, source_shifts.T, source_weights[None], pupil_mask)))


def stages(sizes, spec, mirror, mask_ref, row_ref, col_ref, live):
    half = col_ref.shape[1] // 2
    height = spec.shape[1]
    tiles = spec.shape[0] // 4
    block = lax.axis_index("tx") * sizes[2] + lax.axis_index("src")
    power = lax.rem(block, 4)
    flip = 2 * lax.rem(power, 2)
    middle = (lax.rem(4 - power, 4), power + 1 - 2 * lax.rem(power, 2))
    lane = iota((half, LANES), 1)
    first_half = iota((1, LANES), 1) < LANES // 2

    def cross(n, slot):
        total = [[], []]
        for g in range(GROUP):
            word = live[0, (n + 1) * GROUP + g]
            a, b = word & 1023, (word >> 10) & 1023
            tile, rest = a // LANES, lax.rem(a, LANES)
            keep = lane >= rest
            last = jnp.minimum(tile + 2, tiles - 1)

            def window(source, start, part):
                rows = pl.ds(start, half)
                low = pltpu.roll(mask_ref[part * half : (part + 1) * half, :LANES], rest, 1)
                high = pltpu.roll(mask_ref[part * half : (part + 1) * half, LANES:], rest, 1)
                ends = jnp.where(keep, low, high)
                centre = jnp.where(keep, high, low)
                found = []
                for plane in range(2):
                    outer = jnp.where(keep, source[plane * tiles + tile, rows, :], source[(plane + flip) * tiles + last, rows, :])
                    between = source[middle[plane] * tiles + tile + 1, rows, :]
                    found.append(outer.astype(jnp.bfloat16) * ends + between.astype(jnp.bfloat16) * centre)
                return found

            upper = window(spec, b + half, 0)
            lower = window(mirror, height - half - b, 1)
            total[0].append(jnp.concatenate([upper[0] + lower[0], upper[1] + lower[1]], axis=1))
            total[1].append(jnp.concatenate([lower[1] - upper[1], upper[0] - lower[0]], axis=1))
        for n in range(2):
            slot[n * half : (n + 1) * half] = dot(jnp.concatenate(total[n], axis=1), row_ref[...]).astype(jnp.bfloat16)

    def square(n, source, acc):
        pair = [(live[0, (n + 1) * GROUP + g] >> 20).astype(jnp.float32) for g in range(GROUP)]
        scale = jnp.where(first_half, pair[0], pair[1])
        tall = col_ref.shape[0] // 2
        for part in range(2):
            rows = slice(part * tall, (part + 1) * tall)
            wide = dot(col_ref[rows], source[...])
            real, imag = wide[:, :LANES], wide[:, LANES:]
            acc[rows] += scale * (real * real + imag * imag)

    return cross, square


def image_kernel(
    sizes, live_ref, spec, mirror, mask_ref, row_ref, col_ref, acc, next_inner,
    live, other_inner, live_sem,
):
    load = pltpu.make_async_copy(live_ref, live, live_sem)
    load.start()
    cross, square = stages(sizes, spec, mirror, mask_ref, row_ref, col_ref, live)
    inner = (other_inner, next_inner)
    acc[...] = jnp.zeros_like(acc)
    next_inner[...] = jnp.zeros_like(next_inner)
    load.wait()

    def turn_body(turn_index, carry):
        for g in range(UNROLL):
            n = turn_index * UNROLL + g
            cross(n, inner[g % 2])
            square(n - 1, inner[1 - g % 2], acc)
        return carry

    lax.fori_loop(0, turns_before_tail(live), turn_body, 0)


def image(live, spectrum, mirror, row_table, col_table, masks, sizes):
    cols, length = col_table.shape
    vmem = pl.BlockSpec(memory_space=pltpu.VMEM)
    return pl.pallas_call(
        functools.partial(image_kernel, sizes),
        out_shape=(
            jax.ShapeDtypeStruct((cols, LANES), jnp.float32),
            jax.ShapeDtypeStruct((length, 2 * LANES), jnp.bfloat16),
        ),
        in_specs=[vmem] * 6,
        out_specs=(vmem,) * 2,
        scratch_shapes=[
            pltpu.SMEM(live.shape, jnp.int32),
            pltpu.VMEM((length, 2 * LANES), jnp.bfloat16),
            pltpu.SemaphoreType.DMA(()),
        ],
        compiler_params=pltpu.CompilerParams(vmem_limit_bytes=12 << 20),
        name="image",
    )(live, spectrum, mirror, masks, row_table, col_table)


def exchange_kernel(
    sizes, sources, live_ref, acc, first_inner, spec, mirror, mask_ref, row_ref, col_ref, all_ref, beside,
    live, total, own_ref, strip_ref, inner, live_sem, send_sem, recv_sem, side_send, side_recv,
):
    tx_count, ty_count, src_count = sizes
    pair_count = tx_count // 2
    tx, t, s = lax.axis_index("tx"), lax.axis_index("ty"), lax.axis_index("src")
    pair, core = tx // 2, lax.rem(tx, 2)
    far_s = [s] + others(s, src_count)
    far_pair = [pair] + others(pair, pair_count)
    chips = [(i, k) for k in far_s for i in far_pair]

    def device(chip, other, z):
        return {"tx": 2 * chip[0] + (1 - core if other else core), "ty": z, "src": chip[1]}

    def block(chip, other):
        return (2 * chip[0] + (1 - core if other else core)) * src_count + chip[1]

    across = device(chips[0], True, t)
    barrier = pltpu.get_barrier_semaphore()

    def greet(chip, z):
        pl.semaphore_signal(barrier, inc=1, device_id=device(chip, False, z), device_id_type=MESH)

    load = pltpu.make_async_copy(live_ref, live, live_sem)
    load.start()
    has = (t > 0, t < ty_count - 1)
    beside[...] = jnp.zeros_like(beside)
    pl.semaphore_signal(barrier, inc=1, device_id=across, device_id_type=MESH)
    for chip in chips[1:]:
        greet(chip, t)
    for side in range(2):

        @pl.when(has[side])
        def _():
            for chip in chips:
                greet(chip, t + 2 * side - 1)

    cross, square = stages(sizes, spec, mirror, mask_ref, row_ref, col_ref, live)
    load.wait()
    n = turns_before_tail(live) * UNROLL
    total[...] = acc[...]
    source_inner = first_inner
    for g in range(TAIL):
        if g < TAIL - 1:
            cross(n + g, inner[g % 2])
        square(n + g - 1, source_inner, total)
        source_inner = inner[g % 2]

    level = total[...]
    cols = level.shape[0]
    count_x = own_ref.shape[0]
    level = (level + pltpu.roll(level, LANES // 2, 1)) / (2.0 * sources)
    own = level.T[:count_x].astype(jnp.bfloat16)
    own_ref[...] = own
    strip_ref[0] = level[:PACK, :count_x].astype(jnp.bfloat16)
    strip_ref[1] = level[cols - PACK :, :count_x].astype(jnp.bfloat16)
    all_ref[block(chips[0], False)] = own
    sides = jnp.minimum(t, 1) + jnp.minimum(ty_count - 1 - t, 1)
    pl.semaphore_wait(barrier, len(chips) * (1 + sides))

    def copy(src, dst, send, recv, target):
        return pltpu.make_async_remote_copy(
            src_ref=src, dst_ref=dst, send_sem=send, recv_sem=recv, device_id=target, device_id_type=MESH
        )

    def level_copy(n, chip, other, target, own=False):
        at = block(chip, other)
        return copy(own_ref if own else all_ref.at[at], all_ref.at[at], send_sem.at[n], recv_sem.at[at], target)

    def side_copy(n, side, chip, other, target, own=False):
        at = block(chip, other)
        slot = beside.at[side, at]
        return copy(strip_ref.at[1 - side] if own else slot, slot, side_send.at[side, n], side_recv.at[side, at], target)

    started = []
    for side in range(2):

        @pl.when(has[1 - side])
        def _():
            for n, chip in enumerate(chips):
                side_copy(n, side, chips[0], False, device(chip, False, t + 1 - 2 * side), True).start()

    for n, chip in enumerate(chips[:0:-1]):
        started.append(level_copy(n, chips[0], False, device(chip, False, t), True))
        started[-1].start()
    n = len(chips) - 1
    started.append(level_copy(n, chips[0], False, across, True))
    started[-1].start()
    for chip in chips[1:]:
        n += 1
        level_copy(0, chip, False, across).wait_recv()
        started.append(level_copy(n, chip, False, across))
        started[-1].start()
    for side in range(2):

        @pl.when(has[side])
        def _():
            for n, chip in enumerate(chips):
                side_copy(0, side, chip, False, across).wait_recv()
                side_copy(len(chips) + n, side, chip, False, across).start()

    for chip in chips:
        level_copy(0, chip, True, across).wait_recv()
    for side in range(2):

        @pl.when(has[side])
        def _():
            for n, chip in enumerate(chips):
                side_copy(0, side, chip, True, across).wait_recv()
                side_copy(len(chips) + n, side, chip, False, across).wait_send()

        @pl.when(has[1 - side])
        def _():
            for n, chip in enumerate(chips):
                side_copy(n, side, chips[0], False, device(chip, False, t + 1 - 2 * side), True).wait_send()

    for one in started:
        one.wait_send()


def exchange(sources, live, acc, inner, spectrum, mirror, masks, row_table, col_table, count_x, sizes):
    tx_count, ty_count, src_count = sizes
    blocks = tx_count * src_count
    vmem = pl.BlockSpec(memory_space=pltpu.VMEM)
    cols = acc.shape[0]
    return pl.pallas_call(
        functools.partial(exchange_kernel, sizes, sources),
        out_shape=(
            jax.ShapeDtypeStruct((blocks, count_x, cols), jnp.bfloat16),
            jax.ShapeDtypeStruct((2, blocks, PACK, count_x), jnp.bfloat16),
        ),
        in_specs=[vmem] * 8,
        out_specs=(vmem,) * 2,
        scratch_shapes=[
            pltpu.SMEM(live.shape, jnp.int32),
            pltpu.VMEM(acc.shape, jnp.float32),
            pltpu.VMEM((count_x, cols), jnp.bfloat16),
            pltpu.VMEM((2, PACK, count_x), jnp.bfloat16),
            [pltpu.VMEM(inner.shape, jnp.bfloat16)] * 2,
            pltpu.SemaphoreType.DMA(()),
            pltpu.SemaphoreType.DMA((blocks,)),
            pltpu.SemaphoreType.DMA((blocks,)),
            pltpu.SemaphoreType.DMA((2, blocks)),
            pltpu.SemaphoreType.DMA((2, blocks)),
        ],
        compiler_params=pltpu.CompilerParams(collective_id=1, has_side_effects=True, vmem_limit_bytes=12 << 20),
        name="exchange",
    )(live, acc, inner, spectrum, mirror, masks, row_table, col_table)


def diffuse_kernel(sizes, all_ref, beside, blend_ref, out_ref, first, second):
    tx_count, ty_count, src_count = sizes
    rows, cols = out_ref.shape
    blocks, count, _ = all_ref.shape
    samples = blocks * count
    tall = rows + 2 * EDGE
    tiles = cols // LANES
    row_block = lax.axis_index("tx") * src_count + lax.axis_index("src")
    col_block = lax.axis_index("ty")
    lane = iota((1, LANES), 1)

    def inside(start, size, tile):
        x = row_block * rows - EDGE + start + iota((size, 1), 0)
        y = col_block * cols + tile * LANES + lane
        if tile == tiles:
            y = jnp.where(lane >= LANES // 2, y - cols - LANES, y)
        return (x >= 0) & (x < blocks * rows) & (y >= 0) & (y < ty_count * cols)

    def keep(target, start, tile, value):
        size = value.shape[0]
        target[tile, EDGE + start : EDGE + start + size] = jnp.where(inside(start, size, tile), value, 0.0)

    level = all_ref[...].reshape(samples, cols)
    sides = [jnp.concatenate([beside[side, n] for n in range(blocks)], axis=1) for side in range(2)]
    strip = jnp.concatenate([sides[1], jnp.zeros((LANES - 2 * PACK, samples), jnp.bfloat16), sides[0]], axis=0)
    edge = lax.dot_general(blend_ref[...], strip, (((1,), (1,)), ((), ())), preferred_element_type=jnp.float32)
    keep(first, 0, tiles, 1.0 - jnp.exp(-edge))
    cut = pl.cdiv(tall, 2 * PACK) * PACK
    for start, stop in ((0, cut), (cut, tall)):
        middle = 1.0 - jnp.exp(-dot(blend_ref[start:stop], level))
        for tile in range(tiles):
            keep(first, start, tile, middle[:, tile * LANES : (tile + 1) * LANES])

    def spread(source, start, size, wanted):
        at = EDGE + start
        centre = [source[tile, at : at + size] for tile in range(tiles + 1)]
        after = [pltpu.roll(value, 1, 1) for value in centre]
        ahead = [pltpu.roll(value, LANES - 1, 1) for value in centre]
        for tile in wanted:
            left = jnp.where(lane == 0, after[tile - 1], after[tile])
            right = jnp.where(lane == LANES - 1, ahead[(tile + 1) % (tiles + 1)], ahead[tile])
            near = source[tile, at - 1 : at - 1 + size] + source[tile, at + 1 : at + 1 + size] + left + right
            yield tile, centre[tile] + diffusion_rate * (near - 4.0 * centre[tile])

    chunk = min(rows, 64)
    for start in range(0, tall, chunk):
        size = min(chunk, tall - start)
        for tile, value in spread(first, start, size, range(tiles + 1)):
            keep(second, start, tile, value)
    for start in range(0, rows, chunk):
        for tile, value in spread(second, EDGE + start, chunk, range(tiles)):
            out_ref[start : start + chunk, tile * LANES : (tile + 1) * LANES] = value


def diffuse(levels, beside, blend, sizes):
    rows = blend.shape[0] - 2 * EDGE
    cols = levels.shape[2]
    vmem = pl.BlockSpec(memory_space=pltpu.VMEM)
    return pl.pallas_call(
        functools.partial(diffuse_kernel, sizes),
        out_shape=jax.ShapeDtypeStruct((rows, cols), jnp.float32),
        in_specs=[vmem] * 3,
        out_specs=vmem,
        scratch_shapes=[pltpu.VMEM((cols // LANES + 1, rows + 4 * EDGE, LANES), jnp.float32)] * 2,
        compiler_params=pltpu.CompilerParams(vmem_limit_bytes=12 << 20),
        name="diffuse",
    )(levels, beside, blend)


def body(sizes, cols, spectrum, pupil_mask, source_shifts, source_weights):
    turned, mirror, live, row_table, col_table, masks, blend = gather(
        spectrum, source_shifts, source_weights, pupil_mask, sizes, cols
    )
    sources = source_weights.shape[0] * sizes[2]
    count_x = blend.shape[1] // (sizes[0] * sizes[2])
    acc, inner = image(live, turned, mirror, row_table, col_table, masks, sizes)
    levels, beside = exchange(
        sources, live, acc, inner, turned, mirror, masks, row_table, col_table, count_x, sizes
    )
    return diffuse(levels, beside, blend, sizes)


def solution(mesh):
    sizes = (mesh.shape["tx"], mesh.shape["ty"], mesh.shape["src"])
    placed = (P(None, ("tx", "ty"), "src"), P(), P("src", None), P("src"))
    return jax.shard_map(
        functools.partial(body, sizes, COLS),
        mesh=mesh,
        in_specs=placed,
        out_specs=P(("tx", "src"), "ty"),
        check_vma=False,
    )
```

```python
import functools
import math

import jax
import jax.numpy as jnp
from jax import lax
from jax.experimental import pallas as pl
from jax.experimental.pallas import tpu as pltpu
from jax.sharding import PartitionSpec as P

FRAME = 2048
LANES = 128
COLS = 256
EDGE = 8
PACK = 16
GROUP = 2
UNROLL = 4
TAIL = 12
MESH = pl.DeviceIdType.MESH

diffusion_rate = 0.2


def wave(turns, period):
    quarter = period // 4
    turn = (turns + quarter // 2) // quarter
    angle = (turns - turn * quarter).astype(jnp.float32) * (2 * math.pi / period)
    square = angle * angle
    sine = angle * (1 + square * (-1 / 6 + square * (1 / 120 + square * (-1 / 5040 + square / 362880))))
    cosine = 1 + square * (-1 / 2 + square * (1 / 24 + square * (-1 / 720 + square / 40320)))
    odd = (turn & 1) == 1
    first, second = jnp.where(odd, sine, cosine), jnp.where(odd, cosine, sine)
    return jnp.where(((turn + 1) & 2) == 2, -first, first), jnp.where((turn & 2) == 2, -second, second)


def iota(shape, dim):
    return lax.broadcasted_iota(jnp.int32, shape, dim)


def dot(a, b):
    return jnp.dot(a, b, preferred_element_type=jnp.float32)


def unit(size, back):
    rows, cols = iota((size, size), 0), iota((size, size), 1)
    return jnp.where(rows + cols == size - 1 if back else rows == cols, 1.0, 0.0).astype(jnp.bfloat16)


def flip_bits(index, mask):
    bit = 1
    while bit <= mask:
        if mask & bit:
            index = index + bit * (1 - 2 * lax.rem(index // bit, 2))
        bit *= 2
    return index


def others(index, count):
    if count & (count - 1) == 0:
        return [flip_bits(index, d) for d in range(1, count)]
    return [lax.rem(index + d, count) for d in range(1, count)]


def mates(index, count):
    orders = [
        sorted((i for i in range(count) if i != at), key=lambda i: (i != at ^ 1, abs(i - at), i)) for at in range(count)
    ]
    return [sum(jnp.where(index == at, orders[at][n], 0) for at in range(count)) for n in range(count - 1)]


def row_table(row_ref, count, block, blocks):
    half = row_ref.shape[0] // (2 * GROUP)
    each = LANES // GROUP
    step = FRAME // (count * blocks)
    sample = iota((half, each), 1)
    x = step * (blocks * sample + block)
    cosine, sine = wave((x * iota((half, each), 0)) & (FRAME - 1), FRAME)
    cosine = jnp.where(sample < count, cosine, 0.0)
    sine = jnp.where(sample < count, sine, 0.0)
    none = jnp.zeros((half, each), jnp.float32)
    for g in range(GROUP):
        for part, (real, imag) in enumerate(((cosine, sine), (-sine, cosine))):
            row = [real if n == g else none for n in range(GROUP)] + [imag if n == g else none for n in range(GROUP)]
            at = (2 * g + part) * half
            row_ref[at : at + half] = jnp.concatenate(row, axis=1).astype(jnp.bfloat16)


def col_table(col_ref, t):
    cols, half = col_ref.shape[0], col_ref.shape[1] // 2
    chunk = 64

    def fill(n, carry):
        start = pl.multiple_of(n * chunk, chunk)
        y = t * cols + start + iota((chunk, half), 0)
        cosine, sine = wave((y * (2 * iota((chunk, half), 1) + 1)) & (2 * FRAME - 1), 2 * FRAME)
        col_ref[pl.ds(start, chunk), :half] = cosine.astype(jnp.bfloat16)
        col_ref[pl.ds(start, chunk), half:] = sine.astype(jnp.bfloat16)
        return carry

    lax.fori_loop(0, cols // chunk, fill, 0)


def list_live(live_ref, shifts_ref, weights_ref):
    src_count, _, slots = shifts_ref.shape
    width = live_ref.shape[1]
    weights = weights_ref[:, 0, :].astype(jnp.float32)
    words = shifts_ref[:, 0, :].astype(jnp.float32) + shifts_ref[:, 1, :].astype(jnp.float32) * 1024.0 + weights * 1048576.0
    on = jnp.where(weights > 0, 1.0, 0.0)
    ahead = jnp.where(iota((slots, slots), 0) < iota((slots, slots), 1), 1.0, 0.0)
    rank = dot(on.astype(jnp.bfloat16), ahead.astype(jnp.bfloat16))
    before = jnp.zeros((1, 1), jnp.float32)
    ranks = []
    for k in range(src_count):
        ranks.append(rank[k : k + 1] + before)
        before = before + jnp.sum(on[k : k + 1], axis=1, keepdims=True)
    rank = jnp.where(on > 0, jnp.concatenate(ranks, axis=0), -1.0).T
    words = words.T
    place = (iota((slots, width), 1) - GROUP).astype(jnp.float32)
    total = jnp.zeros((slots, width), jnp.float32)
    for k in range(src_count):
        total += jnp.where(rank[:, k : k + 1] == place, words[:, k : k + 1], 0.0)
    found = jnp.sum(total, axis=0, keepdims=True)
    live_ref[...] = jnp.where(iota((1, width), 1) == width - 1, before, found).astype(jnp.int32)


def turns_before_tail(live):
    steps = jnp.maximum((live[0, live.shape[1] - 1] + GROUP - 1) // GROUP + 1 - TAIL, 0) + 1
    return steps // 4, lax.rem(steps, 4) // 2


def blend_table(blend_ref, block, blocks):
    tall, samples = blend_ref.shape
    rows = tall - 2 * EDGE
    step = FRAME // samples
    count = samples // blocks
    chunk = PACK

    def fill(n, carry):
        start = pl.multiple_of(n * chunk, chunk)
        x = block * rows - EDGE + start + iota((chunk, samples), 0)
        column = iota((chunk, samples), 1)
        owner = column // count
        gap = x - step * (blocks * (column - owner * count) + owner)
        gap = ((gap + FRAME // 2) & (FRAME - 1)) - FRAME // 2
        cosine, sine = wave(gap, 2 * FRAME)
        place = block * rows - EDGE + start + iota((chunk, 1), 0)
        place = place & (2 * step - 1)
        scale = jnp.zeros((chunk, 1), jnp.float32)
        for n in range(2 * step):
            if n % step:
                scale = jnp.where(place == n, math.sin(math.pi * n / step) / samples, scale)
        scale = jnp.where((owner & 1) == 1, -scale, scale)
        here = gap == 0
        table = jnp.where(here, 1.0, scale * cosine / jnp.where(here, 1.0, sine))
        blend_ref[pl.ds(start, chunk)] = table.astype(jnp.bfloat16)
        return carry

    lax.fori_loop(0, tall // chunk, fill, 0)


def gather_kernel(
    sizes, spec_hbm, shift_ref, weight_ref, pupil_hbm, turned_ref, mirror_ref, live_ref, row_ref, col_ref, mask_ref, blend_ref,
    shifts_ref, weights_ref, all_ref, spec_ref, pupil_ref, local_sem, send_sem, recv_sem, side_send, side_recv,
):
    tx_count, ty_count, src_count = sizes
    pair_count = tx_count // 2
    tx, t, s = lax.axis_index("tx"), lax.axis_index("ty"), lax.axis_index("src")
    pair, core = tx // 2, lax.rem(tx, 2)
    other_core = 1 - core
    far_t = mates(t, ty_count)
    far_s = others(s, src_count)
    far_pair = others(pair, pair_count)

    def along_ty(i):
        return {"tx": tx, "ty": i, "src": s}

    def along_src(i):
        return {"tx": tx, "ty": t, "src": i}

    loads = [
        pltpu.make_async_copy(src, dst, local_sem.at[n])
        for n, (src, dst) in enumerate(
            (
                (spec_hbm, spec_ref),
                (pupil_hbm, pupil_ref),
                (shift_ref, shifts_ref.at[s]),
                (weight_ref, weights_ref.at[s]),
            )
        )
    ]
    for load in loads:
        load.start()

    across = {"tx": 2 * pair + other_core, "ty": t, "src": s}
    hood = [(i, k) for k in far_s + [s] for i in far_pair + [pair] if i is not pair or k is not s]
    partners = [along_ty(i) for i in far_t] + [{"tx": 2 * i + core, "ty": t, "src": k} for i, k in hood] + [across]
    barrier = pltpu.get_barrier_semaphore()
    for partner in partners:
        pl.semaphore_signal(barrier, inc=1, device_id=partner, device_id_type=MESH)
    pl.semaphore_wait(barrier, len(partners))
    loads[0].wait()

    started = []
    own = (tx, t, s)

    both = slice(None)

    def part(plane, piece):
        i, j, k = piece
        return all_ref.at[k, plane, i, j], recv_sem.at[0, k, i, j]

    def send(plane, piece, device):
        slot, arrived = part(plane, piece)
        copy = pltpu.make_async_remote_copy(
            src_ref=spec_ref if piece is own else slot,
            dst_ref=slot,
            send_sem=send_sem.at[len(started)],
            recv_sem=arrived,
            device_id=device,
            device_id_type=MESH,
        )
        copy.start()
        started.append(copy)

    def arrive(plane, piece):
        slot, arrived = part(plane, piece)
        pltpu.make_async_remote_copy(
            src_ref=slot,
            dst_ref=slot,
            send_sem=send_sem.at[0],
            recv_sem=arrived,
            device_id=across,
            device_id_type=MESH,
        ).wait_recv()

    def spread(piece):
        for i, k in hood:
            send(both, piece, {"tx": 2 * i + core, "ty": t, "src": k})

    for j in far_t:
        send(both, own, along_ty(j))
    spread(own)
    send(both, own, across)

    side = []
    for n, i in enumerate(far_s):
        for m, (src, dst) in enumerate(((shift_ref, shifts_ref), (weight_ref, weights_ref))):
            copy = pltpu.make_async_remote_copy(
                src_ref=src,
                dst_ref=dst.at[s],
                send_sem=side_send.at[m, n],
                recv_sem=side_recv.at[m, s],
                device_id=along_src(i),
                device_id_type=MESH,
            )
            copy.start()
            side.append(copy)

    for load in loads[1:]:
        load.wait()
    for plane in range(2):
        all_ref[s, plane, tx, t] = spec_ref[plane]
    block = tx * src_count + s
    blocks = tx_count * src_count
    row_table(row_ref, blend_ref.shape[1] // blocks, block, blocks)
    col_table(col_ref, t)
    half = pupil_ref.shape[0] // 2
    pupil = pupil_ref[...].astype(jnp.float32).astype(jnp.bfloat16)
    turned = (((1,), (1,)), ((), ()))
    mask_ref[:half] = lax.dot_general(unit(half, False), pupil[:, half:], turned, preferred_element_type=jnp.float32).astype(jnp.bfloat16)
    mask_ref[half:] = lax.dot_general(unit(half, True), pupil[:, :half], turned, preferred_element_type=jnp.float32).astype(jnp.bfloat16)

    part_rows, part_cols = ty_count * spec_ref.shape[1], spec_ref.shape[2]

    def turn(i, k):
        cell = jnp.concatenate([all_ref[k, plane, i].reshape(part_rows, part_cols) for plane in range(2)], axis=0)
        for back, target in enumerate((turned_ref, mirror_ref)):
            start = (src_count - 1 - k if back else k) * part_cols
            rows = pl.ds(pl.multiple_of(start, part_cols), part_cols)
            value = lax.dot_general(unit(part_cols, back), cell, turned, preferred_element_type=jnp.float32)
            for plane in range(2):
                tile = value[:, plane * part_rows : (plane + 1) * part_rows]
                target[plane * tx_count + i, rows] = tile
                target[(plane + 2) * tx_count + i, rows] = -tile

    def pass_on(i, j, k, also=None):
        piece = (2 * i + core, j, k)
        arrive(both, piece)
        if also is not None:
            send(both, piece, along_ty(also))
        send(both, piece, across)

    mate, far_t = far_t[0], far_t[1:]
    near, distant = hood[1:], hood[:1]
    for i, k in near:
        pass_on(i, t, k, mate)
    for n, j in enumerate(far_t):
        arrive(both, (tx, j, s))
        spread((tx, j, s))
        if n == 0:
            for i, k in distant:
                pass_on(i, t, k, mate)
    for j in [mate] + far_t:
        if j is mate:
            arrive(both, (tx, j, s))
        send(both, (tx, j, s), across)
    turn(tx, s)
    for n, i in enumerate(far_s):
        for m, (src, dst) in enumerate(((shift_ref, shifts_ref), (weight_ref, weights_ref))):
            pltpu.make_async_remote_copy(
                src_ref=src,
                dst_ref=dst.at[i],
                send_sem=side_send.at[m, n],
                recv_sem=side_recv.at[m, i],
                device_id=across,
                device_id_type=MESH,
            ).wait_recv()
    list_live(live_ref, shifts_ref, weights_ref)
    blend_table(blend_ref, block, blocks)
    near_first = [t, mate] + far_t
    for j in near_first:
        arrive(both, (2 * pair + other_core, j, s))
    turn(2 * pair + other_core, s)
    for i, k in near + distant:
        pass_on(i, mate, k)
    for j in far_t:
        for i, k in near + distant:
            pass_on(i, j, k)
    for i, k in near + distant:
        turn(2 * i + core, k)
    for j in near_first:
        for i, k in near + distant:
            arrive(both, (2 * i + other_core, j, k))
    for i, k in near + distant:
        turn(2 * i + other_core, k)
    for copy in started + side:
        copy.wait_send()


def gather(spectrum, source_shifts, source_weights, pupil_mask, sizes, cols):
    tx_count, ty_count, src_count = sizes
    pair_count = tx_count // 2
    _, block_rows, block_cols = spectrum.shape
    slots = source_weights.shape[0]
    length = pupil_mask.shape[0]
    blocks = tx_count * src_count
    samples = 2 * length
    width = pl.cdiv(src_count * slots + (UNROLL + TAIL + 2) * GROUP + 1, LANES) * LANES
    vmem = pl.BlockSpec(memory_space=pltpu.VMEM)
    lines = pair_count * src_count * ty_count
    sends = ty_count - 1 + lines + ty_count * (src_count - 1 + pair_count - 1)
    sends += 3 * ty_count * (src_count - 1) * (pair_count - 1)
    return pl.pallas_call(
        functools.partial(gather_kernel, sizes),
        out_shape=(
            jax.ShapeDtypeStruct((4 * tx_count, src_count * block_cols, ty_count * block_rows), jnp.float32),
            jax.ShapeDtypeStruct((4 * tx_count, src_count * block_cols, ty_count * block_rows), jnp.float32),
            jax.ShapeDtypeStruct((1, width), jnp.int32),
            jax.ShapeDtypeStruct((GROUP * length, 2 * LANES), jnp.bfloat16),
            jax.ShapeDtypeStruct((cols, length), jnp.bfloat16),
            jax.ShapeDtypeStruct((length, length), jnp.bfloat16),
            jax.ShapeDtypeStruct((FRAME // blocks + 2 * EDGE, samples), jnp.bfloat16),
        ),
        in_specs=[pl.BlockSpec(memory_space=pltpu.HBM)] * 4,
        out_specs=(vmem,) * 7,
        scratch_shapes=[
            pltpu.VMEM((src_count, 2, slots), jnp.int32),
            pltpu.VMEM((src_count, 1, slots), jnp.int32),
            pltpu.VMEM((src_count, 2, tx_count, ty_count, block_rows, block_cols), jnp.bfloat16),
            pltpu.VMEM(spectrum.shape, jnp.bfloat16),
            pltpu.VMEM(pupil_mask.shape, jnp.int32),
            pltpu.SemaphoreType.DMA((4,)),
            pltpu.SemaphoreType.DMA((sends,)),
            pltpu.SemaphoreType.DMA((2, src_count, tx_count, ty_count)),
            pltpu.SemaphoreType.DMA((2, src_count)),
            pltpu.SemaphoreType.DMA((2, src_count)),
        ],
        compiler_params=pltpu.CompilerParams(collective_id=0, has_side_effects=True, vmem_limit_bytes=24 << 20),
        name="gather",
    )(*(pltpu.with_memory_space_constraint(a, pltpu.HBM) for a in (spectrum, source_shifts.T, source_weights[None], pupil_mask)))


def stages(sizes, spec, mirror, mask_ref, row_ref, col_ref, live):
    half = col_ref.shape[1] // 2
    height = spec.shape[1]
    tiles = spec.shape[0] // 4
    block = lax.axis_index("tx") * sizes[2] + lax.axis_index("src")
    power = lax.rem(block, 4)
    flip = 2 * lax.rem(power, 2)
    middle = (lax.rem(4 - power, 4), power + 1 - 2 * lax.rem(power, 2))
    lane = iota((half, LANES), 1)
    first_half = iota((1, LANES), 1) < LANES // 2

    def cross(n, slot):
        total = [[], []]
        for g in range(GROUP):
            word = live[0, (n + 1) * GROUP + g]
            a, b = word & 1023, (word >> 10) & 1023
            tile, rest = a // LANES, lax.rem(a, LANES)
            keep = lane >= rest
            last = jnp.minimum(tile + 2, tiles - 1)

            def window(source, start, part):
                rows = pl.ds(start, half)
                low = pltpu.roll(mask_ref[part * half : (part + 1) * half, :LANES], rest, 1)
                high = pltpu.roll(mask_ref[part * half : (part + 1) * half, LANES:], rest, 1)
                ends = jnp.where(keep, low, high)
                centre = jnp.where(keep, high, low)
                found = []
                for plane in range(2):
                    outer = jnp.where(keep, source[plane * tiles + tile, rows, :], source[(plane + flip) * tiles + last, rows, :])
                    between = source[middle[plane] * tiles + tile + 1, rows, :]
                    found.append(outer.astype(jnp.bfloat16) * ends + between.astype(jnp.bfloat16) * centre)
                return found

            upper = window(spec, b + half, 0)
            lower = window(mirror, height - half - b, 1)
            total[0].append(jnp.concatenate([upper[0] + lower[0], upper[1] + lower[1]], axis=1))
            total[1].append(jnp.concatenate([lower[1] - upper[1], upper[0] - lower[0]], axis=1))
        for n in range(2):
            slot[n * half : (n + 1) * half] = dot(jnp.concatenate(total[n], axis=1), row_ref[...]).astype(jnp.bfloat16)

    def square(n, source, acc):
        pair = [(live[0, (n + 1) * GROUP + g] >> 20).astype(jnp.float32) for g in range(GROUP)]
        scale = jnp.where(first_half, pair[0], pair[1])
        tall = col_ref.shape[0] // 2
        for part in range(2):
            rows = slice(part * tall, (part + 1) * tall)
            wide = dot(col_ref[rows], source[...])
            real, imag = wide[:, :LANES], wide[:, LANES:]
            acc[rows] += scale * (real * real + imag * imag)

    return cross, square


def image_kernel(
    sizes, live_ref, spec, mirror, mask_ref, row_ref, col_ref, acc, next_inner,
    live, other_inner, live_sem,
):
    load = pltpu.make_async_copy(live_ref, live, live_sem)
    load.start()
    cross, square = stages(sizes, spec, mirror, mask_ref, row_ref, col_ref, live)
    inner = (other_inner, next_inner)
    acc[...] = jnp.zeros_like(acc)
    next_inner[...] = jnp.zeros_like(next_inner)
    load.wait()

    def run(start, count, steps):
        def turn_body(turn_index, carry):
            for g in range(steps):
                n = start + turn_index * steps + g
                cross(n, inner[g % 2])
                square(n - 1, inner[1 - g % 2], acc)
            return carry

        lax.fori_loop(0, count, turn_body, 0)

    full, half = turns_before_tail(live)
    run(0, full, 4)
    run(4 * full, half, 2)


def image(live, spectrum, mirror, row_table, col_table, masks, sizes):
    cols, length = col_table.shape
    vmem = pl.BlockSpec(memory_space=pltpu.VMEM)
    return pl.pallas_call(
        functools.partial(image_kernel, sizes),
        out_shape=(
            jax.ShapeDtypeStruct((cols, LANES), jnp.float32),
            jax.ShapeDtypeStruct((length, 2 * LANES), jnp.bfloat16),
        ),
        in_specs=[vmem] * 6,
        out_specs=(vmem,) * 2,
        scratch_shapes=[
            pltpu.SMEM(live.shape, jnp.int32),
            pltpu.VMEM((length, 2 * LANES), jnp.bfloat16),
            pltpu.SemaphoreType.DMA(()),
        ],
        compiler_params=pltpu.CompilerParams(vmem_limit_bytes=12 << 20),
        name="image",
    )(live, spectrum, mirror, masks, row_table, col_table)


def exchange_kernel(
    sizes, sources, live_ref, acc, first_inner, spec, mirror, mask_ref, row_ref, col_ref, all_ref, beside,
    live, total, own_ref, strip_ref, inner, live_sem, send_sem, recv_sem, side_send, side_recv,
):
    tx_count, ty_count, src_count = sizes
    pair_count = tx_count // 2
    tx, t, s = lax.axis_index("tx"), lax.axis_index("ty"), lax.axis_index("src")
    pair, core = tx // 2, lax.rem(tx, 2)
    far_s = [s] + others(s, src_count)
    far_pair = [pair] + others(pair, pair_count)
    chips = [(i, k) for k in far_s for i in far_pair]

    def device(chip, other, z):
        return {"tx": 2 * chip[0] + (1 - core if other else core), "ty": z, "src": chip[1]}

    def block(chip, other):
        return (2 * chip[0] + (1 - core if other else core)) * src_count + chip[1]

    across = device(chips[0], True, t)
    barrier = pltpu.get_barrier_semaphore()

    def greet(chip, z):
        pl.semaphore_signal(barrier, inc=1, device_id=device(chip, False, z), device_id_type=MESH)

    load = pltpu.make_async_copy(live_ref, live, live_sem)
    load.start()
    has = (t > 0, t < ty_count - 1)
    beside[...] = jnp.zeros_like(beside)
    pl.semaphore_signal(barrier, inc=1, device_id=across, device_id_type=MESH)
    for chip in chips[1:]:
        greet(chip, t)
    for side in range(2):

        @pl.when(has[side])
        def _():
            for chip in chips:
                greet(chip, t + 2 * side - 1)

    cross, square = stages(sizes, spec, mirror, mask_ref, row_ref, col_ref, live)
    load.wait()
    full, half = turns_before_tail(live)
    n = 4 * full + 2 * half
    total[...] = acc[...]
    source_inner = first_inner
    for g in range(TAIL):
        if g < TAIL - 1:
            cross(n + g, inner[g % 2])
        square(n + g - 1, source_inner, total)
        source_inner = inner[g % 2]

    level = total[...]
    cols = level.shape[0]
    count_x = own_ref.shape[0]
    level = (level + pltpu.roll(level, LANES // 2, 1)) / (2.0 * sources)
    own = level.T[:count_x].astype(jnp.bfloat16)
    own_ref[...] = own
    strip_ref[0] = level[:PACK, :count_x].astype(jnp.bfloat16)
    strip_ref[1] = level[cols - PACK :, :count_x].astype(jnp.bfloat16)
    all_ref[block(chips[0], False)] = own
    sides = jnp.minimum(t, 1) + jnp.minimum(ty_count - 1 - t, 1)
    pl.semaphore_wait(barrier, len(chips) * (1 + sides))

    def copy(src, dst, send, recv, target):
        return pltpu.make_async_remote_copy(
            src_ref=src, dst_ref=dst, send_sem=send, recv_sem=recv, device_id=target, device_id_type=MESH
        )

    def level_copy(n, chip, other, target, own=False):
        at = block(chip, other)
        return copy(own_ref if own else all_ref.at[at], all_ref.at[at], send_sem.at[n], recv_sem.at[at], target)

    def side_copy(n, side, chip, other, target, own=False):
        at = block(chip, other)
        slot = beside.at[side, at]
        return copy(strip_ref.at[1 - side] if own else slot, slot, side_send.at[side, n], side_recv.at[side, at], target)

    started = []
    for side in range(2):

        @pl.when(has[1 - side])
        def _():
            for n, chip in enumerate(chips):
                side_copy(n, side, chips[0], False, device(chip, False, t + 1 - 2 * side), True).start()

    for n, chip in enumerate(chips[:0:-1]):
        started.append(level_copy(n, chips[0], False, device(chip, False, t), True))
        started[-1].start()
    n = len(chips) - 1
    started.append(level_copy(n, chips[0], False, across, True))
    started[-1].start()
    for chip in chips[1:]:
        n += 1
        level_copy(0, chip, False, across).wait_recv()
        started.append(level_copy(n, chip, False, across))
        started[-1].start()
    for side in range(2):

        @pl.when(has[side])
        def _():
            for n, chip in enumerate(chips):
                side_copy(0, side, chip, False, across).wait_recv()
                side_copy(len(chips) + n, side, chip, False, across).start()

    for chip in chips:
        level_copy(0, chip, True, across).wait_recv()
    for side in range(2):

        @pl.when(has[side])
        def _():
            for n, chip in enumerate(chips):
                side_copy(0, side, chip, True, across).wait_recv()
                side_copy(len(chips) + n, side, chip, False, across).wait_send()

        @pl.when(has[1 - side])
        def _():
            for n, chip in enumerate(chips):
                side_copy(n, side, chips[0], False, device(chip, False, t + 1 - 2 * side), True).wait_send()

    for one in started:
        one.wait_send()


def exchange(sources, live, acc, inner, spectrum, mirror, masks, row_table, col_table, count_x, sizes):
    tx_count, ty_count, src_count = sizes
    blocks = tx_count * src_count
    vmem = pl.BlockSpec(memory_space=pltpu.VMEM)
    cols = acc.shape[0]
    return pl.pallas_call(
        functools.partial(exchange_kernel, sizes, sources),
        out_shape=(
            jax.ShapeDtypeStruct((blocks, count_x, cols), jnp.bfloat16),
            jax.ShapeDtypeStruct((2, blocks, PACK, count_x), jnp.bfloat16),
        ),
        in_specs=[vmem] * 8,
        out_specs=(vmem,) * 2,
        scratch_shapes=[
            pltpu.SMEM(live.shape, jnp.int32),
            pltpu.VMEM(acc.shape, jnp.float32),
            pltpu.VMEM((count_x, cols), jnp.bfloat16),
            pltpu.VMEM((2, PACK, count_x), jnp.bfloat16),
            [pltpu.VMEM(inner.shape, jnp.bfloat16)] * 2,
            pltpu.SemaphoreType.DMA(()),
            pltpu.SemaphoreType.DMA((blocks,)),
            pltpu.SemaphoreType.DMA((blocks,)),
            pltpu.SemaphoreType.DMA((2, blocks)),
            pltpu.SemaphoreType.DMA((2, blocks)),
        ],
        compiler_params=pltpu.CompilerParams(collective_id=1, has_side_effects=True, vmem_limit_bytes=12 << 20),
        name="exchange",
    )(live, acc, inner, spectrum, mirror, masks, row_table, col_table)


def diffuse_kernel(sizes, all_ref, beside, blend_ref, out_ref, first, second):
    tx_count, ty_count, src_count = sizes
    rows, cols = out_ref.shape
    blocks, count, _ = all_ref.shape
    samples = blocks * count
    tall = rows + 2 * EDGE
    tiles = cols // LANES
    row_block = lax.axis_index("tx") * src_count + lax.axis_index("src")
    col_block = lax.axis_index("ty")
    lane = iota((1, LANES), 1)

    def inside(start, size, tile):
        x = row_block * rows - EDGE + start + iota((size, 1), 0)
        y = col_block * cols + tile * LANES + lane
        if tile == tiles:
            y = jnp.where(lane >= LANES // 2, y - cols - LANES, y)
        return (x >= 0) & (x < blocks * rows) & (y >= 0) & (y < ty_count * cols)

    def keep(target, start, tile, value):
        size = value.shape[0]
        target[tile, EDGE + start : EDGE + start + size] = jnp.where(inside(start, size, tile), value, 0.0)

    level = all_ref[...].reshape(samples, cols)
    sides = [jnp.concatenate([beside[side, n] for n in range(blocks)], axis=1) for side in range(2)]
    strip = jnp.concatenate([sides[1], jnp.zeros((LANES - 2 * PACK, samples), jnp.bfloat16), sides[0]], axis=0)
    edge = lax.dot_general(blend_ref[...], strip, (((1,), (1,)), ((), ())), preferred_element_type=jnp.float32)
    keep(first, 0, tiles, 1.0 - jnp.exp(-edge))
    cut = pl.cdiv(tall, 2 * PACK) * PACK
    for start, stop in ((0, cut), (cut, tall)):
        middle = 1.0 - jnp.exp(-dot(blend_ref[start:stop], level))
        for tile in range(tiles):
            keep(first, start, tile, middle[:, tile * LANES : (tile + 1) * LANES])

    def spread(source, start, size, wanted):
        at = EDGE + start
        centre = [source[tile, at : at + size] for tile in range(tiles + 1)]
        after = [pltpu.roll(value, 1, 1) for value in centre]
        ahead = [pltpu.roll(value, LANES - 1, 1) for value in centre]
        for tile in wanted:
            left = jnp.where(lane == 0, after[tile - 1], after[tile])
            right = jnp.where(lane == LANES - 1, ahead[(tile + 1) % (tiles + 1)], ahead[tile])
            near = source[tile, at - 1 : at - 1 + size] + source[tile, at + 1 : at + 1 + size] + left + right
            yield tile, centre[tile] + diffusion_rate * (near - 4.0 * centre[tile])

    chunk = min(rows, 64)
    for start in range(0, tall, chunk):
        size = min(chunk, tall - start)
        for tile, value in spread(first, start, size, range(tiles + 1)):
            keep(second, start, tile, value)
    for start in range(0, rows, chunk):
        for tile, value in spread(second, EDGE + start, chunk, range(tiles)):
            out_ref[start : start + chunk, tile * LANES : (tile + 1) * LANES] = value


def diffuse(levels, beside, blend, sizes):
    rows = blend.shape[0] - 2 * EDGE
    cols = levels.shape[2]
    vmem = pl.BlockSpec(memory_space=pltpu.VMEM)
    return pl.pallas_call(
        functools.partial(diffuse_kernel, sizes),
        out_shape=jax.ShapeDtypeStruct((rows, cols), jnp.float32),
        in_specs=[vmem] * 3,
        out_specs=vmem,
        scratch_shapes=[pltpu.VMEM((cols // LANES + 1, rows + 4 * EDGE, LANES), jnp.float32)] * 2,
        compiler_params=pltpu.CompilerParams(vmem_limit_bytes=12 << 20),
        name="diffuse",
    )(levels, beside, blend)


def body(sizes, cols, spectrum, pupil_mask, source_shifts, source_weights):
    turned, mirror, live, row_table, col_table, masks, blend = gather(
        spectrum, source_shifts, source_weights, pupil_mask, sizes, cols
    )
    sources = source_weights.shape[0] * sizes[2]
    count_x = blend.shape[1] // (sizes[0] * sizes[2])
    acc, inner = image(live, turned, mirror, row_table, col_table, masks, sizes)
    levels, beside = exchange(
        sources, live, acc, inner, turned, mirror, masks, row_table, col_table, count_x, sizes
    )
    return diffuse(levels, beside, blend, sizes)


def solution(mesh):
    sizes = (mesh.shape["tx"], mesh.shape["ty"], mesh.shape["src"])
    placed = (P(None, ("tx", "ty"), "src"), P(), P("src", None), P("src"))
    return jax.shard_map(
        functools.partial(body, sizes, COLS),
        mesh=mesh,
        in_specs=placed,
        out_specs=P(("tx", "src"), "ty"),
        check_vma=False,
    )
```

```python
import functools
import math

import jax
import jax.numpy as jnp
from jax import lax
from jax.experimental import pallas as pl
from jax.experimental.pallas import tpu as pltpu
from jax.sharding import PartitionSpec as P

FRAME = 2048
LANES = 128
COLS = 256
EDGE = 8
PACK = 16
CORES = 2
GROUP = 2
UNROLL = 4
TAIL = 8
SHARED = 4
MESH = pl.DeviceIdType.MESH

diffusion_rate = 0.2


def wave(turns, period):
    quarter = period // 4
    turn = (turns + quarter // 2) // quarter
    angle = (turns - turn * quarter).astype(jnp.float32) * (2 * math.pi / period)
    square = angle * angle
    sine = angle * (1 + square * (-1 / 6 + square * (1 / 120 + square * (-1 / 5040 + square / 362880))))
    cosine = 1 + square * (-1 / 2 + square * (1 / 24 + square * (-1 / 720 + square / 40320)))
    odd = (turn & 1) == 1
    first, second = jnp.where(odd, sine, cosine), jnp.where(odd, cosine, sine)
    return jnp.where(((turn + 1) & 2) == 2, -first, first), jnp.where((turn & 2) == 2, -second, second)


def iota(shape, dim):
    return lax.broadcasted_iota(jnp.int32, shape, dim)


def dot(a, b):
    return jnp.dot(a, b, preferred_element_type=jnp.float32)


def unit(size, back):
    rows, cols = iota((size, size), 0), iota((size, size), 1)
    return jnp.where(rows + cols == size - 1 if back else rows == cols, 1.0, 0.0).astype(jnp.bfloat16)


def flip_bits(index, mask):
    bit = 1
    while bit <= mask:
        if mask & bit:
            index = index + bit * (1 - 2 * lax.rem(index // bit, 2))
        bit *= 2
    return index


def others(index, count):
    if count & (count - 1) == 0:
        return [flip_bits(index, d) for d in range(1, count)]
    return [lax.rem(index + d, count) for d in range(1, count)]


def mates(index, count):
    orders = [
        sorted((i for i in range(count) if i != at), key=lambda i: (i != at ^ 1, abs(i - at), i)) for at in range(count)
    ]
    return [sum(jnp.where(index == at, orders[at][n], 0) for at in range(count)) for n in range(count - 1)]


def row_table(row_ref, count, chip, chips):
    half = row_ref.shape[0] // 2
    step = FRAME // (count * chips)
    sample = iota((half, LANES), 1)
    x = step * (chips * sample + chip)
    cosine, sine = wave((x * iota((half, LANES), 0)) & (FRAME - 1), FRAME)
    cosine = jnp.where(sample < count, cosine, 0.0).astype(jnp.bfloat16)
    sine = jnp.where(sample < count, sine, 0.0).astype(jnp.bfloat16)
    row_ref[:half, :LANES] = cosine
    row_ref[:half, LANES:] = sine
    row_ref[half:, :LANES] = -sine
    row_ref[half:, LANES:] = cosine


def col_table(col_ref, t):
    cols, half = col_ref.shape[0], col_ref.shape[1] // 2
    chunk = 64

    def fill(n, carry):
        start = pl.multiple_of(n * chunk, chunk)
        y = t * cols + start + iota((chunk, half), 0)
        cosine, sine = wave((y * (2 * iota((chunk, half), 1) + 1)) & (2 * FRAME - 1), 2 * FRAME)
        col_ref[pl.ds(start, chunk), :half] = cosine.astype(jnp.bfloat16)
        col_ref[pl.ds(start, chunk), half:] = sine.astype(jnp.bfloat16)
        return carry

    lax.fori_loop(0, cols // chunk, fill, 0)


def list_live(live_ref, shifts_ref, weights_ref):
    src_count, _, slots = shifts_ref.shape
    width = live_ref.shape[1]
    weights = weights_ref[:, 0, :].astype(jnp.float32)
    words = shifts_ref[:, 0, :].astype(jnp.float32) + shifts_ref[:, 1, :].astype(jnp.float32) * 1024.0 + weights * 1048576.0
    on = jnp.where(weights > 0, 1.0, 0.0)
    ahead = jnp.where(iota((slots, slots), 0) < iota((slots, slots), 1), 1.0, 0.0)
    rank = dot(on.astype(jnp.bfloat16), ahead.astype(jnp.bfloat16))
    before = jnp.zeros((1, 1), jnp.float32)
    ranks = []
    for k in range(src_count):
        ranks.append(rank[k : k + 1] + before)
        before = before + jnp.sum(on[k : k + 1], axis=1, keepdims=True)
    rank = jnp.where(on > 0, jnp.concatenate(ranks, axis=0), -1.0).T
    words = words.T
    place = iota((slots, width), 1).astype(jnp.float32)
    total = jnp.zeros((slots, width), jnp.float32)
    for k in range(src_count):
        total += jnp.where(rank[:, k : k + 1] == place, words[:, k : k + 1], 0.0)
    found = jnp.sum(total, axis=0, keepdims=True)
    live_ref[...] = jnp.where(iota((1, width), 1) == width - 1, before, found).astype(jnp.int32)


def turns_before_tail(live):
    count = jnp.maximum(live[0, live.shape[1] - 1] - SHARED * GROUP, 0)
    steps = jnp.maximum((count + CORES * GROUP - 1) // (CORES * GROUP) + 1 - TAIL, 0) + 1
    return steps // 4, lax.rem(steps, 4) // 2


def blend_table(blend_ref, block, blocks, src_count):
    tall, samples = blend_ref.shape
    rows = tall - 2 * EDGE
    step = FRAME // samples
    count = samples // blocks
    chunk = PACK

    def fill(n, carry):
        start = pl.multiple_of(n * chunk, chunk)
        x = block * rows - EDGE + start + iota((chunk, samples), 0)
        column = iota((chunk, samples), 1)
        owner = column // count
        line = owner // src_count
        chip = (line // CORES) * src_count + owner - line * src_count
        place = (line & (CORES - 1)) * count + column - owner * count
        gap = x - step * (blocks // CORES * place + chip)
        gap = ((gap + FRAME // 2) & (FRAME - 1)) - FRAME // 2
        cosine, sine = wave(gap, 2 * FRAME)
        place = block * rows - EDGE + start + iota((chunk, 1), 0)
        place = place & (2 * step - 1)
        scale = jnp.zeros((chunk, 1), jnp.float32)
        for n in range(2 * step):
            if n % step:
                scale = jnp.where(place == n, math.sin(math.pi * n / step) / samples, scale)
        scale = jnp.where((chip & 1) == 1, -scale, scale)
        here = gap == 0
        table = jnp.where(here, 1.0, scale * cosine / jnp.where(here, 1.0, sine))
        blend_ref[pl.ds(start, chunk)] = table.astype(jnp.bfloat16)
        return carry

    lax.fori_loop(0, tall // chunk, fill, 0)


def gather_kernel(
    sizes, spec_hbm, shift_ref, weight_ref, pupil_hbm, turned_ref, mirror_ref, live_ref, row_ref, col_ref, mask_ref, blend_ref,
    shifts_ref, weights_ref, all_ref, spec_ref, pupil_ref, local_sem, send_sem, recv_sem, side_send, side_recv,
):
    tx_count, ty_count, src_count = sizes
    pair_count = tx_count // 2
    tx, t, s = lax.axis_index("tx"), lax.axis_index("ty"), lax.axis_index("src")
    pair, core = tx // 2, lax.rem(tx, 2)
    other_core = 1 - core
    far_t = mates(t, ty_count)
    far_s = others(s, src_count)
    far_pair = others(pair, pair_count)

    def along_ty(i):
        return {"tx": tx, "ty": i, "src": s}

    def along_src(i):
        return {"tx": tx, "ty": t, "src": i}

    loads = [
        pltpu.make_async_copy(src, dst, local_sem.at[n])
        for n, (src, dst) in enumerate(
            (
                (spec_hbm, spec_ref),
                (pupil_hbm, pupil_ref),
                (shift_ref, shifts_ref.at[s]),
                (weight_ref, weights_ref.at[s]),
            )
        )
    ]
    for load in loads:
        load.start()

    across = {"tx": 2 * pair + other_core, "ty": t, "src": s}
    hood = [(i, k) for k in far_s + [s] for i in far_pair + [pair] if i is not pair or k is not s]
    partners = [along_ty(i) for i in far_t] + [{"tx": 2 * i + core, "ty": t, "src": k} for i, k in hood] + [across]
    barrier = pltpu.get_barrier_semaphore()
    for partner in partners:
        pl.semaphore_signal(barrier, inc=1, device_id=partner, device_id_type=MESH)
    pl.semaphore_wait(barrier, len(partners))
    loads[0].wait()

    started = []
    own = (tx, t, s)

    both = slice(None)

    def part(plane, piece):
        i, j, k = piece
        return all_ref.at[k, plane, i, j], recv_sem.at[0, k, i, j]

    def send(plane, piece, device):
        slot, arrived = part(plane, piece)
        copy = pltpu.make_async_remote_copy(
            src_ref=spec_ref if piece is own else slot,
            dst_ref=slot,
            send_sem=send_sem.at[len(started)],
            recv_sem=arrived,
            device_id=device,
            device_id_type=MESH,
        )
        copy.start()
        started.append(copy)

    def arrive(plane, piece):
        slot, arrived = part(plane, piece)
        pltpu.make_async_remote_copy(
            src_ref=slot,
            dst_ref=slot,
            send_sem=send_sem.at[0],
            recv_sem=arrived,
            device_id=across,
            device_id_type=MESH,
        ).wait_recv()

    def spread(piece):
        for i, k in hood:
            send(both, piece, {"tx": 2 * i + core, "ty": t, "src": k})

    for j in far_t:
        send(both, own, along_ty(j))
    spread(own)
    send(both, own, across)

    side = []
    for n, i in enumerate(far_s):
        for m, (src, dst) in enumerate(((shift_ref, shifts_ref), (weight_ref, weights_ref))):
            copy = pltpu.make_async_remote_copy(
                src_ref=src,
                dst_ref=dst.at[s],
                send_sem=side_send.at[m, n],
                recv_sem=side_recv.at[m, s],
                device_id=along_src(i),
                device_id_type=MESH,
            )
            copy.start()
            side.append(copy)

    for load in loads[1:]:
        load.wait()
    for plane in range(2):
        all_ref[s, plane, tx, t] = spec_ref[plane]
    block = tx * src_count + s
    blocks = tx_count * src_count
    chips = pair_count * src_count
    row_table(row_ref, blend_ref.shape[1] // chips, pair * src_count + s, chips)
    col_table(col_ref, t)
    half = pupil_ref.shape[0] // 2
    pupil = pupil_ref[...].astype(jnp.float32).astype(jnp.bfloat16)
    turned = (((1,), (1,)), ((), ()))
    mask_ref[:half] = lax.dot_general(unit(half, False), pupil[:, half:], turned, preferred_element_type=jnp.float32).astype(jnp.bfloat16)
    mask_ref[half:] = lax.dot_general(unit(half, True), pupil[:, :half], turned, preferred_element_type=jnp.float32).astype(jnp.bfloat16)

    part_rows, part_cols = ty_count * spec_ref.shape[1], spec_ref.shape[2]

    def turn(i, k):
        cell = jnp.concatenate([all_ref[k, plane, i].reshape(part_rows, part_cols) for plane in range(2)], axis=0)
        for back, target in enumerate((turned_ref, mirror_ref)):
            start = (src_count - 1 - k if back else k) * part_cols
            rows = pl.ds(pl.multiple_of(start, part_cols), part_cols)
            value = lax.dot_general(unit(part_cols, back), cell, turned, preferred_element_type=jnp.float32)
            for plane in range(2):
                tile = value[:, plane * part_rows : (plane + 1) * part_rows]
                target[plane * tx_count + i, rows] = tile
                target[(plane + 2) * tx_count + i, rows] = -tile

    def pass_on(i, j, k, also=None):
        piece = (2 * i + core, j, k)
        arrive(both, piece)
        if also is not None:
            send(both, piece, along_ty(also))
        send(both, piece, across)

    mate, far_t = far_t[0], far_t[1:]
    near, distant = hood[1:], hood[:1]
    for i, k in near:
        pass_on(i, t, k, mate)
    for n, j in enumerate(far_t):
        arrive(both, (tx, j, s))
        spread((tx, j, s))
        if n == 0:
            for i, k in distant:
                pass_on(i, t, k, mate)
    for j in [mate] + far_t:
        if j is mate:
            arrive(both, (tx, j, s))
        send(both, (tx, j, s), across)
    turn(tx, s)
    for n, i in enumerate(far_s):
        for m, (src, dst) in enumerate(((shift_ref, shifts_ref), (weight_ref, weights_ref))):
            pltpu.make_async_remote_copy(
                src_ref=src,
                dst_ref=dst.at[i],
                send_sem=side_send.at[m, n],
                recv_sem=side_recv.at[m, i],
                device_id=across,
                device_id_type=MESH,
            ).wait_recv()
    list_live(live_ref, shifts_ref, weights_ref)
    blend_table(blend_ref, block, blocks, src_count)
    near_first = [t, mate] + far_t
    for j in near_first:
        arrive(both, (2 * pair + other_core, j, s))
    turn(2 * pair + other_core, s)
    for i, k in near + distant:
        pass_on(i, mate, k)
    for j in far_t:
        for i, k in near + distant:
            pass_on(i, j, k)
    for i, k in near + distant:
        turn(2 * i + core, k)
    for j in near_first:
        for i, k in near + distant:
            arrive(both, (2 * i + other_core, j, k))
    for i, k in near + distant:
        turn(2 * i + other_core, k)
    for copy in started + side:
        copy.wait_send()


def gather(spectrum, source_shifts, source_weights, pupil_mask, sizes, cols):
    tx_count, ty_count, src_count = sizes
    pair_count = tx_count // 2
    _, block_rows, block_cols = spectrum.shape
    slots = source_weights.shape[0]
    length = pupil_mask.shape[0]
    blocks = tx_count * src_count
    samples = 2 * length
    width = pl.cdiv(src_count * slots + (UNROLL + TAIL + 2 + SHARED) * CORES * GROUP + 1, LANES) * LANES
    vmem = pl.BlockSpec(memory_space=pltpu.VMEM)
    lines = pair_count * src_count * ty_count
    sends = ty_count - 1 + lines + ty_count * (src_count - 1 + pair_count - 1)
    sends += 3 * ty_count * (src_count - 1) * (pair_count - 1)
    return pl.pallas_call(
        functools.partial(gather_kernel, sizes),
        out_shape=(
            jax.ShapeDtypeStruct((4 * tx_count, src_count * block_cols, ty_count * block_rows), jnp.float32),
            jax.ShapeDtypeStruct((4 * tx_count, src_count * block_cols, ty_count * block_rows), jnp.float32),
            jax.ShapeDtypeStruct((1, width), jnp.int32),
            jax.ShapeDtypeStruct((length, 2 * LANES), jnp.bfloat16),
            jax.ShapeDtypeStruct((cols, length), jnp.bfloat16),
            jax.ShapeDtypeStruct((length, length), jnp.bfloat16),
            jax.ShapeDtypeStruct((FRAME // blocks + 2 * EDGE, samples), jnp.bfloat16),
        ),
        in_specs=[pl.BlockSpec(memory_space=pltpu.HBM)] * 4,
        out_specs=(vmem,) * 7,
        scratch_shapes=[
            pltpu.VMEM((src_count, 2, slots), jnp.int32),
            pltpu.VMEM((src_count, 1, slots), jnp.int32),
            pltpu.VMEM((src_count, 2, tx_count, ty_count, block_rows, block_cols), jnp.bfloat16),
            pltpu.VMEM(spectrum.shape, jnp.bfloat16),
            pltpu.VMEM(pupil_mask.shape, jnp.int32),
            pltpu.SemaphoreType.DMA((4,)),
            pltpu.SemaphoreType.DMA((sends,)),
            pltpu.SemaphoreType.DMA((2, src_count, tx_count, ty_count)),
            pltpu.SemaphoreType.DMA((2, src_count)),
            pltpu.SemaphoreType.DMA((2, src_count)),
        ],
        compiler_params=pltpu.CompilerParams(collective_id=0, has_side_effects=True, vmem_limit_bytes=24 << 20),
        name="gather",
    )(*(pltpu.with_memory_space_constraint(a, pltpu.HBM) for a in (spectrum, source_shifts.T, source_weights[None], pupil_mask)))


def stages(sizes, spec, mirror, mask_ref, row_ref, col_ref, live):
    half = col_ref.shape[1] // 2
    height = spec.shape[1]
    tiles = spec.shape[0] // 4
    tx = lax.axis_index("tx")
    core = lax.rem(tx, CORES)
    power = lax.rem(tx // CORES * sizes[2] + lax.axis_index("src"), 4)
    flip = 2 * lax.rem(power, 2)
    middle = (lax.rem(4 - power, 4), power + 1 - 2 * lax.rem(power, 2))
    lane = iota((half, LANES), 1)

    def mine(n):
        return [live[0, SHARED * GROUP + (n * GROUP + g) * CORES + core] for g in range(GROUP)]

    def shared(n):
        return [live[0, n * GROUP + g] for g in range(GROUP)]

    def cross(words, slot):
        for g, word in enumerate(words):
            a, b = word & 1023, (word >> 10) & 1023
            tile, rest = a // LANES, lax.rem(a, LANES)
            keep = lane >= rest
            last = jnp.minimum(tile + 2, tiles - 1)

            def window(source, start, part):
                rows = pl.ds(start, half)
                low = pltpu.roll(mask_ref[part * half : (part + 1) * half, :LANES], rest, 1)
                high = pltpu.roll(mask_ref[part * half : (part + 1) * half, LANES:], rest, 1)
                ends = jnp.where(keep, low, high)
                centre = jnp.where(keep, high, low)
                found = []
                for plane in range(2):
                    outer = jnp.where(keep, source[plane * tiles + tile, rows, :], source[(plane + flip) * tiles + last, rows, :])
                    between = source[middle[plane] * tiles + tile + 1, rows, :]
                    found.append(outer.astype(jnp.bfloat16) * ends + between.astype(jnp.bfloat16) * centre)
                return found

            upper = window(spec, b + half, 0)
            lower = window(mirror, height - half - b, 1)
            even = jnp.concatenate([upper[0] + lower[0], upper[1] + lower[1]], axis=1)
            odd = jnp.concatenate([lower[1] - upper[1], upper[0] - lower[0]], axis=1)
            slot[g, :half] = dot(even, row_ref[...]).astype(jnp.bfloat16)
            slot[g, half:] = dot(odd, row_ref[...]).astype(jnp.bfloat16)

    def square(words, source, acc):
        tall = col_ref.shape[0] // 2
        scale = [(word >> 20).astype(jnp.float32) for word in words]
        for part in range(2):
            rows = slice(part * tall, (part + 1) * tall)
            total = acc[rows]
            for g in range(GROUP):
                wide = dot(col_ref[rows], source[g])
                real, imag = wide[:, :LANES], wide[:, LANES:]
                total += scale[g] * (real * real + imag * imag)
            acc[rows] = total

    return mine, shared, cross, square


def image_kernel(
    sizes, live_ref, spec, mirror, mask_ref, row_ref, col_ref, acc, next_inner,
    live, other_inner, live_sem,
):
    load = pltpu.make_async_copy(live_ref, live, live_sem)
    load.start()
    mine, shared, cross, square = stages(sizes, spec, mirror, mask_ref, row_ref, col_ref, live)
    inner = (other_inner, next_inner)
    acc[...] = jnp.zeros_like(acc)
    next_inner[...] = jnp.zeros_like(next_inner)
    load.wait()

    def run(start, count, steps):
        def turn_body(turn_index, carry):
            for g in range(steps):
                n = start + turn_index * steps + g
                cross(mine(n), inner[g % 2])
                square(mine(n - 1), inner[1 - g % 2], acc)
            return carry

        lax.fori_loop(0, count, turn_body, 0)

    full, half = turns_before_tail(live)
    run(0, full, 4)
    run(4 * full, half, 2)


def image(live, spectrum, mirror, row_table, col_table, masks, sizes):
    cols, length = col_table.shape
    vmem = pl.BlockSpec(memory_space=pltpu.VMEM)
    return pl.pallas_call(
        functools.partial(image_kernel, sizes),
        out_shape=(
            jax.ShapeDtypeStruct((cols, LANES), jnp.float32),
            jax.ShapeDtypeStruct((GROUP, length, 2 * LANES), jnp.bfloat16),
        ),
        in_specs=[vmem] * 6,
        out_specs=(vmem,) * 2,
        scratch_shapes=[
            pltpu.SMEM(live.shape, jnp.int32),
            pltpu.VMEM((GROUP, length, 2 * LANES), jnp.bfloat16),
            pltpu.SemaphoreType.DMA(()),
        ],
        compiler_params=pltpu.CompilerParams(vmem_limit_bytes=12 << 20),
        name="image",
    )(live, spectrum, mirror, masks, row_table, col_table)


def exchange_kernel(
    sizes, sources, live_ref, acc, first_inner, spec, mirror, mask_ref, row_ref, col_ref, all_ref, beside,
    live, total, part_ref, same_ref, other_ref, own_ref, strip_ref, inner, part_sem, live_sem, send_sem, recv_sem, side_send, side_recv,
):
    tx_count, ty_count, src_count = sizes
    pair_count = tx_count // 2
    tx, t, s = lax.axis_index("tx"), lax.axis_index("ty"), lax.axis_index("src")
    pair, core = tx // 2, lax.rem(tx, 2)
    far_s = [s] + others(s, src_count)
    far_pair = [pair] + others(pair, pair_count)
    chips = [(i, k) for k in far_s for i in far_pair]

    def device(chip, other, z):
        return {"tx": 2 * chip[0] + (1 - core if other else core), "ty": z, "src": chip[1]}

    def block(chip, other):
        return (2 * chip[0] + (1 - core if other else core)) * src_count + chip[1]

    across = device(chips[0], True, t)
    barrier = pltpu.get_barrier_semaphore()

    def greet(chip, z):
        pl.semaphore_signal(barrier, inc=1, device_id=device(chip, False, z), device_id_type=MESH)

    load = pltpu.make_async_copy(live_ref, live, live_sem)
    load.start()
    has = (t > 0, t < ty_count - 1)
    beside[...] = jnp.zeros_like(beside)
    pl.semaphore_signal(barrier, inc=1, device_id=across, device_id_type=MESH)
    for chip in chips[1:]:
        greet(chip, t)
    for side in range(2):

        @pl.when(has[side])
        def _():
            for chip in chips:
                greet(chip, t + 2 * side - 1)

    sides = jnp.minimum(t, 1) + jnp.minimum(ty_count - 1 - t, 1)

    def copy(src, dst, send, recv, target):
        return pltpu.make_async_remote_copy(
            src_ref=src, dst_ref=dst, send_sem=send, recv_sem=recv, device_id=target, device_id_type=MESH
        )

    mine, shared, cross, square = stages(sizes, spec, mirror, mask_ref, row_ref, col_ref, live)
    load.wait()
    full, half = turns_before_tail(live)
    n = 4 * full + 2 * half
    total[...] = acc[...]
    source_inner = first_inner
    for g in range(TAIL):
        cross(mine(n + g) if g < TAIL - 1 else shared(0), inner[g % 2])
        square(mine(n + g - 1), source_inner, total)
        source_inner = inner[g % 2]

    level = (total[...] / (2.0 * sources)).T
    count_x, cols = own_ref.shape
    for n in range(CORES):
        part_ref[n] = level[n * count_x : (n + 1) * count_x]
    pl.semaphore_wait(barrier, len(chips) * (1 + sides))
    reduce = copy(part_ref.at[1 - core], other_ref, part_sem.at[0], part_sem.at[1], across)
    reduce.start()
    total[...] = jnp.zeros_like(total)
    for g in range(SHARED):
        if g < SHARED - 1:
            cross(shared(g + 1), inner[(TAIL + g) % 2])
        square(shared(g), source_inner, total)
        source_inner = inner[(TAIL + g) % 2]
    level = (total[...] / (2.0 * sources)).T
    for n in range(CORES):
        same_ref[n] = level[n * count_x : (n + 1) * count_x]
    reduce.wait()
    level = part_ref[core] + other_ref[...] + same_ref[core]
    own = level.astype(jnp.bfloat16)
    own_ref[...] = own
    strip_ref[0] = level[:, :LANES].T[:PACK].astype(jnp.bfloat16)
    strip_ref[1] = level[:, cols - LANES :].T[LANES - PACK :].astype(jnp.bfloat16)
    all_ref[block(chips[0], False)] = own
    def level_copy(n, chip, other, target, own=False):
        at = block(chip, other)
        return copy(own_ref if own else all_ref.at[at], all_ref.at[at], send_sem.at[n], recv_sem.at[at], target)

    def side_copy(n, side, chip, other, target, own=False):
        at = block(chip, other)
        slot = beside.at[side, at]
        return copy(strip_ref.at[1 - side] if own else slot, slot, side_send.at[side, n], side_recv.at[side, at], target)

    started = []
    for side in range(2):

        @pl.when(has[1 - side])
        def _():
            for n, chip in enumerate(chips):
                side_copy(n, side, chips[0], False, device(chip, False, t + 1 - 2 * side), True).start()

    for n, chip in enumerate(chips[:0:-1]):
        started.append(level_copy(n, chips[0], False, device(chip, False, t), True))
        started[-1].start()
    n = len(chips) - 1
    started.append(level_copy(n, chips[0], False, across, True))
    started[-1].start()
    for chip in chips[1:]:
        n += 1
        level_copy(0, chip, False, across).wait_recv()
        started.append(level_copy(n, chip, False, across))
        started[-1].start()
    for side in range(2):

        @pl.when(has[side])
        def _():
            for n, chip in enumerate(chips):
                side_copy(0, side, chip, False, across).wait_recv()
                side_copy(len(chips) + n, side, chip, False, across).start()

    for chip in chips:
        level_copy(0, chip, True, across).wait_recv()
    for side in range(2):

        @pl.when(has[side])
        def _():
            for n, chip in enumerate(chips):
                side_copy(0, side, chip, True, across).wait_recv()
                side_copy(len(chips) + n, side, chip, False, across).wait_send()

        @pl.when(has[1 - side])
        def _():
            for n, chip in enumerate(chips):
                side_copy(n, side, chips[0], False, device(chip, False, t + 1 - 2 * side), True).wait_send()

    for one in started:
        one.wait_send()


def exchange(sources, live, acc, inner, spectrum, mirror, masks, row_table, col_table, count_x, sizes):
    tx_count, ty_count, src_count = sizes
    blocks = tx_count * src_count
    vmem = pl.BlockSpec(memory_space=pltpu.VMEM)
    cols = acc.shape[0]
    return pl.pallas_call(
        functools.partial(exchange_kernel, sizes, sources),
        out_shape=(
            jax.ShapeDtypeStruct((blocks, count_x, cols), jnp.bfloat16),
            jax.ShapeDtypeStruct((2, blocks, PACK, count_x), jnp.bfloat16),
        ),
        in_specs=[vmem] * 8,
        out_specs=(vmem,) * 2,
        scratch_shapes=[
            pltpu.SMEM(live.shape, jnp.int32),
            pltpu.VMEM(acc.shape, jnp.float32),
            pltpu.VMEM((CORES, count_x, cols), jnp.float32),
            pltpu.VMEM((CORES, count_x, cols), jnp.float32),
            pltpu.VMEM((count_x, cols), jnp.float32),
            pltpu.VMEM((count_x, cols), jnp.bfloat16),
            pltpu.VMEM((2, PACK, count_x), jnp.bfloat16),
            [pltpu.VMEM(inner.shape, jnp.bfloat16)] * 2,
            pltpu.SemaphoreType.DMA((2,)),
            pltpu.SemaphoreType.DMA(()),
            pltpu.SemaphoreType.DMA((blocks,)),
            pltpu.SemaphoreType.DMA((blocks,)),
            pltpu.SemaphoreType.DMA((2, blocks)),
            pltpu.SemaphoreType.DMA((2, blocks)),
        ],
        compiler_params=pltpu.CompilerParams(collective_id=1, has_side_effects=True, vmem_limit_bytes=12 << 20),
        name="exchange",
    )(live, acc, inner, spectrum, mirror, masks, row_table, col_table)


def diffuse_kernel(sizes, all_ref, beside, blend_ref, out_ref, first, second):
    tx_count, ty_count, src_count = sizes
    rows, cols = out_ref.shape
    blocks, count, _ = all_ref.shape
    samples = blocks * count
    tall = rows + 2 * EDGE
    tiles = cols // LANES
    row_block = lax.axis_index("tx") * src_count + lax.axis_index("src")
    col_block = lax.axis_index("ty")
    lane = iota((1, LANES), 1)

    def inside(start, size, tile):
        x = row_block * rows - EDGE + start + iota((size, 1), 0)
        y = col_block * cols + tile * LANES + lane
        if tile == tiles:
            y = jnp.where(lane >= LANES // 2, y - cols - LANES, y)
        return (x >= 0) & (x < blocks * rows) & (y >= 0) & (y < ty_count * cols)

    def keep(target, start, tile, value):
        size = value.shape[0]
        target[tile, EDGE + start : EDGE + start + size] = jnp.where(inside(start, size, tile), value, 0.0)

    level = all_ref[...].reshape(samples, cols)
    sides = [jnp.concatenate([beside[side, n] for n in range(blocks)], axis=1) for side in range(2)]
    strip = jnp.concatenate([sides[1], jnp.zeros((LANES - 2 * PACK, samples), jnp.bfloat16), sides[0]], axis=0)
    edge = lax.dot_general(blend_ref[...], strip, (((1,), (1,)), ((), ())), preferred_element_type=jnp.float32)
    keep(first, 0, tiles, 1.0 - jnp.exp(-edge))
    cut = pl.cdiv(tall, 2 * PACK) * PACK
    for start, stop in ((0, cut), (cut, tall)):
        middle = 1.0 - jnp.exp(-dot(blend_ref[start:stop], level))
        for tile in range(tiles):
            keep(first, start, tile, middle[:, tile * LANES : (tile + 1) * LANES])

    def spread(source, start, size, wanted):
        at = EDGE + start
        centre = [source[tile, at : at + size] for tile in range(tiles + 1)]
        after = [pltpu.roll(value, 1, 1) for value in centre]
        ahead = [pltpu.roll(value, LANES - 1, 1) for value in centre]
        for tile in wanted:
            left = jnp.where(lane == 0, after[tile - 1], after[tile])
            right = jnp.where(lane == LANES - 1, ahead[(tile + 1) % (tiles + 1)], ahead[tile])
            near = source[tile, at - 1 : at - 1 + size] + source[tile, at + 1 : at + 1 + size] + left + right
            yield tile, centre[tile] + diffusion_rate * (near - 4.0 * centre[tile])

    chunk = min(rows, 64)
    for start in range(0, tall, chunk):
        size = min(chunk, tall - start)
        for tile, value in spread(first, start, size, range(tiles + 1)):
            keep(second, start, tile, value)
    for start in range(0, rows, chunk):
        for tile, value in spread(second, EDGE + start, chunk, range(tiles)):
            out_ref[start : start + chunk, tile * LANES : (tile + 1) * LANES] = value


def diffuse(levels, beside, blend, sizes):
    rows = blend.shape[0] - 2 * EDGE
    cols = levels.shape[2]
    vmem = pl.BlockSpec(memory_space=pltpu.VMEM)
    return pl.pallas_call(
        functools.partial(diffuse_kernel, sizes),
        out_shape=jax.ShapeDtypeStruct((rows, cols), jnp.float32),
        in_specs=[vmem] * 3,
        out_specs=vmem,
        scratch_shapes=[pltpu.VMEM((cols // LANES + 1, rows + 4 * EDGE, LANES), jnp.float32)] * 2,
        compiler_params=pltpu.CompilerParams(vmem_limit_bytes=12 << 20),
        name="diffuse",
    )(levels, beside, blend)


def body(sizes, cols, spectrum, pupil_mask, source_shifts, source_weights):
    turned, mirror, live, row_table, col_table, masks, blend = gather(
        spectrum, source_shifts, source_weights, pupil_mask, sizes, cols
    )
    sources = source_weights.shape[0] * sizes[2]
    count_x = blend.shape[1] // (sizes[0] * sizes[2])
    acc, inner = image(live, turned, mirror, row_table, col_table, masks, sizes)
    levels, beside = exchange(
        sources, live, acc, inner, turned, mirror, masks, row_table, col_table, count_x, sizes
    )
    return diffuse(levels, beside, blend, sizes)


def solution(mesh):
    sizes = (mesh.shape["tx"], mesh.shape["ty"], mesh.shape["src"])
    placed = (P(None, ("tx", "ty"), "src"), P(), P("src", None), P("src"))
    return jax.shard_map(
        functools.partial(body, sizes, COLS),
        mesh=mesh,
        in_specs=placed,
        out_specs=P(("tx", "src"), "ty"),
        check_vma=False,
    )
```

```python
import functools
import math

import jax
import jax.numpy as jnp
from jax import lax
from jax.experimental import pallas as pl
from jax.experimental.pallas import tpu as pltpu
from jax.sharding import PartitionSpec as P

FRAME = 2048
LANES = 128
COLS = 256
EDGE = 8
PACK = 16
CORES = 2
GROUP = 2
UNROLL = 4
TAIL = 8
SHARED = 4
MESH = pl.DeviceIdType.MESH

diffusion_rate = 0.2


def wave(turns, period):
    quarter = period // 4
    turn = (turns + quarter // 2) // quarter
    angle = (turns - turn * quarter).astype(jnp.float32) * (2 * math.pi / period)
    square = angle * angle
    sine = angle * (1 + square * (-1 / 6 + square * (1 / 120 + square * (-1 / 5040 + square / 362880))))
    cosine = 1 + square * (-1 / 2 + square * (1 / 24 + square * (-1 / 720 + square / 40320)))
    odd = (turn & 1) == 1
    first, second = jnp.where(odd, sine, cosine), jnp.where(odd, cosine, sine)
    return jnp.where(((turn + 1) & 2) == 2, -first, first), jnp.where((turn & 2) == 2, -second, second)


def iota(shape, dim):
    return lax.broadcasted_iota(jnp.int32, shape, dim)


def dot(a, b):
    return jnp.dot(a, b, preferred_element_type=jnp.float32)


def unit(size, back):
    rows, cols = iota((size, size), 0), iota((size, size), 1)
    return jnp.where(rows + cols == size - 1 if back else rows == cols, 1.0, 0.0).astype(jnp.bfloat16)


def flip_bits(index, mask):
    bit = 1
    while bit <= mask:
        if mask & bit:
            index = index + bit * (1 - 2 * lax.rem(index // bit, 2))
        bit *= 2
    return index


def others(index, count):
    if count & (count - 1) == 0:
        return [flip_bits(index, d) for d in range(1, count)]
    return [lax.rem(index + d, count) for d in range(1, count)]


def mates(index, count):
    orders = [
        sorted((i for i in range(count) if i != at), key=lambda i: (i != at ^ 1, abs(i - at), i)) for at in range(count)
    ]
    return [sum(jnp.where(index == at, orders[at][n], 0) for at in range(count)) for n in range(count - 1)]


def row_table(row_ref, count, chip, chips):
    half = row_ref.shape[0] // 2
    step = FRAME // (count * chips)
    sample = iota((half, LANES), 1)
    x = step * (chips * sample + chip)
    cosine, sine = wave((x * iota((half, LANES), 0)) & (FRAME - 1), FRAME)
    cosine = jnp.where(sample < count, cosine, 0.0).astype(jnp.bfloat16)
    sine = jnp.where(sample < count, sine, 0.0).astype(jnp.bfloat16)
    row_ref[:half, :LANES] = cosine
    row_ref[:half, LANES:] = sine
    row_ref[half:, :LANES] = -sine
    row_ref[half:, LANES:] = cosine


def col_table(col_ref, t):
    cols, half = col_ref.shape[0], col_ref.shape[1] // 2
    chunk = 64

    def fill(n, carry):
        start = pl.multiple_of(n * chunk, chunk)
        y = t * cols + start + iota((chunk, half), 0)
        cosine, sine = wave((y * (2 * iota((chunk, half), 1) + 1)) & (2 * FRAME - 1), 2 * FRAME)
        col_ref[pl.ds(start, chunk), :half] = cosine.astype(jnp.bfloat16)
        col_ref[pl.ds(start, chunk), half:] = sine.astype(jnp.bfloat16)
        return carry

    lax.fori_loop(0, cols // chunk, fill, 0)


def list_live(live_ref, shifts_ref, weights_ref):
    src_count, _, slots = shifts_ref.shape
    width = live_ref.shape[1]
    weights = weights_ref[:, 0, :].astype(jnp.float32)
    words = shifts_ref[:, 0, :].astype(jnp.float32) + shifts_ref[:, 1, :].astype(jnp.float32) * 1024.0 + weights * 1048576.0
    on = jnp.where(weights > 0, 1.0, 0.0)
    ahead = jnp.where(iota((slots, slots), 0) < iota((slots, slots), 1), 1.0, 0.0)
    rank = dot(on.astype(jnp.bfloat16), ahead.astype(jnp.bfloat16))
    before = jnp.zeros((1, 1), jnp.float32)
    ranks = []
    for k in range(src_count):
        ranks.append(rank[k : k + 1] + before)
        before = before + jnp.sum(on[k : k + 1], axis=1, keepdims=True)
    rank = jnp.where(on > 0, jnp.concatenate(ranks, axis=0), -1.0).T
    words = words.T
    place = iota((slots, width), 1).astype(jnp.float32)
    total = jnp.zeros((slots, width), jnp.float32)
    for k in range(src_count):
        total += jnp.where(rank[:, k : k + 1] == place, words[:, k : k + 1], 0.0)
    found = jnp.sum(total, axis=0, keepdims=True)
    live_ref[...] = jnp.where(iota((1, width), 1) == width - 1, before, found).astype(jnp.int32)


def turns_before_tail(live):
    count = jnp.maximum(live[0, live.shape[1] - 1] - SHARED * GROUP, 0)
    steps = jnp.maximum((count + CORES * GROUP - 1) // (CORES * GROUP) + 1 - TAIL, 0) + 1
    return steps // 4, lax.rem(steps, 4) // 2


def blend_table(blend_ref, block, blocks, src_count):
    tall, samples = blend_ref.shape
    rows = tall - 2 * EDGE
    step = FRAME // samples
    count = samples // blocks
    chunk = PACK

    def fill(n, carry):
        start = pl.multiple_of(n * chunk, chunk)
        x = block * rows - EDGE + start + iota((chunk, samples), 0)
        column = iota((chunk, samples), 1)
        owner = column // count
        line = owner // src_count
        chip = (line // CORES) * src_count + owner - line * src_count
        place = (line & (CORES - 1)) * count + column - owner * count
        gap = x - step * (blocks // CORES * place + chip)
        gap = ((gap + FRAME // 2) & (FRAME - 1)) - FRAME // 2
        cosine, sine = wave(gap, 2 * FRAME)
        place = block * rows - EDGE + start + iota((chunk, 1), 0)
        place = place & (2 * step - 1)
        scale = jnp.zeros((chunk, 1), jnp.float32)
        for n in range(2 * step):
            if n % step:
                scale = jnp.where(place == n, math.sin(math.pi * n / step) / samples, scale)
        scale = jnp.where((chip & 1) == 1, -scale, scale)
        here = gap == 0
        table = jnp.where(here, 1.0, scale * cosine / jnp.where(here, 1.0, sine))
        blend_ref[pl.ds(start, chunk)] = table.astype(jnp.bfloat16)
        return carry

    lax.fori_loop(0, tall // chunk, fill, 0)


def gather_kernel(
    sizes, spec_hbm, shift_ref, weight_ref, pupil_hbm, turned_ref, mirror_ref, live_ref, row_ref, col_ref, mask_ref, blend_ref,
    shifts_ref, weights_ref, all_ref, spec_ref, pupil_ref, local_sem, send_sem, recv_sem, side_send, side_recv,
):
    tx_count, ty_count, src_count = sizes
    pair_count = tx_count // 2
    tx, t, s = lax.axis_index("tx"), lax.axis_index("ty"), lax.axis_index("src")
    pair, core = tx // 2, lax.rem(tx, 2)
    other_core = 1 - core
    far_t = mates(t, ty_count)
    far_s = others(s, src_count)
    far_pair = others(pair, pair_count)

    def along_ty(i):
        return {"tx": tx, "ty": i, "src": s}

    def along_src(i):
        return {"tx": tx, "ty": t, "src": i}

    loads = [
        pltpu.make_async_copy(src, dst, local_sem.at[n])
        for n, (src, dst) in enumerate(
            (
                (spec_hbm, spec_ref),
                (pupil_hbm, pupil_ref),
                (shift_ref, shifts_ref.at[s]),
                (weight_ref, weights_ref.at[s]),
            )
        )
    ]
    for load in loads:
        load.start()

    across = {"tx": 2 * pair + other_core, "ty": t, "src": s}
    hood = [(i, k) for k in far_s + [s] for i in far_pair + [pair] if i is not pair or k is not s]
    partners = [along_ty(i) for i in far_t] + [{"tx": 2 * i + core, "ty": t, "src": k} for i, k in hood] + [across]
    barrier = pltpu.get_barrier_semaphore()
    for partner in partners:
        pl.semaphore_signal(barrier, inc=1, device_id=partner, device_id_type=MESH)
    pl.semaphore_wait(barrier, len(partners))
    loads[0].wait()

    started = []
    own = (tx, t, s)

    both = slice(None)

    def part(plane, piece):
        i, j, k = piece
        return all_ref.at[k, plane, i, j], recv_sem.at[0, k, i, j]

    def send(plane, piece, device):
        slot, arrived = part(plane, piece)
        copy = pltpu.make_async_remote_copy(
            src_ref=spec_ref if piece is own else slot,
            dst_ref=slot,
            send_sem=send_sem.at[len(started)],
            recv_sem=arrived,
            device_id=device,
            device_id_type=MESH,
        )
        copy.start()
        started.append(copy)

    def arrive(plane, piece):
        slot, arrived = part(plane, piece)
        pltpu.make_async_remote_copy(
            src_ref=slot,
            dst_ref=slot,
            send_sem=send_sem.at[0],
            recv_sem=arrived,
            device_id=across,
            device_id_type=MESH,
        ).wait_recv()

    def spread(piece):
        for i, k in hood:
            send(both, piece, {"tx": 2 * i + core, "ty": t, "src": k})

    for j in far_t:
        send(both, own, along_ty(j))
    spread(own)
    send(both, own, across)

    side = []
    for n, i in enumerate(far_s):
        for m, (src, dst) in enumerate(((shift_ref, shifts_ref), (weight_ref, weights_ref))):
            copy = pltpu.make_async_remote_copy(
                src_ref=src,
                dst_ref=dst.at[s],
                send_sem=side_send.at[m, n],
                recv_sem=side_recv.at[m, s],
                device_id=along_src(i),
                device_id_type=MESH,
            )
            copy.start()
            side.append(copy)

    for load in loads[1:]:
        load.wait()
    for plane in range(2):
        all_ref[s, plane, tx, t] = spec_ref[plane]
    block = tx * src_count + s
    blocks = tx_count * src_count
    chips = pair_count * src_count
    row_table(row_ref, blend_ref.shape[1] // chips, pair * src_count + s, chips)
    col_table(col_ref, t)
    half = pupil_ref.shape[0] // 2
    pupil = pupil_ref[...].astype(jnp.float32).astype(jnp.bfloat16)
    turned = (((1,), (1,)), ((), ()))
    mask_ref[:half] = lax.dot_general(unit(half, False), pupil[:, half:], turned, preferred_element_type=jnp.float32).astype(jnp.bfloat16)
    mask_ref[half:] = lax.dot_general(unit(half, True), pupil[:, :half], turned, preferred_element_type=jnp.float32).astype(jnp.bfloat16)

    part_rows, part_cols = ty_count * spec_ref.shape[1], spec_ref.shape[2]

    def turn(i, k):
        cell = jnp.concatenate([all_ref[k, plane, i].reshape(part_rows, part_cols) for plane in range(2)], axis=0)
        for back, target in enumerate((turned_ref, mirror_ref)):
            start = (src_count - 1 - k if back else k) * part_cols
            rows = pl.ds(pl.multiple_of(start, part_cols), part_cols)
            value = lax.dot_general(unit(part_cols, back), cell, turned, preferred_element_type=jnp.float32)
            for plane in range(2):
                tile = value[:, plane * part_rows : (plane + 1) * part_rows]
                target[plane * tx_count + i, rows] = tile
                target[(plane + 2) * tx_count + i, rows] = -tile

    def pass_on(i, j, k, also=None):
        piece = (2 * i + core, j, k)
        arrive(both, piece)
        if also is not None:
            send(both, piece, along_ty(also))
        send(both, piece, across)

    mate, far_t = far_t[0], far_t[1:]
    near, distant = hood[1:], hood[:1]
    for i, k in near:
        pass_on(i, t, k, mate)
    for n, j in enumerate(far_t):
        arrive(both, (tx, j, s))
        spread((tx, j, s))
        if n == 0:
            for i, k in distant:
                pass_on(i, t, k, mate)
    for j in [mate] + far_t:
        if j is mate:
            arrive(both, (tx, j, s))
        send(both, (tx, j, s), across)
    turn(tx, s)
    for n, i in enumerate(far_s):
        for m, (src, dst) in enumerate(((shift_ref, shifts_ref), (weight_ref, weights_ref))):
            pltpu.make_async_remote_copy(
                src_ref=src,
                dst_ref=dst.at[i],
                send_sem=side_send.at[m, n],
                recv_sem=side_recv.at[m, i],
                device_id=across,
                device_id_type=MESH,
            ).wait_recv()
    list_live(live_ref, shifts_ref, weights_ref)
    blend_table(blend_ref, block, blocks, src_count)
    near_first = [t, mate] + far_t
    for j in near_first:
        arrive(both, (2 * pair + other_core, j, s))
    turn(2 * pair + other_core, s)
    for i, k in near + distant:
        pass_on(i, mate, k)
    for j in far_t:
        for i, k in near + distant:
            pass_on(i, j, k)
    for i, k in near + distant:
        turn(2 * i + core, k)
    for j in near_first:
        for i, k in near + distant:
            arrive(both, (2 * i + other_core, j, k))
    for i, k in near + distant:
        turn(2 * i + other_core, k)
    for copy in started + side:
        copy.wait_send()


def gather(spectrum, source_shifts, source_weights, pupil_mask, sizes, cols):
    tx_count, ty_count, src_count = sizes
    pair_count = tx_count // 2
    _, block_rows, block_cols = spectrum.shape
    slots = source_weights.shape[0]
    length = pupil_mask.shape[0]
    blocks = tx_count * src_count
    samples = 2 * length
    width = pl.cdiv(src_count * slots + (UNROLL + TAIL + 2 + SHARED) * CORES * GROUP + 1, LANES) * LANES
    vmem = pl.BlockSpec(memory_space=pltpu.VMEM)
    lines = pair_count * src_count * ty_count
    sends = ty_count - 1 + lines + ty_count * (src_count - 1 + pair_count - 1)
    sends += 3 * ty_count * (src_count - 1) * (pair_count - 1)
    return pl.pallas_call(
        functools.partial(gather_kernel, sizes),
        out_shape=(
            jax.ShapeDtypeStruct((4 * tx_count, src_count * block_cols, ty_count * block_rows), jnp.float32),
            jax.ShapeDtypeStruct((4 * tx_count, src_count * block_cols, ty_count * block_rows), jnp.float32),
            jax.ShapeDtypeStruct((1, width), jnp.int32),
            jax.ShapeDtypeStruct((length, 2 * LANES), jnp.bfloat16),
            jax.ShapeDtypeStruct((cols, length), jnp.bfloat16),
            jax.ShapeDtypeStruct((length, length), jnp.bfloat16),
            jax.ShapeDtypeStruct((FRAME // blocks + 2 * EDGE, samples), jnp.bfloat16),
        ),
        in_specs=[pl.BlockSpec(memory_space=pltpu.HBM)] * 4,
        out_specs=(vmem,) * 7,
        scratch_shapes=[
            pltpu.VMEM((src_count, 2, slots), jnp.int32),
            pltpu.VMEM((src_count, 1, slots), jnp.int32),
            pltpu.VMEM((src_count, 2, tx_count, ty_count, block_rows, block_cols), jnp.bfloat16),
            pltpu.VMEM(spectrum.shape, jnp.bfloat16),
            pltpu.VMEM(pupil_mask.shape, jnp.int32),
            pltpu.SemaphoreType.DMA((4,)),
            pltpu.SemaphoreType.DMA((sends,)),
            pltpu.SemaphoreType.DMA((2, src_count, tx_count, ty_count)),
            pltpu.SemaphoreType.DMA((2, src_count)),
            pltpu.SemaphoreType.DMA((2, src_count)),
        ],
        compiler_params=pltpu.CompilerParams(collective_id=0, has_side_effects=True, vmem_limit_bytes=24 << 20),
        name="gather",
    )(*(pltpu.with_memory_space_constraint(a, pltpu.HBM) for a in (spectrum, source_shifts.T, source_weights[None], pupil_mask)))


def stages(sizes, spec, mirror, mask_ref, row_ref, col_ref, live):
    half = col_ref.shape[1] // 2
    height = spec.shape[1]
    tiles = spec.shape[0] // 4
    tx = lax.axis_index("tx")
    core = lax.rem(tx, CORES)
    power = lax.rem(tx // CORES * sizes[2] + lax.axis_index("src"), 4)
    flip = 2 * lax.rem(power, 2)
    middle = (lax.rem(4 - power, 4), power + 1 - 2 * lax.rem(power, 2))
    lane = iota((half, LANES), 1)

    def mine(n):
        return [live[0, SHARED * GROUP + (n * GROUP + g) * CORES + core] for g in range(GROUP)]

    def shared(n):
        return [live[0, n * GROUP + g] for g in range(GROUP)]

    def cross(words, slot):
        for g, word in enumerate(words):
            a, b = word & 1023, (word >> 10) & 1023
            tile, rest = a // LANES, lax.rem(a, LANES)
            keep = lane >= rest
            last = jnp.minimum(tile + 2, tiles - 1)

            def window(source, start, part):
                rows = pl.ds(start, half)
                low = pltpu.roll(mask_ref[part * half : (part + 1) * half, :LANES], rest, 1)
                high = pltpu.roll(mask_ref[part * half : (part + 1) * half, LANES:], rest, 1)
                ends = jnp.where(keep, low, high)
                centre = jnp.where(keep, high, low)
                found = []
                for plane in range(2):
                    outer = jnp.where(keep, source[plane * tiles + tile, rows, :], source[(plane + flip) * tiles + last, rows, :])
                    between = source[middle[plane] * tiles + tile + 1, rows, :]
                    found.append(outer.astype(jnp.bfloat16) * ends + between.astype(jnp.bfloat16) * centre)
                return found

            upper = window(spec, b + half, 0)
            lower = window(mirror, height - half - b, 1)
            even = jnp.concatenate([upper[0] + lower[0], upper[1] + lower[1]], axis=1)
            odd = jnp.concatenate([lower[1] - upper[1], upper[0] - lower[0]], axis=1)
            slot[g, :half] = dot(even, row_ref[...]).astype(jnp.bfloat16)
            slot[g, half:] = dot(odd, row_ref[...]).astype(jnp.bfloat16)

    def square(words, source, acc):
        tall = col_ref.shape[0] // 2
        scale = [(word >> 20).astype(jnp.float32) for word in words]
        for part in range(2):
            rows = slice(part * tall, (part + 1) * tall)
            total = acc[rows]
            for g in range(GROUP):
                wide = dot(col_ref[rows], source[g])
                real, imag = wide[:, :LANES], wide[:, LANES:]
                total += scale[g] * (real * real + imag * imag)
            acc[rows] = total

    return mine, shared, cross, square


def image_kernel(
    sizes, live_ref, spec, mirror, mask_ref, row_ref, col_ref, acc, next_inner,
    live, other_inner, live_sem,
):
    load = pltpu.make_async_copy(live_ref, live, live_sem)
    load.start()
    mine, shared, cross, square = stages(sizes, spec, mirror, mask_ref, row_ref, col_ref, live)
    inner = (other_inner, next_inner)
    acc[...] = jnp.zeros_like(acc)
    next_inner[...] = jnp.zeros_like(next_inner)
    load.wait()

    def run(start, count, steps):
        def turn_body(turn_index, carry):
            for g in range(steps):
                n = start + turn_index * steps + g
                cross(mine(n), inner[g % 2])
                square(mine(n - 1), inner[1 - g % 2], acc)
            return carry

        lax.fori_loop(0, count, turn_body, 0)

    full, half = turns_before_tail(live)
    run(0, full, 4)
    run(4 * full, half, 2)


def image(live, spectrum, mirror, row_table, col_table, masks, sizes):
    cols, length = col_table.shape
    vmem = pl.BlockSpec(memory_space=pltpu.VMEM)
    return pl.pallas_call(
        functools.partial(image_kernel, sizes),
        out_shape=(
            jax.ShapeDtypeStruct((cols, LANES), jnp.float32),
            jax.ShapeDtypeStruct((GROUP, length, 2 * LANES), jnp.bfloat16),
        ),
        in_specs=[vmem] * 6,
        out_specs=(vmem,) * 2,
        scratch_shapes=[
            pltpu.SMEM(live.shape, jnp.int32),
            pltpu.VMEM((GROUP, length, 2 * LANES), jnp.bfloat16),
            pltpu.SemaphoreType.DMA(()),
        ],
        compiler_params=pltpu.CompilerParams(
            vmem_limit_bytes=12 << 20
        ),
        name="image",
    )(live, spectrum, mirror, masks, row_table, col_table)


def exchange_kernel(
    sizes, sources, live_ref, acc, first_inner, spec, mirror, mask_ref, row_ref, col_ref, all_ref, beside,
    live, total, part_ref, same_ref, other_ref, own_ref, strip_ref, inner, part_sem, live_sem, send_sem, recv_sem, side_send, side_recv,
):
    tx_count, ty_count, src_count = sizes
    pair_count = tx_count // 2
    tx, t, s = lax.axis_index("tx"), lax.axis_index("ty"), lax.axis_index("src")
    pair, core = tx // 2, lax.rem(tx, 2)
    far_s = [s] + others(s, src_count)
    far_pair = [pair] + others(pair, pair_count)
    chips = [(i, k) for k in far_s for i in far_pair]

    def device(chip, other, z):
        return {"tx": 2 * chip[0] + (1 - core if other else core), "ty": z, "src": chip[1]}

    def block(chip, other):
        return (2 * chip[0] + (1 - core if other else core)) * src_count + chip[1]

    across = device(chips[0], True, t)
    barrier = pltpu.get_barrier_semaphore()

    def greet(chip, z):
        pl.semaphore_signal(barrier, inc=1, device_id=device(chip, False, z), device_id_type=MESH)

    load = pltpu.make_async_copy(live_ref, live, live_sem)
    load.start()
    has = (t > 0, t < ty_count - 1)
    beside[...] = jnp.zeros_like(beside)
    pl.semaphore_signal(barrier, inc=1, device_id=across, device_id_type=MESH)
    for chip in chips[1:]:
        greet(chip, t)
    for side in range(2):

        @pl.when(has[side])
        def _():
            for chip in chips:
                greet(chip, t + 2 * side - 1)

    sides = jnp.minimum(t, 1) + jnp.minimum(ty_count - 1 - t, 1)

    def copy(src, dst, send, recv, target):
        return pltpu.make_async_remote_copy(
            src_ref=src, dst_ref=dst, send_sem=send, recv_sem=recv, device_id=target, device_id_type=MESH
        )

    mine, shared, cross, square = stages(sizes, spec, mirror, mask_ref, row_ref, col_ref, live)
    load.wait()
    full, half = turns_before_tail(live)
    n = 4 * full + 2 * half
    total[...] = acc[...]
    source_inner = first_inner
    for g in range(TAIL):
        cross(mine(n + g) if g < TAIL - 1 else shared(0), inner[g % 2])
        square(mine(n + g - 1), source_inner, total)
        source_inner = inner[g % 2]

    level = (total[...] / (2.0 * sources)).T
    count_x, cols = own_ref.shape
    for n in range(CORES):
        part_ref[n] = level[n * count_x : (n + 1) * count_x]
    pl.semaphore_wait(barrier, len(chips) * (1 + sides))
    reduce = copy(part_ref.at[1 - core], other_ref, part_sem.at[0], part_sem.at[1], across)
    reduce.start()
    total[...] = jnp.zeros_like(total)
    for g in range(SHARED):
        if g < SHARED - 1:
            cross(shared(g + 1), inner[(TAIL + g) % 2])
        square(shared(g), source_inner, total)
        source_inner = inner[(TAIL + g) % 2]
    level = (total[...] / (2.0 * sources)).T
    for n in range(CORES):
        same_ref[n] = level[n * count_x : (n + 1) * count_x]
    reduce.wait()
    level = part_ref[core] + other_ref[...] + same_ref[core]
    own = level.astype(jnp.bfloat16)
    own_ref[...] = own
    strip_ref[0] = level[:, :LANES].T[:PACK].astype(jnp.bfloat16)
    strip_ref[1] = level[:, cols - LANES :].T[LANES - PACK :].astype(jnp.bfloat16)
    all_ref[block(chips[0], False)] = own
    def level_copy(n, chip, other, target, own=False):
        at = block(chip, other)
        return copy(own_ref if own else all_ref.at[at], all_ref.at[at], send_sem.at[n], recv_sem.at[at], target)

    def side_copy(n, side, chip, other, target, own=False):
        at = block(chip, other)
        slot = beside.at[side, at]
        return copy(strip_ref.at[1 - side] if own else slot, slot, side_send.at[side, n], side_recv.at[side, at], target)

    started = []
    for side in range(2):

        @pl.when(has[1 - side])
        def _():
            for n, chip in enumerate(chips):
                side_copy(n, side, chips[0], False, device(chip, False, t + 1 - 2 * side), True).start()

    for n, chip in enumerate(chips[:0:-1]):
        started.append(level_copy(n, chips[0], False, device(chip, False, t), True))
        started[-1].start()
    n = len(chips) - 1
    started.append(level_copy(n, chips[0], False, across, True))
    started[-1].start()
    for chip in chips[1:]:
        n += 1
        level_copy(0, chip, False, across).wait_recv()
        started.append(level_copy(n, chip, False, across))
        started[-1].start()
    for side in range(2):

        @pl.when(has[side])
        def _():
            for n, chip in enumerate(chips):
                side_copy(0, side, chip, False, across).wait_recv()
                side_copy(len(chips) + n, side, chip, False, across).start()

    for chip in chips:
        level_copy(0, chip, True, across).wait_recv()
    for side in range(2):

        @pl.when(has[side])
        def _():
            for n, chip in enumerate(chips):
                side_copy(0, side, chip, True, across).wait_recv()
                side_copy(len(chips) + n, side, chip, False, across).wait_send()

        @pl.when(has[1 - side])
        def _():
            for n, chip in enumerate(chips):
                side_copy(n, side, chips[0], False, device(chip, False, t + 1 - 2 * side), True).wait_send()

    for one in started:
        one.wait_send()


def exchange(sources, live, acc, inner, spectrum, mirror, masks, row_table, col_table, count_x, sizes):
    tx_count, ty_count, src_count = sizes
    blocks = tx_count * src_count
    vmem = pl.BlockSpec(memory_space=pltpu.VMEM)
    cols = acc.shape[0]
    return pl.pallas_call(
        functools.partial(exchange_kernel, sizes, sources),
        out_shape=(
            jax.ShapeDtypeStruct((blocks, count_x, cols), jnp.bfloat16),
            jax.ShapeDtypeStruct((2, blocks, PACK, count_x), jnp.bfloat16),
        ),
        in_specs=[vmem] * 8,
        out_specs=(vmem,) * 2,
        scratch_shapes=[
            pltpu.SMEM(live.shape, jnp.int32),
            pltpu.VMEM(acc.shape, jnp.float32),
            pltpu.VMEM((CORES, count_x, cols), jnp.float32),
            pltpu.VMEM((CORES, count_x, cols), jnp.float32),
            pltpu.VMEM((count_x, cols), jnp.float32),
            pltpu.VMEM((count_x, cols), jnp.bfloat16),
            pltpu.VMEM((2, PACK, count_x), jnp.bfloat16),
            [pltpu.VMEM(inner.shape, jnp.bfloat16)] * 2,
            pltpu.SemaphoreType.DMA((2,)),
            pltpu.SemaphoreType.DMA(()),
            pltpu.SemaphoreType.DMA((blocks,)),
            pltpu.SemaphoreType.DMA((blocks,)),
            pltpu.SemaphoreType.DMA((2, blocks)),
            pltpu.SemaphoreType.DMA((2, blocks)),
        ],
        compiler_params=pltpu.CompilerParams(collective_id=1, has_side_effects=True, vmem_limit_bytes=12 << 20),
        name="exchange",
    )(live, acc, inner, spectrum, mirror, masks, row_table, col_table)


def diffuse_kernel(sizes, all_ref, beside, blend_ref, out_ref, first, second, stage, out_sem):
    tx_count, ty_count, src_count = sizes
    rows, cols = out_ref.shape
    blocks, count, _ = all_ref.shape
    samples = blocks * count
    tall = rows + 2 * EDGE
    tiles = cols // LANES
    row_block = lax.axis_index("tx") * src_count + lax.axis_index("src")
    col_block = lax.axis_index("ty")
    lane = iota((1, LANES), 1)

    def inside(start, size, tile):
        x = row_block * rows - EDGE + start + iota((size, 1), 0)
        y = col_block * cols + tile * LANES + lane
        if tile == tiles:
            y = jnp.where(lane >= LANES // 2, y - cols - LANES, y)
        return (x >= 0) & (x < blocks * rows) & (y >= 0) & (y < ty_count * cols)

    def keep(target, start, tile, value):
        size = value.shape[0]
        target[tile, EDGE + start : EDGE + start + size] = jnp.where(inside(start, size, tile), value, 0.0)

    level = all_ref[...].reshape(samples, cols)
    sides = [jnp.concatenate([beside[side, n] for n in range(blocks)], axis=1) for side in range(2)]
    strip = jnp.concatenate([sides[1], jnp.zeros((LANES - 2 * PACK, samples), jnp.bfloat16), sides[0]], axis=0)
    edge = lax.dot_general(blend_ref[...], strip, (((1,), (1,)), ((), ())), preferred_element_type=jnp.float32)
    keep(first, 0, tiles, 1.0 - jnp.exp(-edge))
    cut = pl.cdiv(tall, 2 * PACK) * PACK
    for start, stop in ((0, cut), (cut, tall)):
        middle = 1.0 - jnp.exp(-dot(blend_ref[start:stop], level))
        for tile in range(tiles):
            keep(first, start, tile, middle[:, tile * LANES : (tile + 1) * LANES])

    def spread(source, start, size, wanted):
        at = EDGE + start
        centre = [source[tile, at : at + size] for tile in range(tiles + 1)]
        after = [pltpu.roll(value, 1, 1) for value in centre]
        ahead = [pltpu.roll(value, LANES - 1, 1) for value in centre]
        for tile in wanted:
            left = jnp.where(lane == 0, after[tile - 1], after[tile])
            right = jnp.where(lane == LANES - 1, ahead[(tile + 1) % (tiles + 1)], ahead[tile])
            near = source[tile, at - 1 : at - 1 + size] + source[tile, at + 1 : at + 1 + size] + left + right
            yield tile, centre[tile] + diffusion_rate * (near - 4.0 * centre[tile])

    chunk = min(rows, 64)
    for start in range(0, tall, chunk):
        size = min(chunk, tall - start)
        for tile, value in spread(first, start, size, range(tiles + 1)):
            keep(second, start, tile, value)
    copies = []
    for start in range(0, rows, chunk):
        for tile, value in spread(second, EDGE + start, chunk, range(tiles)):
            stage[start : start + chunk, tile * LANES : (tile + 1) * LANES] = value
        part = pl.ds(start, chunk)
        copies.append(pltpu.make_async_copy(stage.at[part], out_ref.at[part], out_sem.at[start // chunk]))
        copies[-1].start()
    for copy in copies:
        copy.wait()


def diffuse(levels, beside, blend, sizes):
    rows = blend.shape[0] - 2 * EDGE
    cols = levels.shape[2]
    vmem = pl.BlockSpec(memory_space=pltpu.VMEM)
    return pl.pallas_call(
        functools.partial(diffuse_kernel, sizes),
        out_shape=jax.ShapeDtypeStruct((rows, cols), jnp.float32),
        in_specs=[vmem] * 3,
        out_specs=pl.BlockSpec(memory_space=pltpu.HBM),
        scratch_shapes=[pltpu.VMEM((cols // LANES + 1, rows + 4 * EDGE, LANES), jnp.float32)] * 2
        + [pltpu.VMEM((rows, cols), jnp.float32), pltpu.SemaphoreType.DMA((rows // min(rows, 64),))],
        compiler_params=pltpu.CompilerParams(vmem_limit_bytes=12 << 20),
        name="diffuse",
    )(levels, beside, blend)


def body(sizes, cols, spectrum, pupil_mask, source_shifts, source_weights):
    turned, mirror, live, row_table, col_table, masks, blend = gather(
        spectrum, source_shifts, source_weights, pupil_mask, sizes, cols
    )
    sources = source_weights.shape[0] * sizes[2]
    count_x = blend.shape[1] // (sizes[0] * sizes[2])
    acc, inner = image(live, turned, mirror, row_table, col_table, masks, sizes)
    levels, beside = exchange(
        sources, live, acc, inner, turned, mirror, masks, row_table, col_table, count_x, sizes
    )
    return diffuse(levels, beside, blend, sizes)


def solution(mesh):
    sizes = (mesh.shape["tx"], mesh.shape["ty"], mesh.shape["src"])
    placed = (P(None, ("tx", "ty"), "src"), P(), P("src", None), P("src"))
    return jax.shard_map(
        functools.partial(body, sizes, COLS),
        mesh=mesh,
        in_specs=placed,
        out_specs=P(("tx", "src"), "ty"),
        check_vma=False,
    )
```
